512 devices in a mesh: tgt: 16 (over y, x), src: 32 (over z, core).
Axes of the slice: x: 4, y: 4, z: 16, core: 2. Of those that a mesh axis runs over, the one named last changes fastest.
Arguments:
- positions: float32 [3, 262144], P(None, ('tgt', 'src')), may hold values from -1 to 1
- velocities: float32 [3, 262144], P(None, ('tgt', 'src')), may hold values from -3 to 3
- accels: float32 [3, 262144], P(None, ('tgt', 'src')), may hold values from -6 to 6
- jerks: float32 [3, 262144], P(None, ('tgt', 'src')), may hold values from -12 to 12
- masses: float32 [262144], P(('tgt', 'src')), may hold values from 0.2 to 5
- levels: int32 [262144], P(('tgt', 'src')), may hold values from 0 to 3
- active_first: int32 [4096], P('tgt'), may hold values from -1 to 262143, as said below
- active_second: int32 [2048], P('tgt'), may hold values from -1 to 262143, as said below
Outputs:
- new_positions: float32 [3, 262144], P(None, ('tgt', 'src'))
- new_velocities: float32 [3, 262144], P(None, ('tgt', 'src'))
- new_accels: float32 [3, 262144], P(None, ('tgt', 'src'))
- new_jerks: float32 [3, 262144], P(None, ('tgt', 'src'))
The draws below stay inside these ranges and needn't reach their ends.
Inputs may be any that keep to these rules, and one draw needn't show every extreme that they name: Target group g owns slots g * 256 to (g + 1) * 256 - 1. In each group the star numbers come first and -1 fills the remaining slots; no star is named twice anywhere in active_first; every group names at least one star, and some group names 256. Target group g owns slots g * 128 to (g + 1) * 128 - 1. In each group the star numbers come first and -1 fills the remaining slots; no star is named twice anywhere in active_second; every group names at least one star, and some group names 128. Stars may also appear in active_first.
All inputs are finite; a program needn't handle non-finite values.
Results may differ from the reference program's by a relative error of at most 0.0003.
Values sent between devices are 32-bit elements; how exact they have to be, the bound alone decides.
No kernel may reach another device: no remote copies, remote signals or barrier semaphores. Data moves between devices by JAX's collectives and lax.ppermute only.
A program may use at most 64 MiB of HBM per device.

```python
import math
import jax
import jax.numpy as jnp
from jax import lax

GRP1 = 256
GRP2 = 128
TILE = 128
LEVELS = 4
NSTAR = 262144
N_TGT = 16


def draw_list(key, group_len):
    key_counts, key_group, key_shuffle = jax.random.split(key, 3)
    counts = jax.random.randint(key_counts, (N_TGT,), max(1, group_len // 8), group_len // 2 + 1)
    full_group = jax.random.randint(key_group, (), 0, N_TGT)
    counts = jnp.where(jnp.arange(N_TGT) == full_group, group_len, counts)
    shuffled = jax.random.permutation(key_shuffle, NSTAR)[:N_TGT * group_len].reshape(N_TGT, group_len)
    slot_index = jnp.arange(group_len)[None, :]
    return jnp.where(slot_index < counts[:, None], shuffled, -1).reshape(-1).astype(jnp.int32)


def draw_active_first(key, part):
    return draw_list(jax.random.fold_in(key, 7), GRP1)


def draw_active_second(key, part):
    return draw_list(jax.random.fold_in(key, 11), GRP2)


def plant(drawn, key, least, largest):
    dims = drawn.shape
    index_at = [jax.random.randint(jax.random.fold_in(key, axis), (), 0, dims[axis]) for axis in range(len(dims))]
    drawn = drawn.at[tuple(index_at)].set(least)
    longest = dims.index(max(dims))
    index_at[longest] = (index_at[longest] + 1) % dims[longest]
    return drawn.at[tuple(index_at)].set(largest)


def steps_of(rng, dims, cuts, least, largest):
    loudness, own = 1.0, jax.random.fold_in(rng, 6)
    for dim, parts in cuts:
        draws = jnp.exp(jax.random.uniform(jax.random.fold_in(own, dim), (parts,), jnp.float32, least / len(cuts), largest / len(cuts)))
        loudness = loudness * jnp.repeat(draws, dims[dim] // parts).reshape([-1 if axis == dim else 1 for axis in range(len(dims))])
    return loudness


def bell_draw(own_key, shape, deviation, reach, cuts=(), kind=jnp.bfloat16):
    factor_of = steps_of(own_key, shape, cuts, -0.22, 0.18) if cuts else 1.0
    drawn = jax.random.normal(own_key, shape, jnp.float32) * deviation * factor_of
    return jnp.minimum(jnp.maximum(drawn, -reach), reach).astype(kind)


def setup_inputs(seed: int = 0) -> dict:
    arg_keys = jax.random.split(jax.random.key(seed), 9)
    positions = jnp.clip(jax.random.uniform(arg_keys[0], (3, NSTAR), jnp.float32, -1.0, 1.0) * steps_of(arg_keys[0], (3, NSTAR), ((1, 512),), -0.4, 0.0), -1.0, 1.0)
    velocities = bell_draw(arg_keys[1], (3, NSTAR), 0.5, 3.0, ((1, 512),), jnp.float32)
    accels = bell_draw(arg_keys[2], (3, NSTAR), 1.0, 6.0, ((1, 512),), jnp.float32)
    jerks = bell_draw(arg_keys[3], (3, NSTAR), 2.0, 12.0, ((1, 512),), jnp.float32)
    masses = jnp.clip(jnp.exp(math.log(5.0) - 3.218876 * jax.random.uniform(arg_keys[4], (NSTAR,), jnp.float32) ** steps_of(arg_keys[4], (NSTAR,), ((0, 512),), -0.2, 0.2)), 0.2, 5.0)
    levels = plant(jax.random.randint(arg_keys[5], (NSTAR,), 0, LEVELS), jax.random.fold_in(arg_keys[5], 1), 0, LEVELS - 1).astype(jnp.int32)
    active_first = draw_active_first(jax.random.fold_in(arg_keys[8], 71), 0)
    active_second = draw_active_second(jax.random.fold_in(arg_keys[8], 71), 0)
    return dict(positions=positions, velocities=velocities, accels=accels, jerks=jerks, masses=masses, levels=levels, active_first=active_first, active_second=active_second)


SOFTENING_SQ = 0.0001
BASE_STEP = 0.5

def predict(states, span):
    ahead_pos = states[0:3] + span * (states[3:6] + span * (states[6:9] * 0.5 + span * states[9:12] / 6.0))
    moving = states[3:6] + span * (states[6:9] + span * states[9:12] * 0.5)
    return (ahead_pos, moving)

def pair_block(tile_place, tile_speed, tile_ident, sources, source_ident):
    offset = sources[0:3, None, :] - tile_place[:, :, None]
    motion = sources[3:6, None, :] - tile_speed[:, :, None]
    dist_sq = lax.optimization_barrier(jnp.sum(offset * offset, axis=0)) + SOFTENING_SQ
    inverse = lax.rsqrt(dist_sq)
    inverse_sq = inverse * inverse
    weight3 = jnp.where(source_ident[None, :] == tile_ident[:, None], 0.0, sources[6][None, :] * inverse_sq * inverse)
    closing = lax.optimization_barrier(jnp.sum(offset * motion, axis=0))
    attract = lax.optimization_barrier(jnp.sum(offset * weight3, axis=2))
    change = lax.optimization_barrier(jnp.sum(motion * weight3 - 3.0 * (closing * inverse_sq * weight3) * offset, axis=2))
    return jnp.concatenate([attract, change], axis=0)

def correct(ahead_pos, moving, old_accel, old_jolt, span, forces):
    new_acc = forces[0:3]
    new_jolt = forces[3:6]
    second_term = -6.0 * (old_accel - new_acc) - span * (4.0 * old_jolt + 2.0 * new_jolt)
    third_term = 12.0 * (old_accel - new_acc) + 6.0 * span * (old_jolt + new_jolt)
    new_place = ahead_pos + span * span * (second_term / 24.0 + third_term / 120.0)
    new_speed = moving + span * (second_term / 6.0 + third_term / 24.0)
    return jnp.concatenate([new_place, new_speed, new_acc, new_jolt], axis=0)

def target_forces(tgt_place, tgt_speed, tgt_ident, sources, source_ident):
    slot_count = tgt_place.shape[1]
    tile_count = slot_count // TILE
    block_len = min(8192, NSTAR)
    block_count = NSTAR // block_len
    src_blocks = sources.reshape(7, block_count, block_len).transpose(1, 0, 2)
    ident_blocks = source_ident.reshape(block_count, block_len)

    def per_tile(tile_no):
        place_tile = lax.dynamic_slice_in_dim(tgt_place, tile_no * TILE, TILE, 1)
        speed_tile = lax.dynamic_slice_in_dim(tgt_speed, tile_no * TILE, TILE, 1)
        ident_tile = lax.dynamic_slice_in_dim(tgt_ident, tile_no * TILE, TILE, 0)

        def add_block(running, source_pair):
            return (running + pair_block(place_tile, speed_tile, ident_tile, source_pair[0], source_pair[1]), None)
        running, _ = lax.scan(add_block, jnp.zeros((6, TILE), jnp.float32), (src_blocks, ident_blocks))
        return running
    tiled = lax.map(per_tile, jnp.arange(tile_count, dtype=jnp.int32))
    return tiled.transpose(1, 0, 2).reshape(6, slot_count)

def block_step(states, last_time, weights, active, now_time):
    span_all = now_time - last_time
    ahead_pos, moving = predict(states, span_all[None, :])
    sources = jnp.concatenate([ahead_pos, moving, weights[None, :]], axis=0)
    is_valid = active >= 0
    safe_ids = jnp.where(is_valid, active, 0).astype(jnp.int32)
    tgt_states = jnp.take(states, safe_ids, axis=1)
    tgt_span = jnp.take(span_all, safe_ids)[None, :]
    tgt_ahead = jnp.take(ahead_pos, safe_ids, axis=1)
    tgt_moving = jnp.take(moving, safe_ids, axis=1)
    forces = target_forces(tgt_ahead, tgt_moving, active, sources, jnp.arange(NSTAR, dtype=jnp.int32))
    corrected = correct(tgt_ahead, tgt_moving, tgt_states[6:9], tgt_states[9:12], tgt_span, forces)
    write_at = jnp.where(is_valid, active, NSTAR).astype(jnp.int32)
    states = states.at[:, write_at].set(corrected, mode='drop')
    last_time = last_time.at[write_at].set(now_time, mode='drop')
    return (states, last_time)

def reference(positions, velocities, accels, jerks, masses, levels, active_first, active_second):
    states = jnp.concatenate([positions, velocities, accels, jerks], axis=0)
    last_time = -BASE_STEP * jnp.exp2(-levels.astype(jnp.float32))
    weights = masses / NSTAR
    states, last_time = block_step(states, last_time, weights, active_first, 0.0)
    states, last_time = block_step(states, last_time, weights, active_second, BASE_STEP / (1 << LEVELS))
    return (states[0:3], states[3:6], states[6:9], states[9:12])
```

```python
import jax
import jax.numpy as jnp
from jax import lax
from jax.experimental import pallas as pl
from jax.experimental.pallas import tpu as pltpu
from jax.sharding import Mesh
from jax.sharding import PartitionSpec as P

TILE = 128
LEVELS = 4
LANES = 128
FIRST_ROOM = 256
SECOND_ROOM = 128

SOFTENING_SQ = 0.0001
BASE_STEP = 0.5
TIME_FIRST = 0.0
TIME_SECOND = BASE_STEP / (1 << LEVELS)
SRC = ("z", "core")


def sent_to_all(shard, axis):
    copies = jnp.broadcast_to(shard, (lax.axis_size(axis), *shard.shape))
    return lax.all_to_all(copies, axis, split_axis=0, concat_axis=0, tiled=True)


def laid_out(tiles, dim):
    dims = list(tiles.shape[1:])
    dims[dim] *= tiles.shape[0]
    return jnp.moveaxis(tiles, 0, dim).reshape(dims)


def gathered_copies(shard, axis, dim):
    tiles = sent_to_all(shard, axis)
    return laid_out(tiles, dim)


def over_pieces(shard, axis):
    return lax.all_gather(shard, axis).sum(0)


def taken_together(shard, axis):
    return sent_to_all(shard, axis).sum(axis=0)


def predict(states, span):
    ahead_pos = states[0:3] + span * (
        states[3:6] + span * (states[6:9] * 0.5 + span * states[9:12] / 6.0)
    )
    moving = states[3:6] + span * (states[6:9] + span * states[9:12] * 0.5)
    return (ahead_pos, moving)


def pair_block(tile_place, tile_speed, tile_ident, sources, source_ident):
    offset = sources[0:3, None, :] - tile_place[:, :, None]
    motion = sources[3:6, None, :] - tile_speed[:, :, None]
    dist_sq = jnp.sum(offset * offset, axis=0) + SOFTENING_SQ
    inverse = lax.rsqrt(dist_sq)
    inverse_sq = inverse * inverse
    weight3 = jnp.where(
        source_ident[None, :] == tile_ident[:, None],
        0.0,
        sources[6][None, :] * inverse_sq * inverse,
    )
    closing = jnp.sum(offset * motion, axis=0)
    attract = jnp.sum(offset * weight3, axis=2)
    change = jnp.sum(motion * weight3 - 3.0 * (closing * inverse_sq * weight3) * offset, axis=2)
    return jnp.concatenate([attract, change], axis=0)


def correct(ahead_pos, moving, old_accel, old_jolt, span, forces):
    new_acc = forces[0:3]
    new_jolt = forces[3:6]
    second_term = -6.0 * (old_accel - new_acc) - span * (4.0 * old_jolt + 2.0 * new_jolt)
    third_term = 12.0 * (old_accel - new_acc) + 6.0 * span * (old_jolt + new_jolt)
    new_place = ahead_pos + span * span * (second_term / 24.0 + third_term / 120.0)
    new_speed = moving + span * (second_term / 6.0 + third_term / 24.0)
    return jnp.concatenate([new_place, new_speed, new_acc, new_jolt], axis=0)


def tile_forces(held, tgt_ahead, tgt_moving, slot_ids, tiles_used, shard_part, idents):
    length = shard_part.shape[1]
    block_len = length
    while block_len > 2048 and block_len % 2 == 0:
        block_len = block_len // 2
    block_count = length // block_len
    src_blocks = shard_part.reshape(7, block_count, block_len).transpose(1, 0, 2)
    ident_blocks = idents.reshape(block_count, block_len)

    def one_tile(tile_no, carried):
        place_tile = lax.dynamic_slice_in_dim(tgt_ahead, tile_no * TILE, TILE, 1)
        speed_tile = lax.dynamic_slice_in_dim(tgt_moving, tile_no * TILE, TILE, 1)
        ident_tile = lax.dynamic_slice_in_dim(slot_ids, tile_no * TILE, TILE, 0)

        def add_block(running, source_pair):
            return (
                running
                + pair_block(place_tile, speed_tile, ident_tile, source_pair[0], source_pair[1]),
                None,
            )

        running, _ = lax.scan(
            add_block, jnp.zeros((6, TILE), jnp.float32), (src_blocks, ident_blocks)
        )
        before = lax.dynamic_slice_in_dim(carried, tile_no * TILE, TILE, 1)
        return lax.dynamic_update_slice_in_dim(carried, before + running, tile_no * TILE, 1)

    return lax.fori_loop(0, tiles_used, one_tile, held)


def advance(states, last_time, weights, active, now_time, s_dev, n_tgt, n_src, my_row, my_column):
    slot_count = active.shape[0]
    own_first = (my_row * n_src + my_column) * s_dev
    listed = gathered_copies(active, "tgt", 0)
    span_all = now_time - last_time
    my_slots = lax.dynamic_slice_in_dim(listed, my_row * slot_count, slot_count, 0)
    filled = jnp.sum((my_slots >= 0).astype(jnp.int32))
    tiles_used = (filled + TILE - 1) // TILE
    local_at = listed - own_first
    is_owned = (listed >= 0) & (local_at >= 0) & (local_at < s_dev)
    stacked = jnp.concatenate([states, span_all[None, :], weights[None, :]], axis=0)
    column_all = gathered_copies(stacked, "tgt", 1)
    owner_col = my_slots // s_dev % n_src
    places = my_slots // (s_dev * n_src) * s_dev + my_slots % s_dev
    mine_owned = (my_slots >= 0) & (owner_col == my_column)
    chosen = jnp.take(column_all[0:13], jnp.clip(places, 0, n_tgt * s_dev - 1), axis=1)
    partial_rows = jnp.where(mine_owned[None, :], chosen, 0.0)
    ahead_pos, moving = predict(column_all[0:12], column_all[12:13])
    sources = jnp.concatenate([ahead_pos, moving, column_all[13:14]], axis=0)
    target = over_pieces(partial_rows, SRC)
    tgt_ahead, tgt_moving = predict(target[0:12], target[12:13])
    zero_forces = jnp.zeros((6, slot_count), jnp.float32)
    columns = jnp.arange(sources.shape[1], dtype=jnp.int32)
    idents = columns // s_dev * (s_dev * n_src) + my_column * s_dev + columns % s_dev
    partial_forces = tile_forces(
        zero_forces, tgt_ahead, tgt_moving, my_slots, tiles_used, sources, idents
    )
    forces = taken_together(partial_forces, SRC)
    corrected = correct(tgt_ahead, tgt_moving, target[6:9], target[9:12], target[12:13], forces)
    returned = gathered_copies(corrected, "tgt", 1)
    write_at = jnp.where(is_owned, local_at, s_dev)
    states = states.at[:, write_at].set(returned, mode="drop")
    last_time = last_time.at[write_at].set(now_time, mode="drop")
    return (states, last_time)


def whole_program(positions, velocities, accels, jerks, masses, levels, active_first, active_second):
    s_dev = positions.shape[1]
    n_tgt = lax.axis_size("tgt")
    n_src = lax.axis_size(SRC)
    my_row = lax.axis_index("tgt")
    my_column = lax.axis_index(SRC)
    weights = masses / (s_dev * n_tgt * n_src)
    states = jnp.concatenate([positions, velocities, accels, jerks], axis=0)
    last_time = -BASE_STEP * jnp.exp2(-levels.astype(jnp.float32))
    for now_time, active in ((TIME_FIRST, active_first), (TIME_SECOND, active_second)):
        states, last_time = advance(
            states, last_time, weights, active, now_time, s_dev, n_tgt, n_src, my_row, my_column
        )
    return (states[0:3], states[3:6], states[6:9], states[9:12])


def log2_of(size):
    assert size & (size - 1) == 0, "size"
    return size.bit_length() - 1


def iota(shape, dim):
    return lax.broadcasted_iota(jnp.int32, shape, dim)


def lane_pick(table, lanes):
    return lax.gather(
        table,
        lanes[:, :, None],
        lax.GatherDimensionNumbers(
            offset_dims=(),
            collapsed_slice_dims=(1,),
            start_index_map=(1,),
            operand_batching_dims=(0,),
            start_indices_batching_dims=(0,),
        ),
        slice_sizes=(1, 1),
        mode=lax.GatherScatterMode.PROMISE_IN_BOUNDS,
    )


def turned(rows):
    pad = jnp.zeros((LANES - rows.shape[0], LANES), rows.dtype)
    return jnp.concatenate([rows, pad], axis=0).T


def rows_of(values, count):
    width = values[0].shape[1]
    below = count - sum(v.shape[0] for v in values)
    pad = [jnp.zeros((below, width), jnp.float32)] if below else []
    return jnp.concatenate(list(values) + pad, axis=0)


def prepare_kernel(pos, vel, acc, jerk, mass, levels, first, second, column_out, row_out):
    s_dev = pos.shape[1]
    stars = row_out.shape[0]
    last = -BASE_STEP * jnp.exp2(-levels[...].astype(jnp.float32))
    states = jnp.concatenate([pos[...], vel[...], acc[...], jerk[...]], axis=0)
    room = first.shape[1] + second.shape[1]
    lists = [first[...].astype(jnp.float32), second[...].astype(jnp.float32)]
    if s_dev > room:
        lists.append(jnp.full((1, s_dev - room), -1.0, jnp.float32))
    listed = jnp.concatenate(lists, axis=1)
    column = rows_of([states, last, listed], 16)
    ahead, moving = predict(states, TIME_FIRST - last)
    row = rows_of([ahead, moving, mass[...]], 8)
    for copy in range(column_out.shape[0]):
        column_out[copy] = column
    for copy in range(stars):
        row_out[copy] = row


def matching_slots(listed, column, n_src, s_dev):
    ids = listed.astype(jnp.int32)
    valid = ids >= 0
    column_of = jnp.where(valid, (ids >> log2_of(s_dev)) & (n_src - 1), -1)
    per_column = jnp.zeros((n_src, ids.shape[1]), jnp.float32)
    for row in range(ids.shape[0]):
        here = column_of[row : row + 1] == iota((n_src, ids.shape[1]), 0)
        per_column = per_column + here.astype(jnp.float32)
    most = jnp.max(jnp.sum(per_column, axis=1, keepdims=True))
    return column_of == column, most


def packed_ids(listed, mine, room):
    n_rows, width = listed.shape
    flags = mine.astype(jnp.float32)
    upto = (iota((width, width), 0) <= iota((width, width), 1)).astype(jnp.bfloat16)
    inside = jnp.dot(flags.astype(jnp.bfloat16), upto, preferred_element_type=jnp.float32)
    totals = jnp.broadcast_to(inside[:, width - 1 : width], (n_rows, LANES))
    place = jnp.zeros((1, LANES), jnp.float32)
    before = []
    for row in range(n_rows):
        before.append(place)
        place = place + totals[row : row + 1]
    count = jnp.max(place)
    start = jnp.concatenate(before, axis=0)[:, 0:1]
    slot = jnp.where(mine, (inside + start).astype(jnp.int32) - 1, -1)
    columns, rows = [], []
    for part in range(room // LANES):
        found = jnp.zeros((LANES, LANES), jnp.float32)
        want = iota((LANES, LANES), 0) + part * LANES
        for row in range(n_rows):
            for chunk in range(width // LANES):
                cut = slice(chunk * LANES, (chunk + 1) * LANES)
                hit = jnp.broadcast_to(slot[row : row + 1, cut], (LANES, LANES)) == want
                found = found + jnp.where(hit, listed[row : row + 1, cut] + 1.0, 0.0)
        ids = jnp.broadcast_to(jnp.sum(found, axis=1, keepdims=True) - 1.0, (LANES, LANES))
        columns.append(ids)
        rows.append(ids.T[0:1])
    return columns, rows, count


def select_kernel(n_src, slots_first, slots_second, where_am_i, held, target_out, turned_out, info_out):
    n_tgt, _, s_dev = held.shape
    my_row, my_column = where_am_i[0], where_am_i[1]
    star_bits, row_bits = log2_of(s_dev), log2_of(s_dev * n_src)
    listed = held[:, 13, :]
    first, second = listed[:, :slots_first], listed[:, slots_first : slots_first + slots_second]
    mine_first, most_first = matching_slots(first, my_column, n_src, s_dev)
    mine_second, most_second = matching_slots(second, my_column, n_src, s_dev)
    cols_first, rows_first, count_first = packed_ids(first, mine_first, FIRST_ROOM)
    cols_second, rows_second, count_second = packed_ids(second, mine_second, SECOND_ROOM)
    info_out[0] = count_first.astype(jnp.int32)
    info_out[1] = count_second.astype(jnp.int32)
    fits = (most_first <= FIRST_ROOM) & (most_second <= SECOND_ROOM)
    info_out[2] = fits.astype(jnp.int32)
    info_out[3] = my_row
    ids = [r.astype(jnp.int32) for r in rows_first + rows_second]
    per_row = s_dev // LANES
    lane = [jnp.broadcast_to(i & (LANES - 1), (16, LANES)) for i in ids]
    chunk_of = [
        jnp.where(i >= 0, (i >> row_bits) * per_row + ((i & (s_dev - 1)) >> log2_of(LANES)), -1) for i in ids
    ]

    def one_row(row, picked):
        for chunk in range(per_row):
            table = held[row, :, chunk * LANES : (chunk + 1) * LANES]
            picked = [
                jnp.where(chunk_of[g] == row * per_row + chunk, lane_pick(table, lane[g]), picked[g])
                for g in range(len(ids))
            ]
        return picked

    picked = lax.fori_loop(0, n_tgt, one_row, [jnp.zeros((16, LANES), jnp.float32)] * len(ids))
    for g, (states, number) in enumerate(zip(picked, ids)):
        key = jnp.where((number >= 0) & ((number >> row_bits) == my_row), number & (s_dev - 1), -1)
        ahead, moving = predict(states[0:12], TIME_FIRST - states[12:13])
        key = key.astype(jnp.float32)
        number = number.astype(jnp.float32)
        cut = slice(g * LANES, (g + 1) * LANES)
        target_out[:, cut] = rows_of([states[0:13], number, key], 16)
        turned_out[cut, :] = turned(rows_of([ahead, moving, key, number], 8))


def force_kernel(info, near, far, turned_in, force_out, sums):
    count, my_z = info[0], info[1]
    n_z, _, s_dev = near.shape
    copies, _, room = force_out.shape
    tall = 16
    sums[...] = jnp.zeros_like(sums)

    def one_block(block, _):
        at = pl.ds(pl.multiple_of(block * tall, tall), tall)
        facts = turned_in[at, :]
        target = [jnp.broadcast_to(facts[:, j : j + 1], (tall, LANES)) for j in range(6)]
        key = jnp.broadcast_to(facts[:, 6:7], (tall, LANES)).astype(jnp.int32)

        def segment(ref, which, running, own):
            running = list(running)
            for chunk in range(s_dev // LANES):
                cut = slice(chunk * LANES, (chunk + 1) * LANES)
                source = [jnp.broadcast_to(ref[which, j : j + 1, cut], (tall, LANES)) for j in range(7)]
                rx, ry, rz = (source[j] - target[j] for j in range(3))
                ux, uy, uz = (source[j] - target[j] for j in range(3, 6))
                inverse = lax.rsqrt((rx * rx + ry * ry + rz * rz) + SOFTENING_SQ)
                inverse_sq = inverse * inverse
                weight3 = source[6] * inverse * inverse_sq
                if own:
                    weight3 = jnp.where(key == iota((tall, LANES), 1) + chunk * LANES, 0.0, weight3)
                closing = (rx * ux + ry * uy + rz * uz) * inverse_sq * weight3
                parts = (
                    rx * weight3, ry * weight3, rz * weight3,
                    ux * weight3, uy * weight3, uz * weight3,
                    rx * closing, ry * closing, rz * closing,
                )
                running = [a + b for a, b in zip(running, parts)]
            return tuple(running)

        def both(step, running):
            running = segment(far, step, running, False)
            which = jnp.where(step < my_z, step, step + 1)
            which = jnp.where(step == n_z - 1, my_z, which)
            return lax.cond(
                step == n_z - 1,
                lambda r: segment(near, which, r, True),
                lambda r: segment(near, which, r, False),
                running,
            )

        zero = jnp.zeros((tall, LANES), jnp.float32)
        running = lax.fori_loop(0, n_z, both, (zero,) * 9)
        totals = [jnp.sum(r, axis=1, keepdims=True) for r in running]
        totals = totals[0:3] + [totals[3 + j] - 3.0 * totals[6 + j] for j in range(3)]
        lanes = iota((tall, LANES), 1)
        packed = jnp.zeros((tall, LANES), jnp.float32)
        for j in range(6):
            packed = jnp.where(lanes == j, jnp.broadcast_to(totals[j], (tall, LANES)), packed)
        sums[at, :] = packed
        return 0

    lax.fori_loop(0, (count + tall - 1) // tall, one_block, 0)
    for part in range(room // LANES):
        cut = slice(part * LANES, (part + 1) * LANES)
        rows = sums[cut, :].T[0:8]
        for copy in range(copies):
            force_out[copy, :, cut] = rows


def summed(received):
    total = received[0]
    for row in range(1, received.shape[0]):
        total = total + received[row]
    return total


def placed(values, keys, old, room):
    s_dev = old.shape[1]
    outs, hits = [], []
    for chunk in range(s_dev // LANES):
        star = (iota((LANES, LANES), 1) + chunk * LANES).astype(jnp.float32)
        found = jnp.zeros((LANES, LANES), jnp.float32)
        for part in range(room // LANES):
            number = (iota((LANES, LANES), 0) + part * LANES + 1).astype(jnp.float32)
            found = found + jnp.where(keys[part] == star, number, 0.0)
        slot = jnp.sum(found, axis=0, keepdims=True).astype(jnp.int32) - 1
        new = picked_slots(values, slot, room)
        hit = slot >= 0
        hits.append(hit)
        outs.append(jnp.where(hit, new, old[:, chunk * LANES : (chunk + 1) * LANES]))
    return outs, hits


def picked_slots(values, slot, room):
    lane = jnp.broadcast_to(slot & (LANES - 1), (16, LANES))
    new = jnp.zeros((16, LANES), jnp.float32)
    for part in range(room // LANES):
        pick = lane_pick(values[:, part * LANES : (part + 1) * LANES], lane)
        new = jnp.where((slot >> log2_of(LANES)) == part, pick, new)
    return new


def correct_kernel(received, target, turned_in, old_states, old_last, weights, row_out, own_out, second_out, turned_out):
    copies, _, s_dev = row_out.shape
    room = received.shape[2]
    forces = summed(received)
    states = target[0:12, :room]
    span = TIME_FIRST - target[12:13, :room]
    ahead, moving = predict(states, span)
    corrected = correct(ahead, moving, states[6:9], states[9:12], span, forces[0:6])
    corrected = jnp.concatenate([corrected, jnp.full((1, room), TIME_FIRST, jnp.float32), jnp.zeros((3, room), jnp.float32)], axis=0)
    columns = [turned_in[part * LANES : (part + 1) * LANES, :] for part in range(room // LANES)]
    keys = [jnp.broadcast_to(c[:, 6:7], (LANES, LANES)) for c in columns]
    numbers = [jnp.broadcast_to(c[:, 7:8], (LANES, LANES)) for c in columns]
    old = rows_of([old_states[...], old_last[...]], 16)
    outs, _ = placed(corrected, keys, old, room)
    for chunk, states_new in enumerate(outs):
        cut = slice(chunk * LANES, (chunk + 1) * LANES)
        own_out[:, cut] = states_new
        ahead, moving = predict(states_new[0:12], TIME_SECOND - states_new[12:13])
        row = rows_of([ahead, moving, weights[:, cut]], 8)
        for copy in range(copies):
            row_out[copy, :, cut] = row
    other = target[:, room : room + SECOND_ROOM]
    number = other[13:14]
    found = jnp.zeros((LANES, LANES), jnp.float32)
    for part in range(room // LANES):
        place = (iota((LANES, LANES), 0) + part * LANES + 1).astype(jnp.float32)
        found = found + jnp.where((numbers[part] == number) & (numbers[part] >= 0.0), place, 0.0)
    slot = jnp.sum(found, axis=0, keepdims=True).astype(jnp.int32) - 1
    states = jnp.where(slot >= 0, picked_slots(corrected, slot, room), other)
    span = TIME_SECOND - states[12:13]
    ahead, moving = predict(states[0:12], span)
    second_out[...] = rows_of([ahead, moving, states[6:12], span], 16)
    turned_out[...] = turned(rows_of([ahead, moving, other[14:15]], 8))


def finish_kernel(received, second, turned_in, own, pos_out, vel_out, acc_out, jerk_out):
    forces = summed(received)
    facts = second[...]
    corrected = correct(facts[0:3], facts[3:6], facts[6:9], facts[9:12], facts[12:13], forces[0:6])
    corrected = jnp.concatenate([corrected, jnp.zeros((4, SECOND_ROOM), jnp.float32)], axis=0)
    keys = [jnp.broadcast_to(turned_in[:, 6:7], (LANES, LANES))]
    outs, _ = placed(corrected, keys, own[...], SECOND_ROOM)
    for chunk, new in enumerate(outs):
        cut = slice(chunk * LANES, (chunk + 1) * LANES)
        pos_out[:, cut] = new[0:3]
        vel_out[:, cut] = new[3:6]
        acc_out[:, cut] = new[6:9]
        jerk_out[:, cut] = new[9:12]


def f32(*shape):
    return jax.ShapeDtypeStruct(shape, jnp.float32)


INTERPRET = False


def call(kernel, outs, name, scalars=0, operands=0, scratch=(), smem_out=None):
    smem, vmem = pl.BlockSpec(memory_space=pltpu.SMEM), pl.BlockSpec(memory_space=pltpu.VMEM)
    return pl.pallas_call(
        kernel,
        out_shape=outs,
        in_specs=[smem] * scalars + [vmem] * operands,
        out_specs=tuple(smem if i == smem_out else vmem for i in range(len(outs))),
        scratch_shapes=list(scratch),
        name=name,
        interpret=INTERPRET,
    )


def exchanged(copies, axis):
    return lax.all_to_all(copies, axis, split_axis=0, concat_axis=0, tiled=True)


def other_core(near):
    return lax.ppermute(near, "core", [(0, 1), (1, 0)])


def shards(positions, velocities, accels, jerks, masses, levels, active_first, active_second):
    s_dev = positions.shape[1]
    n_tgt, n_z, n_src = lax.axis_size("tgt"), lax.axis_size("z"), lax.axis_size(SRC)
    my_row, my_column, my_z = lax.axis_index("tgt"), lax.axis_index(SRC), lax.axis_index("z")
    weights = (masses / (s_dev * n_tgt * n_src)).reshape(1, s_dev)
    column_copies, row_copies = call(prepare_kernel, (f32(n_tgt, 16, s_dev), f32(n_z, 8, s_dev)), "prepare", 0, 8)(
        positions, velocities, accels, jerks, weights, levels.reshape(1, s_dev),
        active_first.reshape(1, -1), active_second.reshape(1, -1),
    )
    near = exchanged(row_copies, "z")
    column = exchanged(column_copies, "tgt")
    far = other_core(near)
    all_room = FIRST_ROOM + SECOND_ROOM

    def select(where_am_i, held, *outs):
        select_kernel(n_src, active_first.shape[0], active_second.shape[0], where_am_i, held, *outs)

    target, columns, info = call(
        select, (f32(16, all_room), f32(all_room, LANES), jax.ShapeDtypeStruct((4,), jnp.int32)), "select", 1, 1, smem_out=2
    )(jnp.stack([my_row, my_column]).astype(jnp.int32), column)

    def by_columns(args):
        near, far, target, columns, info, weights = args[:6]
        states = jnp.concatenate(args[6:10], axis=0)
        last = -BASE_STEP * jnp.exp2(-args[11].astype(jnp.float32)).reshape(1, s_dev)
        first_info = jnp.stack([info[0], my_z]).astype(jnp.int32)
        second_info = jnp.stack([info[1], my_z]).astype(jnp.int32)
        (partial,) = call(
            force_kernel, (f32(n_tgt, 8, FIRST_ROOM),), "forces_first", 1, 3, [pltpu.VMEM((FIRST_ROOM, LANES), jnp.float32)]
        )(first_info, near, far, columns)
        received = exchanged(partial, "tgt")
        row_copies, own, second, second_columns = call(
            correct_kernel,
            (f32(n_z, 8, s_dev), f32(16, s_dev), f32(16, SECOND_ROOM), f32(LANES, LANES)),
            "correct", 0, 6,
        )(received, target, columns, states, last, weights)
        near = exchanged(row_copies, "z")
        far = other_core(near)
        (partial,) = call(
            force_kernel, (f32(n_tgt, 8, SECOND_ROOM),), "forces_second", 1, 3, [pltpu.VMEM((SECOND_ROOM, LANES), jnp.float32)]
        )(second_info, near, far, second_columns)
        received = exchanged(partial, "tgt")
        return call(finish_kernel, (f32(3, s_dev),) * 4, "finish", 0, 4)(received, second, second_columns, own)

    inputs = (positions, velocities, accels, jerks, masses, levels, active_first, active_second)
    return lax.cond(
        info[2] == 1,
        lambda args: tuple(by_columns(args)),
        lambda args: whole_program(*args[6:]),
        (near, far, target, columns, info, weights, *inputs),
    )


def solution(mesh):
    n_tgt, n_src = mesh.devices.shape
    finer = Mesh(mesh.devices.reshape(n_tgt, n_src // 2, 2), ("tgt", "z", "core"))
    stars = ("tgt", "z", "core")
    vector, scalar = P(None, stars), P(stars)
    return jax.shard_map(
        shards,
        mesh=finer,
        in_specs=(vector, vector, vector, vector, scalar, scalar, P("tgt"), P("tgt")),
        out_specs=(vector,) * 4,
        check_vma=False,
    )
```

```python
import functools

import jax
import jax.numpy as jnp
from jax import lax
from jax.experimental import pallas as pl
from jax.experimental.pallas import tpu as pltpu
from jax.sharding import Mesh
from jax.sharding import PartitionSpec as P

TILE = 128
LEVELS = 4
LANES = 128
FIRST_ROOM = 256
SECOND_ROOM = 128

SOFTENING_SQ = 0.0001
BASE_STEP = 0.5
TIME_FIRST = 0.0
TIME_SECOND = BASE_STEP / (1 << LEVELS)
SRC = ("z", "core")


def sent_to_all(shard, axis):
    copies = jnp.broadcast_to(shard, (lax.axis_size(axis), *shard.shape))
    return lax.all_to_all(copies, axis, split_axis=0, concat_axis=0, tiled=True)


def laid_out(tiles, dim):
    dims = list(tiles.shape[1:])
    dims[dim] *= tiles.shape[0]
    return jnp.moveaxis(tiles, 0, dim).reshape(dims)


def gathered_copies(shard, axis, dim):
    tiles = sent_to_all(shard, axis)
    return laid_out(tiles, dim)


def over_pieces(shard, axis):
    return lax.all_gather(shard, axis).sum(0)


def taken_together(shard, axis):
    return sent_to_all(shard, axis).sum(axis=0)


def predict(states, span):
    ahead_pos = states[0:3] + span * (
        states[3:6] + span * (states[6:9] * 0.5 + span * states[9:12] / 6.0)
    )
    moving = states[3:6] + span * (states[6:9] + span * states[9:12] * 0.5)
    return (ahead_pos, moving)


def pair_block(tile_place, tile_speed, tile_ident, sources, source_ident):
    offset = sources[0:3, None, :] - tile_place[:, :, None]
    motion = sources[3:6, None, :] - tile_speed[:, :, None]
    dist_sq = jnp.sum(offset * offset, axis=0) + SOFTENING_SQ
    inverse = lax.rsqrt(dist_sq)
    inverse_sq = inverse * inverse
    weight3 = jnp.where(
        source_ident[None, :] == tile_ident[:, None],
        0.0,
        sources[6][None, :] * inverse_sq * inverse,
    )
    closing = jnp.sum(offset * motion, axis=0)
    attract = jnp.sum(offset * weight3, axis=2)
    change = jnp.sum(motion * weight3 - 3.0 * (closing * inverse_sq * weight3) * offset, axis=2)
    return jnp.concatenate([attract, change], axis=0)


def correct(ahead_pos, moving, old_accel, old_jolt, span, forces):
    new_acc = forces[0:3]
    new_jolt = forces[3:6]
    second_term = -6.0 * (old_accel - new_acc) - span * (4.0 * old_jolt + 2.0 * new_jolt)
    third_term = 12.0 * (old_accel - new_acc) + 6.0 * span * (old_jolt + new_jolt)
    new_place = ahead_pos + span * span * (second_term / 24.0 + third_term / 120.0)
    new_speed = moving + span * (second_term / 6.0 + third_term / 24.0)
    return jnp.concatenate([new_place, new_speed, new_acc, new_jolt], axis=0)


def tile_forces(held, tgt_ahead, tgt_moving, slot_ids, tiles_used, shard_part, idents):
    length = shard_part.shape[1]
    block_len = length
    while block_len > 2048 and block_len % 2 == 0:
        block_len = block_len // 2
    block_count = length // block_len
    src_blocks = shard_part.reshape(7, block_count, block_len).transpose(1, 0, 2)
    ident_blocks = idents.reshape(block_count, block_len)

    def one_tile(tile_no, carried):
        place_tile = lax.dynamic_slice_in_dim(tgt_ahead, tile_no * TILE, TILE, 1)
        speed_tile = lax.dynamic_slice_in_dim(tgt_moving, tile_no * TILE, TILE, 1)
        ident_tile = lax.dynamic_slice_in_dim(slot_ids, tile_no * TILE, TILE, 0)

        def add_block(running, source_pair):
            return (
                running
                + pair_block(place_tile, speed_tile, ident_tile, source_pair[0], source_pair[1]),
                None,
            )

        running, _ = lax.scan(
            add_block, jnp.zeros((6, TILE), jnp.float32), (src_blocks, ident_blocks)
        )
        before = lax.dynamic_slice_in_dim(carried, tile_no * TILE, TILE, 1)
        return lax.dynamic_update_slice_in_dim(carried, before + running, tile_no * TILE, 1)

    return lax.fori_loop(0, tiles_used, one_tile, held)


def advance(states, last_time, weights, active, now_time, s_dev, n_tgt, n_src, my_row, my_column):
    slot_count = active.shape[0]
    own_first = (my_row * n_src + my_column) * s_dev
    listed = gathered_copies(active, "tgt", 0)
    span_all = now_time - last_time
    my_slots = lax.dynamic_slice_in_dim(listed, my_row * slot_count, slot_count, 0)
    filled = jnp.sum((my_slots >= 0).astype(jnp.int32))
    tiles_used = (filled + TILE - 1) // TILE
    local_at = listed - own_first
    is_owned = (listed >= 0) & (local_at >= 0) & (local_at < s_dev)
    stacked = jnp.concatenate([states, span_all[None, :], weights[None, :]], axis=0)
    column_all = gathered_copies(stacked, "tgt", 1)
    owner_col = my_slots // s_dev % n_src
    places = my_slots // (s_dev * n_src) * s_dev + my_slots % s_dev
    mine_owned = (my_slots >= 0) & (owner_col == my_column)
    chosen = jnp.take(column_all[0:13], jnp.clip(places, 0, n_tgt * s_dev - 1), axis=1)
    partial_rows = jnp.where(mine_owned[None, :], chosen, 0.0)
    ahead_pos, moving = predict(column_all[0:12], column_all[12:13])
    sources = jnp.concatenate([ahead_pos, moving, column_all[13:14]], axis=0)
    target = over_pieces(partial_rows, SRC)
    tgt_ahead, tgt_moving = predict(target[0:12], target[12:13])
    zero_forces = jnp.zeros((6, slot_count), jnp.float32)
    columns = jnp.arange(sources.shape[1], dtype=jnp.int32)
    idents = columns // s_dev * (s_dev * n_src) + my_column * s_dev + columns % s_dev
    partial_forces = tile_forces(
        zero_forces, tgt_ahead, tgt_moving, my_slots, tiles_used, sources, idents
    )
    forces = taken_together(partial_forces, SRC)
    corrected = correct(tgt_ahead, tgt_moving, target[6:9], target[9:12], target[12:13], forces)
    returned = gathered_copies(corrected, "tgt", 1)
    write_at = jnp.where(is_owned, local_at, s_dev)
    states = states.at[:, write_at].set(returned, mode="drop")
    last_time = last_time.at[write_at].set(now_time, mode="drop")
    return (states, last_time)


def whole_program(positions, velocities, accels, jerks, masses, levels, active_first, active_second):
    s_dev = positions.shape[1]
    n_tgt = lax.axis_size("tgt")
    n_src = lax.axis_size(SRC)
    my_row = lax.axis_index("tgt")
    my_column = lax.axis_index(SRC)
    weights = masses / (s_dev * n_tgt * n_src)
    states = jnp.concatenate([positions, velocities, accels, jerks], axis=0)
    last_time = -BASE_STEP * jnp.exp2(-levels.astype(jnp.float32))
    for now_time, active in ((TIME_FIRST, active_first), (TIME_SECOND, active_second)):
        states, last_time = advance(
            states, last_time, weights, active, now_time, s_dev, n_tgt, n_src, my_row, my_column
        )
    return (states[0:3], states[3:6], states[6:9], states[9:12])


def log2_of(size):
    assert size & (size - 1) == 0, "size"
    return size.bit_length() - 1


def iota(shape, dim):
    return lax.broadcasted_iota(jnp.int32, shape, dim)


def lane_pick(table, lanes):
    return lax.gather(
        table,
        lanes[:, :, None],
        lax.GatherDimensionNumbers(
            offset_dims=(),
            collapsed_slice_dims=(1,),
            start_index_map=(1,),
            operand_batching_dims=(0,),
            start_indices_batching_dims=(0,),
        ),
        slice_sizes=(1, 1),
        mode=lax.GatherScatterMode.PROMISE_IN_BOUNDS,
    )


def turned(rows):
    pad = jnp.zeros((LANES - rows.shape[0], LANES), rows.dtype)
    return jnp.concatenate([rows, pad], axis=0).T


def rows_of(values, count):
    width = values[0].shape[1]
    below = count - sum(v.shape[0] for v in values)
    pad = [jnp.zeros((below, width), jnp.float32)] if below else []
    return jnp.concatenate(list(values) + pad, axis=0)


def prepare_kernel(n_stars, pos, vel, acc, jerk, mass, levels, first, second, column_out, row_out, own_out):
    s_dev = pos.shape[1]
    stars = row_out.shape[0]
    last = -BASE_STEP * jnp.exp2(-levels[...].astype(jnp.float32))
    states = jnp.concatenate([pos[...], vel[...], acc[...], jerk[...]], axis=0)
    room = first.shape[1] + second.shape[1]
    lists = [first[...].astype(jnp.float32), second[...].astype(jnp.float32)]
    if s_dev > room:
        lists.append(jnp.full((1, s_dev - room), -1.0, jnp.float32))
    listed = jnp.concatenate(lists, axis=1)
    column = rows_of([states, last, listed], 16)
    ahead, moving = predict(states, TIME_FIRST - last)
    weights = mass[...] / n_stars
    row = rows_of([ahead, moving, weights], 8)
    own_out[...] = rows_of([states, last, weights], 16)
    for copy in range(column_out.shape[0]):
        column_out[copy] = column
    for copy in range(stars):
        row_out[copy] = row


def matching_slots(listed, column, n_src, s_dev):
    ids = listed.astype(jnp.int32)
    valid = ids >= 0
    column_of = jnp.where(valid, (ids >> log2_of(s_dev)) & (n_src - 1), -1)
    per_column = jnp.zeros((n_src, ids.shape[1]), jnp.float32)
    for row in range(ids.shape[0]):
        here = column_of[row : row + 1] == iota((n_src, ids.shape[1]), 0)
        per_column = per_column + here.astype(jnp.float32)
    most = jnp.max(jnp.sum(per_column, axis=1, keepdims=True))
    return column_of == column, most


def packed_ids(listed, mine, room):
    n_rows, width = listed.shape
    flags = mine.astype(jnp.float32)
    upto = (iota((width, width), 0) <= iota((width, width), 1)).astype(jnp.bfloat16)
    inside = jnp.dot(flags.astype(jnp.bfloat16), upto, preferred_element_type=jnp.float32)
    totals = jnp.broadcast_to(inside[:, width - 1 : width], (n_rows, LANES))
    place = jnp.zeros((1, LANES), jnp.float32)
    before = []
    for row in range(n_rows):
        before.append(place)
        place = place + totals[row : row + 1]
    count = jnp.max(place)
    start = jnp.concatenate(before, axis=0)[:, 0:1]
    slot = jnp.where(mine, (inside + start).astype(jnp.int32) - 1, -1)
    columns, rows = [], []
    for part in range(room // LANES):
        found = jnp.zeros((LANES, LANES), jnp.float32)
        want = iota((LANES, LANES), 0) + part * LANES
        for row in range(n_rows):
            for chunk in range(width // LANES):
                cut = slice(chunk * LANES, (chunk + 1) * LANES)
                hit = jnp.broadcast_to(slot[row : row + 1, cut], (LANES, LANES)) == want
                found = found + jnp.where(hit, listed[row : row + 1, cut] + 1.0, 0.0)
        ids = jnp.broadcast_to(jnp.sum(found, axis=1, keepdims=True) - 1.0, (LANES, LANES))
        columns.append(ids)
        rows.append(ids.T[0:1])
    return columns, rows, count


def select_kernel(n_src, slots_first, slots_second, held, target_out, turned_out, info_out):
    n_tgt, _, s_dev = held.shape
    my_row, my_column = lax.axis_index("tgt"), lax.axis_index(SRC)
    row_bits = log2_of(s_dev * n_src)
    listed = held[:, 13, :]
    first, second = listed[:, :slots_first], listed[:, slots_first : slots_first + slots_second]
    mine_first, most_first = matching_slots(first, my_column, n_src, s_dev)
    mine_second, most_second = matching_slots(second, my_column, n_src, s_dev)
    _, rows_first, count_first = packed_ids(first, mine_first, FIRST_ROOM)
    _, rows_second, count_second = packed_ids(second, mine_second, SECOND_ROOM)
    info_out[0] = count_first.astype(jnp.int32)
    info_out[1] = count_second.astype(jnp.int32)
    fits = (most_first <= FIRST_ROOM) & (most_second <= SECOND_ROOM)
    info_out[2] = fits.astype(jnp.int32)
    info_out[3] = lax.axis_index("z")
    ids = [r.astype(jnp.int32) for r in rows_first + rows_second]
    per_row = s_dev // LANES
    lane = [jnp.broadcast_to(i & (LANES - 1), (16, LANES)) for i in ids]
    chunk_of = [
        jnp.where(i >= 0, (i >> row_bits) * per_row + ((i & (s_dev - 1)) >> log2_of(LANES)), -1) for i in ids
    ]

    def one_row(row, picked):
        for chunk in range(per_row):
            table = held[row, :, chunk * LANES : (chunk + 1) * LANES]
            picked = [
                jnp.where(chunk_of[g] == row * per_row + chunk, lane_pick(table, lane[g]), picked[g])
                for g in range(len(ids))
            ]
        return picked

    picked = lax.fori_loop(0, n_tgt, one_row, [jnp.zeros((16, LANES), jnp.float32)] * len(ids))
    for g, (states, number) in enumerate(zip(picked, ids)):
        key = jnp.where((number >= 0) & ((number >> row_bits) == my_row), number & (s_dev - 1), -1)
        ahead, moving = predict(states[0:12], TIME_FIRST - states[12:13])
        key = key.astype(jnp.float32)
        number = number.astype(jnp.float32)
        cut = slice(g * LANES, (g + 1) * LANES)
        target_out[:, cut] = rows_of([states[0:13], number, key], 16)
        turned_out[cut, :] = turned(rows_of([ahead, moving, key, number], 8))


def force_sums(count, my_z, turned_in, near_of, far_of, s_dev, n_z, force_out, sums):
    copies, _, room = force_out.shape
    sums[...] = jnp.zeros_like(sums)

    def one_block(first, tall):
        at = pl.ds(pl.multiple_of(first, 8), tall)
        facts = turned_in[at, :]
        target = [jnp.broadcast_to(facts[:, j : j + 1], (tall, LANES)) for j in range(6)]
        key = jnp.broadcast_to(facts[:, 6:7], (tall, LANES)).astype(jnp.int32)

        def segment(source_of, which, running, own=False):
            for chunk in range(s_dev // LANES):
                source = [jnp.broadcast_to(source_of(which, j, chunk), (tall, LANES)) for j in range(7)]
                rx, ry, rz = (source[j] - target[j] for j in range(3))
                ux, uy, uz = (source[j] - target[j] for j in range(3, 6))
                inverse = lax.rsqrt((rx * rx + ry * ry + rz * rz) + SOFTENING_SQ)
                inverse_sq = inverse * inverse
                weight3 = source[6] * inverse * inverse_sq
                if own:
                    weight3 = jnp.where(key == iota((tall, LANES), 1) + chunk * LANES, 0.0, weight3)
                closing = (rx * ux + ry * uy + rz * uz) * inverse_sq * weight3
                parts = (
                    rx * weight3, ry * weight3, rz * weight3,
                    ux * weight3, uy * weight3, uz * weight3,
                    rx * closing, ry * closing, rz * closing,
                )
                running = [a + b for a, b in zip(running, parts)]
            return running

        def both(step, running):
            running = segment(far_of, step, list(running))
            return tuple(segment(near_of, jnp.where(step < my_z, step, step + 1), running))

        zero = jnp.zeros((tall, LANES), jnp.float32)
        running = lax.fori_loop(0, n_z - 1, both, (zero,) * 9)
        running = segment(far_of, n_z - 1, list(running))
        running = segment(near_of, my_z, running, own=True)
        totals = [jnp.sum(r, axis=1, keepdims=True) for r in running]
        totals = totals[0:3] + [totals[3 + j] - 3.0 * totals[6 + j] for j in range(3)]
        lanes = iota((tall, LANES), 1)
        packed = jnp.zeros((tall, LANES), jnp.float32)
        for j in range(6):
            packed = jnp.where(lanes == j, jnp.broadcast_to(totals[j], (tall, LANES)), packed)
        sums[at, :] = packed

    tall_blocks = (count + 7) // 16
    pl.loop(0, tall_blocks)(lambda block: one_block(block * 16, 16))
    pl.when(count > tall_blocks * 16)(lambda: one_block(tall_blocks * 16, 8))
    for part in range(room // LANES):
        cut = slice(part * LANES, (part + 1) * LANES)
        rows = sums[cut, :].T[0:8]
        for copy in range(copies):
            force_out[copy, :, cut] = rows


def in_rows(ref):
    return lambda which, value, chunk: ref[which, value : value + 1, chunk * LANES : (chunk + 1) * LANES]


def in_chunks(ref, weight_ref):
    def source_of(which, value, chunk):
        if value == 6:
            return weight_ref[which, :, chunk * LANES : (chunk + 1) * LANES]
        return ref[which, chunk * 6 + value : chunk * 6 + value + 1, :]

    return source_of


def first_force_kernel(info, near, far, turned_in, force_out, near_weights, far_weights, sums):
    n_z, _, s_dev = near.shape
    near_weights[...] = near[:, 6:7, :]
    far_weights[...] = far[:, 6:7, :]
    force_sums(info[0], info[3], turned_in, in_rows(near), in_rows(far), s_dev, n_z, force_out, sums)


def second_force_kernel(info, near, far, near_weights, far_weights, turned_in, force_out, sums):
    n_z, _, s_dev = near_weights.shape
    near_of, far_of = in_chunks(near, near_weights), in_chunks(far, far_weights)
    force_sums(info[1], info[3], turned_in, near_of, far_of, s_dev, n_z, force_out, sums)


def summed(received):
    total = received[0]
    for row in range(1, received.shape[0]):
        total = total + received[row]
    return total


def placed(values, keys, old, room):
    s_dev = old.shape[1]
    outs, hits = [], []
    for chunk in range(s_dev // LANES):
        star = (iota((LANES, LANES), 1) + chunk * LANES).astype(jnp.float32)
        found = jnp.zeros((LANES, LANES), jnp.float32)
        for part in range(room // LANES):
            number = (iota((LANES, LANES), 0) + part * LANES + 1).astype(jnp.float32)
            found = found + jnp.where(keys[part] == star, number, 0.0)
        slot = jnp.sum(found, axis=0, keepdims=True).astype(jnp.int32) - 1
        new = picked_slots(values, slot, room)
        hit = slot >= 0
        hits.append(hit)
        outs.append(jnp.where(hit, new, old[:, chunk * LANES : (chunk + 1) * LANES]))
    return outs, hits


def picked_slots(values, slot, room):
    lane = jnp.broadcast_to(slot & (LANES - 1), (16, LANES))
    new = jnp.zeros((16, LANES), jnp.float32)
    for part in range(room // LANES):
        pick = lane_pick(values[:, part * LANES : (part + 1) * LANES], lane)
        new = jnp.where((slot >> log2_of(LANES)) == part, pick, new)
    return new


def correct_kernel(received, target, turned_in, old, row_out, own_out, second_out, turned_out):
    copies = row_out.shape[0]
    room = received.shape[2]
    forces = summed(received)
    states = target[0:12, :room]
    span = TIME_FIRST - target[12:13, :room]
    ahead, moving = predict(states, span)
    corrected = correct(ahead, moving, states[6:9], states[9:12], span, forces[0:6])
    corrected = jnp.concatenate([corrected, jnp.full((1, room), TIME_FIRST, jnp.float32), jnp.zeros((3, room), jnp.float32)], axis=0)
    columns = [turned_in[part * LANES : (part + 1) * LANES, :] for part in range(room // LANES)]
    keys = [jnp.broadcast_to(c[:, 6:7], (LANES, LANES)) for c in columns]
    numbers = [jnp.broadcast_to(c[:, 7:8], (LANES, LANES)) for c in columns]
    outs, _ = placed(corrected, keys, old[...], room)
    for chunk, states_new in enumerate(outs):
        cut = slice(chunk * LANES, (chunk + 1) * LANES)
        own_out[:, cut] = states_new
        ahead, moving = predict(states_new[0:12], TIME_SECOND - states_new[12:13])
        row = jnp.concatenate([ahead, moving], axis=0)
        for copy in range(copies):
            row_out[copy, 6 * chunk : 6 * chunk + 6, :] = row
    other = target[:, room : room + SECOND_ROOM]
    number = other[13:14]
    found = jnp.zeros((LANES, LANES), jnp.float32)
    for part in range(room // LANES):
        place = (iota((LANES, LANES), 0) + part * LANES + 1).astype(jnp.float32)
        found = found + jnp.where((numbers[part] == number) & (numbers[part] >= 0.0), place, 0.0)
    slot = jnp.sum(found, axis=0, keepdims=True).astype(jnp.int32) - 1
    states = jnp.where(slot >= 0, picked_slots(corrected, slot, room), other)
    span = TIME_SECOND - states[12:13]
    ahead, moving = predict(states[0:12], span)
    second_out[...] = rows_of([ahead, moving, states[6:12], span], 16)
    turned_out[...] = turned(rows_of([ahead, moving, other[14:15]], 8))


def finish_kernel(received, second, turned_in, own, pos_out, vel_out, acc_out, jerk_out):
    forces = summed(received)
    facts = second[...]
    corrected = correct(facts[0:3], facts[3:6], facts[6:9], facts[9:12], facts[12:13], forces[0:6])
    corrected = jnp.concatenate([corrected, jnp.zeros((4, SECOND_ROOM), jnp.float32)], axis=0)
    keys = [jnp.broadcast_to(turned_in[:, 6:7], (LANES, LANES))]
    outs, _ = placed(corrected, keys, own[...], SECOND_ROOM)
    for chunk, new in enumerate(outs):
        cut = slice(chunk * LANES, (chunk + 1) * LANES)
        pos_out[:, cut] = new[0:3]
        vel_out[:, cut] = new[3:6]
        acc_out[:, cut] = new[6:9]
        jerk_out[:, cut] = new[9:12]


def f32(*shape):
    return jax.ShapeDtypeStruct(shape, jnp.float32)


INTERPRET = False


def call(kernel, outs, scalars=0, operands=0, scratch=(), smem_out=None):
    smem, vmem = pl.BlockSpec(memory_space=pltpu.SMEM), pl.BlockSpec(memory_space=pltpu.VMEM)
    return pl.pallas_call(
        kernel,
        out_shape=outs,
        in_specs=[smem] * scalars + [vmem] * operands,
        out_specs=tuple(smem if i == smem_out else vmem for i in range(len(outs))),
        scratch_shapes=list(scratch),
        interpret=INTERPRET,
    )


def exchanged(copies, axis):
    return lax.all_to_all(copies, axis, split_axis=0, concat_axis=0, tiled=True)


def other_core(near):
    return lax.ppermute(near, "core", [(0, 1), (1, 0)])


def shards(positions, velocities, accels, jerks, masses, levels, active_first, active_second):
    s_dev = positions.shape[1]
    n_tgt, n_z, n_src = lax.axis_size("tgt"), lax.axis_size("z"), lax.axis_size(SRC)
    n_stars = s_dev * n_tgt * n_src
    column_copies, row_copies, own = call(
        functools.partial(prepare_kernel, n_stars), (f32(n_tgt, 16, s_dev), f32(n_z, 8, s_dev), f32(16, s_dev)), 0, 8
    )(
        positions, velocities, accels, jerks, masses.reshape(1, s_dev), levels.reshape(1, s_dev),
        active_first.reshape(1, -1), active_second.reshape(1, -1),
    )
    near = exchanged(row_copies, "z")
    column = exchanged(column_copies, "tgt")
    far = other_core(near)
    all_room = FIRST_ROOM + SECOND_ROOM
    target, columns, info = call(
        functools.partial(select_kernel, n_src, active_first.shape[0], active_second.shape[0]),
        (f32(16, all_room), f32(all_room, LANES), jax.ShapeDtypeStruct((4,), jnp.int32)), 0, 1, smem_out=2,
    )(column)

    def by_columns(near_first, far_first, target, columns, info, own, *inputs):
        partial, near_weights, far_weights = call(
            first_force_kernel, (f32(n_tgt, 8, FIRST_ROOM), f32(n_z, 1, s_dev), f32(n_z, 1, s_dev)), 1, 3, [pltpu.VMEM((FIRST_ROOM, LANES), jnp.float32)]
        )(info, near_first, far_first, columns)
        received = exchanged(partial, "tgt")
        row_copies, own, second, second_columns = call(
            correct_kernel,
            (f32(n_z, 6 * s_dev // LANES, LANES), f32(16, s_dev), f32(16, SECOND_ROOM), f32(LANES, LANES)),
            0, 4,
        )(received, target, columns, own)
        near = exchanged(row_copies, "z")
        far = other_core(near)
        (partial,) = call(
            second_force_kernel, (f32(n_tgt, 8, SECOND_ROOM),), 1, 5, [pltpu.VMEM((SECOND_ROOM, LANES), jnp.float32)]
        )(info, near, far, near_weights, far_weights, second_columns)
        received = exchanged(partial, "tgt")
        return tuple(call(finish_kernel, (f32(3, s_dev),) * 4, 0, 4)(received, second, second_columns, own))

    def anywhere(near_first, far_first, target, columns, info, own, *inputs):
        return whole_program(*inputs)

    inputs = (positions, velocities, accels, jerks, masses, levels, active_first, active_second)
    return lax.cond(info[2] == 1, by_columns, anywhere, near, far, target, columns, info, own, *inputs)


def solution(mesh):
    n_tgt, n_src = mesh.devices.shape
    finer = Mesh(mesh.devices.reshape(n_tgt, n_src // 2, 2), ("tgt", "z", "core"))
    stars = ("tgt", "z", "core")
    vector, scalar = P(None, stars), P(stars)
    return jax.shard_map(
        shards,
        mesh=finer,
        in_specs=(vector, vector, vector, vector, scalar, scalar, P("tgt"), P("tgt")),
        out_specs=(vector,) * 4,
        check_vma=False,
    )
```

```python
import functools

import jax
import jax.numpy as jnp
from jax import lax
from jax.experimental import pallas as pl
from jax.experimental.pallas import tpu as pltpu
from jax.sharding import Mesh
from jax.sharding import PartitionSpec as P

TILE = 128
LEVELS = 4
LANES = 128
FIRST_ROOM = 256
SECOND_ROOM = 128
OWN_ROOM = 32

SOFTENING_SQ = 0.0001
BASE_STEP = 0.5
TIME_FIRST = 0.0
TIME_SECOND = BASE_STEP / (1 << LEVELS)
SRC = ("z", "core")


def sent_to_all(shard, axis):
    copies = jnp.broadcast_to(shard, (lax.axis_size(axis), *shard.shape))
    return lax.all_to_all(copies, axis, split_axis=0, concat_axis=0, tiled=True)


def laid_out(tiles, dim):
    dims = list(tiles.shape[1:])
    dims[dim] *= tiles.shape[0]
    return jnp.moveaxis(tiles, 0, dim).reshape(dims)


def gathered_copies(shard, axis, dim):
    tiles = sent_to_all(shard, axis)
    return laid_out(tiles, dim)


def over_pieces(shard, axis):
    return lax.all_gather(shard, axis).sum(0)


def taken_together(shard, axis):
    return sent_to_all(shard, axis).sum(axis=0)


def predict(states, span):
    ahead_pos = states[0:3] + span * (
        states[3:6] + span * (states[6:9] * 0.5 + span * states[9:12] / 6.0)
    )
    moving = states[3:6] + span * (states[6:9] + span * states[9:12] * 0.5)
    return (ahead_pos, moving)


def pair_block(tile_place, tile_speed, tile_ident, sources, source_ident):
    offset = sources[0:3, None, :] - tile_place[:, :, None]
    motion = sources[3:6, None, :] - tile_speed[:, :, None]
    dist_sq = jnp.sum(offset * offset, axis=0) + SOFTENING_SQ
    inverse = lax.rsqrt(dist_sq)
    inverse_sq = inverse * inverse
    weight3 = jnp.where(
        source_ident[None, :] == tile_ident[:, None],
        0.0,
        sources[6][None, :] * inverse_sq * inverse,
    )
    closing = jnp.sum(offset * motion, axis=0)
    attract = jnp.sum(offset * weight3, axis=2)
    change = jnp.sum(motion * weight3 - 3.0 * (closing * inverse_sq * weight3) * offset, axis=2)
    return jnp.concatenate([attract, change], axis=0)


def correct(ahead_pos, moving, old_accel, old_jolt, span, forces):
    new_acc = forces[0:3]
    new_jolt = forces[3:6]
    second_term = -6.0 * (old_accel - new_acc) - span * (4.0 * old_jolt + 2.0 * new_jolt)
    third_term = 12.0 * (old_accel - new_acc) + 6.0 * span * (old_jolt + new_jolt)
    new_place = ahead_pos + span * span * (second_term / 24.0 + third_term / 120.0)
    new_speed = moving + span * (second_term / 6.0 + third_term / 24.0)
    return jnp.concatenate([new_place, new_speed, new_acc, new_jolt], axis=0)


def tile_forces(held, tgt_ahead, tgt_moving, slot_ids, tiles_used, shard_part, idents):
    length = shard_part.shape[1]
    block_len = length
    while block_len > 2048 and block_len % 2 == 0:
        block_len = block_len // 2
    block_count = length // block_len
    src_blocks = shard_part.reshape(7, block_count, block_len).transpose(1, 0, 2)
    ident_blocks = idents.reshape(block_count, block_len)

    def one_tile(tile_no, carried):
        place_tile = lax.dynamic_slice_in_dim(tgt_ahead, tile_no * TILE, TILE, 1)
        speed_tile = lax.dynamic_slice_in_dim(tgt_moving, tile_no * TILE, TILE, 1)
        ident_tile = lax.dynamic_slice_in_dim(slot_ids, tile_no * TILE, TILE, 0)

        def add_block(running, source_pair):
            return (
                running
                + pair_block(place_tile, speed_tile, ident_tile, source_pair[0], source_pair[1]),
                None,
            )

        running, _ = lax.scan(
            add_block, jnp.zeros((6, TILE), jnp.float32), (src_blocks, ident_blocks)
        )
        before = lax.dynamic_slice_in_dim(carried, tile_no * TILE, TILE, 1)
        return lax.dynamic_update_slice_in_dim(carried, before + running, tile_no * TILE, 1)

    return lax.fori_loop(0, tiles_used, one_tile, held)


def advance(states, last_time, weights, active, now_time, s_dev, n_tgt, n_src, my_row, my_column):
    slot_count = active.shape[0]
    own_first = (my_row * n_src + my_column) * s_dev
    listed = gathered_copies(active, "tgt", 0)
    span_all = now_time - last_time
    my_slots = lax.dynamic_slice_in_dim(listed, my_row * slot_count, slot_count, 0)
    filled = jnp.sum((my_slots >= 0).astype(jnp.int32))
    tiles_used = (filled + TILE - 1) // TILE
    local_at = listed - own_first
    is_owned = (listed >= 0) & (local_at >= 0) & (local_at < s_dev)
    stacked = jnp.concatenate([states, span_all[None, :], weights[None, :]], axis=0)
    column_all = gathered_copies(stacked, "tgt", 1)
    owner_col = my_slots // s_dev % n_src
    places = my_slots // (s_dev * n_src) * s_dev + my_slots % s_dev
    mine_owned = (my_slots >= 0) & (owner_col == my_column)
    chosen = jnp.take(column_all[0:13], jnp.clip(places, 0, n_tgt * s_dev - 1), axis=1)
    partial_rows = jnp.where(mine_owned[None, :], chosen, 0.0)
    ahead_pos, moving = predict(column_all[0:12], column_all[12:13])
    sources = jnp.concatenate([ahead_pos, moving, column_all[13:14]], axis=0)
    target = over_pieces(partial_rows, SRC)
    tgt_ahead, tgt_moving = predict(target[0:12], target[12:13])
    zero_forces = jnp.zeros((6, slot_count), jnp.float32)
    columns = jnp.arange(sources.shape[1], dtype=jnp.int32)
    idents = columns // s_dev * (s_dev * n_src) + my_column * s_dev + columns % s_dev
    partial_forces = tile_forces(
        zero_forces, tgt_ahead, tgt_moving, my_slots, tiles_used, sources, idents
    )
    forces = taken_together(partial_forces, SRC)
    corrected = correct(tgt_ahead, tgt_moving, target[6:9], target[9:12], target[12:13], forces)
    returned = gathered_copies(corrected, "tgt", 1)
    write_at = jnp.where(is_owned, local_at, s_dev)
    states = states.at[:, write_at].set(returned, mode="drop")
    last_time = last_time.at[write_at].set(now_time, mode="drop")
    return (states, last_time)


def whole_program(positions, velocities, accels, jerks, masses, levels, active_first, active_second):
    s_dev = positions.shape[1]
    n_tgt = lax.axis_size("tgt")
    n_src = lax.axis_size(SRC)
    my_row = lax.axis_index("tgt")
    my_column = lax.axis_index(SRC)
    weights = masses / (s_dev * n_tgt * n_src)
    states = jnp.concatenate([positions, velocities, accels, jerks], axis=0)
    last_time = -BASE_STEP * jnp.exp2(-levels.astype(jnp.float32))
    for now_time, active in ((TIME_FIRST, active_first), (TIME_SECOND, active_second)):
        states, last_time = advance(
            states, last_time, weights, active, now_time, s_dev, n_tgt, n_src, my_row, my_column
        )
    return (states[0:3], states[3:6], states[6:9], states[9:12])


def log2_of(size):
    assert size & (size - 1) == 0, "size"
    return size.bit_length() - 1


def iota(shape, dim):
    return lax.broadcasted_iota(jnp.int32, shape, dim)


def lane_pick(table, lanes):
    return lax.gather(
        table,
        lanes[:, :, None],
        lax.GatherDimensionNumbers(
            offset_dims=(),
            collapsed_slice_dims=(1,),
            start_index_map=(1,),
            operand_batching_dims=(0,),
            start_indices_batching_dims=(0,),
        ),
        slice_sizes=(1, 1),
        mode=lax.GatherScatterMode.PROMISE_IN_BOUNDS,
    )


def turned(rows):
    pad = jnp.zeros((LANES - rows.shape[0], LANES), rows.dtype)
    return jnp.concatenate([rows, pad], axis=0).T


def rows_of(values, count):
    width = values[0].shape[1]
    below = count - sum(v.shape[0] for v in values)
    pad = [jnp.zeros((below, width), jnp.float32)] if below else []
    return jnp.concatenate(list(values) + pad, axis=0)


def prepare_kernel(n_stars, pos, vel, acc, jerk, mass, levels, first, second, column_out, row_out, own_out):
    s_dev = pos.shape[1]
    last = -BASE_STEP * jnp.exp2(-levels[...].astype(jnp.float32))
    states = jnp.concatenate([pos[...], vel[...], acc[...], jerk[...]], axis=0)
    weights = mass[...] / n_stars
    room = first.shape[1] + second.shape[1]
    lists = [first[...].astype(jnp.float32), second[...].astype(jnp.float32)]
    if s_dev > room:
        lists.append(jnp.full((1, s_dev - room), -1.0, jnp.float32))
    listed = jnp.concatenate(lists, axis=1)
    column = rows_of([states, last, listed, weights], 16)
    for copy in range(column_out.shape[0]):
        column_out[copy] = column
    ahead, moving = predict(states, TIME_FIRST - last)
    ahead_second, moving_second = predict(states, TIME_SECOND - last)
    row_out[...] = jnp.concatenate([ahead, moving, weights, ahead_second, moving_second], axis=0)
    own_out[...] = rows_of([states, last, weights], 16)


def matching_slots(listed, column, n_src, s_dev):
    ids = listed.astype(jnp.int32)
    n_tgt, width = ids.shape
    valid = ids >= 0
    column_of = jnp.where(valid, (ids >> log2_of(s_dev)) & (n_src - 1), -1)
    row_of = jnp.where(valid, ids >> log2_of(s_dev * n_src), -1)
    cells = jnp.zeros((n_tgt, n_src), jnp.float32)
    for slots in range(n_tgt):
        in_row = (row_of[slots : slots + 1] == iota((n_tgt, width), 0)).astype(jnp.bfloat16)
        in_column = (column_of[slots : slots + 1] == iota((n_src, width), 0)).astype(jnp.bfloat16)
        cells = cells + lax.dot_general(
            in_row, in_column, (((1,), (1,)), ((), ())), preferred_element_type=jnp.float32
        )
    return column_of == column, jnp.max(jnp.sum(cells, axis=0, keepdims=True)), jnp.max(cells)


def slot_numbers(mine):
    n_rows, width = mine.shape
    upto = (iota((width, width), 0) <= iota((width, width), 1)).astype(jnp.bfloat16)
    inside = jnp.dot(mine.astype(jnp.bfloat16), upto, preferred_element_type=jnp.float32)
    totals = jnp.broadcast_to(inside[:, width - 1 : width], (n_rows, LANES))
    place = jnp.zeros((1, LANES), jnp.float32)
    before = []
    for row in range(n_rows):
        before.append(place)
        place = place + totals[row : row + 1]
    start = jnp.concatenate(before, axis=0)[:, 0:1]
    return jnp.where(mine, (inside + start).astype(jnp.int32) - 1, -1), jnp.max(place)


def packed_ids(listed, slot, part):
    n_rows, width = listed.shape
    found = jnp.zeros((LANES, LANES), jnp.float32)
    want = iota((LANES, LANES), 0) + part * LANES
    for row in range(n_rows):
        for chunk in range(width // LANES):
            cut = slice(chunk * LANES, (chunk + 1) * LANES)
            hit = jnp.broadcast_to(slot[row : row + 1, cut], (LANES, LANES)) == want
            found = found + jnp.where(hit, listed[row : row + 1, cut] + 1.0, 0.0)
    ids = jnp.broadcast_to(jnp.sum(found, axis=1, keepdims=True) - 1.0, (LANES, LANES))
    return ids.T[0:1]


def target_facts(number, held, my_row, n_src):
    n_tgt, _, s_dev = held.shape
    row_bits, per_row = log2_of(s_dev * n_src), s_dev // LANES
    ids = number.astype(jnp.int32)
    lane = jnp.broadcast_to(ids & (LANES - 1), (16, LANES))
    chunk_of = jnp.where(ids >= 0, (ids >> row_bits) * per_row + ((ids & (s_dev - 1)) >> log2_of(LANES)), -1)

    def one_row(row, picked):
        for chunk in range(per_row):
            table = held[row, :, chunk * LANES : (chunk + 1) * LANES]
            picked = jnp.where(chunk_of == row * per_row + chunk, lane_pick(table, lane), picked)
        return picked

    picked = lax.fori_loop(0, n_tgt, one_row, jnp.zeros((16, LANES), jnp.float32), unroll=2)
    key = jnp.where((ids >= 0) & ((ids >> row_bits) == my_row), ids & (s_dev - 1), -1)
    return rows_of([picked[0:13], number, picked[14:15], key.astype(jnp.float32)], 16)


def select_kernel(n_src, slots_first, slots_second, held, target_out, turned_out, info_out):
    s_dev = held.shape[2]
    my_row, my_column = lax.axis_index("tgt"), lax.axis_index(SRC)
    listed = held[:, 13, :]
    first, second = listed[:, :slots_first], listed[:, slots_first : slots_first + slots_second]
    mine, most_first, most_own = matching_slots(first, my_column, n_src, s_dev)
    _, most_second, _ = matching_slots(second, my_column, n_src, s_dev)
    slot, count = slot_numbers(mine)
    count = count.astype(jnp.int32)
    info_out[0] = count
    fits = (most_first <= FIRST_ROOM) & (most_second <= SECOND_ROOM) & (most_own <= OWN_ROOM)
    info_out[1] = fits.astype(jnp.int32)

    def fill(part):
        facts = target_facts(packed_ids(first, slot, part), held, my_row, n_src)
        ahead, moving = predict(facts[0:12], TIME_FIRST - facts[12:13])
        cut = slice(part * LANES, (part + 1) * LANES)
        target_out[:, cut] = facts
        turned_out[cut, :] = turned(rows_of([ahead, moving, facts[15:16], facts[13:14]], 8))

    fill(0)
    for part in range(1, FIRST_ROOM // LANES):
        pl.when(count > part * LANES)(functools.partial(fill, part))

        @pl.when(count <= part * LANES)
        def _():
            cut = slice(part * LANES, (part + 1) * LANES)
            target_out[:, cut] = jnp.full((16, LANES), -1.0, jnp.float32)
            turned_out[cut, :] = jnp.full((LANES, LANES), -1.0, jnp.float32)


def found_slots(keys, wanted):
    found = jnp.zeros((LANES, LANES), jnp.float32)
    for part, key in enumerate(keys):
        place = (iota((LANES, LANES), 0) + part * LANES + 1).astype(jnp.float32)
        found = found + jnp.where((key == wanted) & (key >= 0.0), place, 0.0)
    return jnp.sum(found, axis=0, keepdims=True).astype(jnp.int32) - 1


def plan_kernel(n_src, slots_first, slots_second, held, first_target, turned_in, second_out, plan_out, info_out):
    s_dev = held.shape[2]
    my_row, my_column = lax.axis_index("tgt"), lax.axis_index(SRC)
    listed = held[:, 13, slots_first : slots_first + slots_second]
    ids = listed.astype(jnp.int32)
    mine = (ids >= 0) & (((ids >> log2_of(s_dev)) & (n_src - 1)) == my_column)
    slot, count = slot_numbers(mine)
    info_out[0] = count.astype(jnp.int32)
    facts = target_facts(packed_ids(listed, slot, 0), held, my_row, n_src)
    second_out[...] = facts
    parts = FIRST_ROOM // LANES
    columns = [turned_in[part * LANES : (part + 1) * LANES, :] for part in range(parts)]
    keys = [jnp.broadcast_to(c[:, 6:7], (LANES, LANES)) for c in columns]
    numbers = [jnp.broadcast_to(c[:, 7:8], (LANES, LANES)) for c in columns]
    second_keys = [jnp.broadcast_to(facts[15:16], (LANES, LANES)).T]
    plan_out[...] = jnp.full(plan_out.shape, -1, jnp.int32)
    for chunk in range(s_dev // LANES):
        cut = slice(chunk * LANES, (chunk + 1) * LANES)
        star = (iota((1, LANES), 1) + chunk * LANES).astype(jnp.float32)
        plan_out[0:1, cut] = found_slots(keys, star)
        plan_out[1:2, cut] = found_slots(second_keys, star)
    plan_out[2:3, 0:LANES] = found_slots(numbers, facts[13:14])
    own = [(key >= 0.0) for key in keys]
    upto = (iota((LANES, LANES), 1) <= iota((LANES, LANES), 0)).astype(jnp.bfloat16)
    before = jnp.zeros((1, LANES), jnp.float32)
    order = []
    for flags in own:
        inside = jnp.dot(upto, flags.astype(jnp.bfloat16), preferred_element_type=jnp.float32) + before
        order.append(jnp.where(flags, inside - 1.0, -1.0))
        before = inside[LANES - 1 : LANES]
    plan_out[3:4, 0:LANES] = found_slots(order, iota((1, LANES), 1).astype(jnp.float32))


def pair_terms(source, target, own_place=None, key=None):
    rx, ry, rz = (source[j] - target[j] for j in range(3))
    ux, uy, uz = (source[j] - target[j] for j in range(3, 6))
    inverse = lax.rsqrt((rx * rx + ry * ry + rz * rz) + SOFTENING_SQ)
    inverse_sq = inverse * inverse
    weight3 = source[6] * inverse * inverse_sq
    if own_place is not None:
        weight3 = jnp.where(key == own_place, 0.0, weight3)
    closing = (rx * ux + ry * uy + rz * uz) * inverse_sq * weight3
    return (
        rx * weight3, ry * weight3, rz * weight3,
        ux * weight3, uy * weight3, uz * weight3,
        rx * closing, ry * closing, rz * closing,
    )


def added(running, parts):
    return tuple(a + b for a, b in zip(running, parts))


def target_blocks(count, turned_in, sums, visit):
    def one_block(first, tall):
        at = pl.ds(pl.multiple_of(first, 8), tall)
        facts = turned_in[at, :]
        target = [jnp.broadcast_to(facts[:, j : j + 1], (tall, LANES)) for j in range(6)]
        key = jnp.broadcast_to(facts[:, 6:7], (tall, LANES))
        running = visit(tall, target, key, (jnp.zeros((tall, LANES), jnp.float32),) * 9)
        totals = [running[j] for j in range(3)] + [running[3 + j] - 3.0 * running[6 + j] for j in range(3)]
        lanes = iota((tall, LANES), 1)
        packed = sums[at, :]
        for j in range(6):
            total = jnp.broadcast_to(jnp.sum(totals[j], axis=1, keepdims=True), (tall, LANES))
            packed = packed + jnp.where(lanes == j, total, 0.0)
        sums[at, :] = packed

    tall_blocks = (count + 7) // 16
    pl.loop(0, tall_blocks)(lambda block: one_block(block * 16, 16))
    pl.when(count > tall_blocks * 16)(lambda: one_block(tall_blocks * 16, 8))


def row_sums(count, stars, first_row, turned_in, sums):
    n_src, _, s_dev = stars.shape
    my_column = lax.axis_index(SRC)
    rows = [first_row + j for j in range(6)] + [6]
    sums[...] = jnp.zeros_like(sums)

    def visit(tall, target, key, running):
        def segment(which, running, own):
            for chunk in range(s_dev // LANES):
                cut = slice(chunk * LANES, (chunk + 1) * LANES)
                source = [jnp.broadcast_to(stars[which, j : j + 1, cut], (tall, LANES)) for j in rows]
                place = (iota((tall, LANES), 1) + chunk * LANES).astype(jnp.float32) if own else None
                running = added(running, pair_terms(source, target, place, key))
            return running

        running = lax.fori_loop(0, my_column, lambda which, r: segment(which, r, False), running)
        running = segment(my_column, running, True)
        return lax.fori_loop(my_column + 1, n_src, lambda which, r: segment(which, r, False), running)

    target_blocks(count, turned_in, sums, visit)


def write_sums(sums, force_out):
    copies, _, room = force_out.shape
    for part in range(room // LANES):
        cut = slice(part * LANES, (part + 1) * LANES)
        rows = sums[cut, :].T[0:8]
        for copy in range(copies):
            force_out[copy, :, cut] = rows


def first_force_kernel(info, stars, turned_in, force_out, sums):
    row_sums(info[0], stars, 0, turned_in, sums)
    write_sums(sums, force_out)


def second_force_kernel(info, stars, turned_in, sums_out):
    row_sums(info[0], stars, 7, turned_in, sums_out)


def update_force_kernel(info, near, far, turned_in, sums_in, force_out, sums, stars):
    n_z = near.shape[0]
    my_z = lax.axis_index("z")
    half = iota((8, LANES), 1) < LANES // 2
    for z in range(n_z):
        both = jnp.where(half, near[z], pltpu.roll(far[z], LANES // 2, axis=1))
        place = jnp.where(half[7:8] & (my_z == z), both[7:8], -2.0)
        stars[z] = jnp.concatenate([both[0:7], place], axis=0)
    sums[...] = sums_in[...]

    def visit(tall, target, key, running):
        def one(z, running):
            source = [jnp.broadcast_to(stars[z, j : j + 1, :], (tall, LANES)) for j in range(8)]
            return added(running, pair_terms(source, target, source[7], key))

        return lax.fori_loop(0, n_z, one, running, unroll=4)

    target_blocks(info[0], turned_in, sums, visit)
    write_sums(sums, force_out)


def summed(received):
    total = received[0]
    for row in range(1, received.shape[0]):
        total = total + received[row]
    return total


def picked_slots(values, slot):
    lane = jnp.broadcast_to(slot & (LANES - 1), (16, LANES))
    new = jnp.zeros((16, LANES), jnp.float32)
    for part in range(values.shape[1] // LANES):
        pick = lane_pick(values[:, part * LANES : (part + 1) * LANES], lane)
        new = jnp.where((slot >> log2_of(LANES)) == part, pick, new)
    return new


def correct_kernel(received, target, second, plan, own, update_out, own_out, second_out, turned_out):
    copies = update_out.shape[0]
    room = received.shape[2]
    s_dev = own.shape[1]
    forces = summed(received)
    states = target[0:12, :]
    span = TIME_FIRST - target[12:13, :]
    ahead, moving = predict(states, span)
    corrected = correct(ahead, moving, states[6:9], states[9:12], span, forces[0:6])
    corrected = rows_of([corrected, jnp.full((1, room), TIME_FIRST, jnp.float32)], 16)
    slot = plan[3:4, 0:LANES]
    old = picked_slots(target[...], slot)
    new = picked_slots(corrected, slot)
    present = slot >= 0
    weight, place = old[14:15], jnp.where(present, old[15:16], -1.0)
    ahead_new, moving_new = predict(new[0:12], TIME_SECOND - new[12:13])
    ahead_old, moving_old = predict(old[0:12], TIME_SECOND - old[12:13])
    arrived = jnp.concatenate([ahead_new, moving_new, weight, place], axis=0)
    left = jnp.concatenate([ahead_old, moving_old, -weight, place], axis=0)
    lane = iota((8, LANES), 1)
    update = jnp.where(lane < OWN_ROOM, arrived, pltpu.roll(left, OWN_ROOM, axis=1))
    update = jnp.where(lane < 2 * OWN_ROOM, update, 0.0)
    for copy in range(copies):
        update_out[copy] = update
    for chunk in range(s_dev // LANES):
        cut = slice(chunk * LANES, (chunk + 1) * LANES)
        slot = plan[0:1, cut]
        own_out[:, cut] = jnp.where(slot >= 0, picked_slots(corrected, slot), own[:, cut])
    other = second[...]
    slot = plan[2:3, 0:LANES]
    states = jnp.where(slot >= 0, picked_slots(corrected, slot), other)
    span = TIME_SECOND - states[12:13]
    ahead, moving = predict(states[0:12], span)
    second_out[...] = rows_of([ahead, moving, states[6:12], span], 16)
    turned_out[...] = turned(rows_of([ahead, moving, other[15:16]], 8))


def finish_kernel(received, second, plan, own, pos_out, vel_out, acc_out, jerk_out):
    forces = summed(received)
    facts = second[...]
    corrected = correct(facts[0:3], facts[3:6], facts[6:9], facts[9:12], facts[12:13], forces[0:6])
    corrected = rows_of([corrected], 16)
    for chunk in range(own.shape[1] // LANES):
        cut = slice(chunk * LANES, (chunk + 1) * LANES)
        slot = plan[1:2, cut]
        new = jnp.where(slot >= 0, picked_slots(corrected, slot), own[:, cut])
        pos_out[:, cut] = new[0:3]
        vel_out[:, cut] = new[3:6]
        acc_out[:, cut] = new[6:9]
        jerk_out[:, cut] = new[9:12]


def f32(*shape):
    return jax.ShapeDtypeStruct(shape, jnp.float32)


INTERPRET = False


def call(kernel, outs, scalars=0, operands=0, scratch=(), smem_out=None):
    smem, vmem = pl.BlockSpec(memory_space=pltpu.SMEM), pl.BlockSpec(memory_space=pltpu.VMEM)
    return pl.pallas_call(
        kernel,
        out_shape=outs,
        in_specs=[smem] * scalars + [vmem] * operands,
        out_specs=tuple(smem if i == smem_out else vmem for i in range(len(outs))),
        scratch_shapes=list(scratch),
        interpret=INTERPRET,
    )


def exchanged(copies, axis):
    return lax.all_to_all(copies, axis, split_axis=0, concat_axis=0, tiled=True)


def other_core(near):
    return lax.ppermute(near, "core", [(0, 1), (1, 0)])


def shards(positions, velocities, accels, jerks, masses, levels, active_first, active_second):
    s_dev = positions.shape[1]
    n_tgt, n_z, n_src = lax.axis_size("tgt"), lax.axis_size("z"), lax.axis_size(SRC)
    n_stars = s_dev * n_tgt * n_src
    scalar = jax.ShapeDtypeStruct((2,), jnp.int32)
    lists = (n_src, active_first.shape[0], active_second.shape[0])
    column_copies, row, own = call(
        functools.partial(prepare_kernel, n_stars), (f32(n_tgt, 16, s_dev), f32(13, s_dev), f32(16, s_dev)), 0, 8
    )(
        positions, velocities, accels, jerks, masses.reshape(1, s_dev), levels.reshape(1, s_dev),
        active_first.reshape(1, -1), active_second.reshape(1, -1),
    )
    column = exchanged(column_copies, "tgt")
    stars = lax.all_gather(row, SRC)
    target, columns, info = call(
        functools.partial(select_kernel, *lists), (f32(16, FIRST_ROOM), f32(FIRST_ROOM, LANES), scalar), 0, 1, smem_out=2
    )(column)

    def by_columns(stars, column, target, columns, info, own, *inputs):
        (partial,) = call(
            first_force_kernel, (f32(n_tgt, 8, FIRST_ROOM),), 1, 2, [pltpu.VMEM((FIRST_ROOM, LANES), jnp.float32)]
        )(info, stars, columns)
        received = exchanged(partial, "tgt")
        second, plan, second_info = call(
            functools.partial(plan_kernel, *lists),
            (f32(16, SECOND_ROOM), jax.ShapeDtypeStruct((8, s_dev), jnp.int32), scalar), 0, 3, smem_out=2,
        )(column, target, columns)
        update, own, second, second_columns = call(
            correct_kernel, (f32(n_z, 8, LANES), f32(16, s_dev), f32(16, SECOND_ROOM), f32(LANES, LANES)), 0, 5
        )(received, target, second, plan, own)
        near = exchanged(update, "z")
        (sums,) = call(second_force_kernel, (f32(SECOND_ROOM, LANES),), 1, 2)(second_info, stars, second_columns)
        far = other_core(near)
        (partial,) = call(
            update_force_kernel, (f32(n_tgt, 8, SECOND_ROOM),), 1, 4,
            [pltpu.VMEM((SECOND_ROOM, LANES), jnp.float32), pltpu.VMEM((n_z, 8, LANES), jnp.float32)],
        )(second_info, near, far, second_columns, sums)
        received = exchanged(partial, "tgt")
        return tuple(call(finish_kernel, (f32(3, s_dev),) * 4, 0, 4)(received, second, plan, own))

    def anywhere(stars, column, target, columns, info, own, *inputs):
        return whole_program(*inputs)

    inputs = (positions, velocities, accels, jerks, masses, levels, active_first, active_second)
    return lax.cond(info[1] == 1, by_columns, anywhere, stars, column, target, columns, info, own, *inputs)


def solution(mesh):
    n_tgt, n_src = mesh.devices.shape
    finer = Mesh(mesh.devices.reshape(n_tgt, n_src // 2, 2), ("tgt", "z", "core"))
    stars = ("tgt", "z", "core")
    vector, scalar = P(None, stars), P(stars)
    return jax.shard_map(
        shards,
        mesh=finer,
        in_specs=(vector, vector, vector, vector, scalar, scalar, P("tgt"), P("tgt")),
        out_specs=(vector,) * 4,
        check_vma=False,
    )
```

```python
import functools

import jax
import jax.numpy as jnp
from jax import lax
from jax.experimental import pallas as pl
from jax.experimental.pallas import tpu as pltpu
from jax.sharding import Mesh
from jax.sharding import PartitionSpec as P

TILE = 128
LEVELS = 4
LANES = 128
FIRST_ROOM = 256
SECOND_ROOM = 128
OWN_ROOM = 32

SOFTENING_SQ = 0.0001
BASE_STEP = 0.5
TIME_FIRST = 0.0
TIME_SECOND = BASE_STEP / (1 << LEVELS)
SRC = ("z", "core")


def sent_to_all(shard, axis):
    copies = jnp.broadcast_to(shard, (lax.axis_size(axis), *shard.shape))
    return lax.all_to_all(copies, axis, split_axis=0, concat_axis=0, tiled=True)


def laid_out(tiles, dim):
    dims = list(tiles.shape[1:])
    dims[dim] *= tiles.shape[0]
    return jnp.moveaxis(tiles, 0, dim).reshape(dims)


def gathered_copies(shard, axis, dim):
    tiles = sent_to_all(shard, axis)
    return laid_out(tiles, dim)


def over_pieces(shard, axis):
    return lax.all_gather(shard, axis).sum(0)


def taken_together(shard, axis):
    return sent_to_all(shard, axis).sum(axis=0)


def predict(states, span):
    ahead_pos = states[0:3] + span * (
        states[3:6] + span * (states[6:9] * 0.5 + span * states[9:12] / 6.0)
    )
    moving = states[3:6] + span * (states[6:9] + span * states[9:12] * 0.5)
    return (ahead_pos, moving)


def pair_block(tile_place, tile_speed, tile_ident, sources, source_ident):
    offset = sources[0:3, None, :] - tile_place[:, :, None]
    motion = sources[3:6, None, :] - tile_speed[:, :, None]
    dist_sq = jnp.sum(offset * offset, axis=0) + SOFTENING_SQ
    inverse = lax.rsqrt(dist_sq)
    inverse_sq = inverse * inverse
    weight3 = jnp.where(
        source_ident[None, :] == tile_ident[:, None],
        0.0,
        sources[6][None, :] * inverse_sq * inverse,
    )
    closing = jnp.sum(offset * motion, axis=0)
    attract = jnp.sum(offset * weight3, axis=2)
    change = jnp.sum(motion * weight3 - 3.0 * (closing * inverse_sq * weight3) * offset, axis=2)
    return jnp.concatenate([attract, change], axis=0)


def correct(ahead_pos, moving, old_accel, old_jolt, span, forces):
    new_acc = forces[0:3]
    new_jolt = forces[3:6]
    second_term = -6.0 * (old_accel - new_acc) - span * (4.0 * old_jolt + 2.0 * new_jolt)
    third_term = 12.0 * (old_accel - new_acc) + 6.0 * span * (old_jolt + new_jolt)
    new_place = ahead_pos + span * span * (second_term / 24.0 + third_term / 120.0)
    new_speed = moving + span * (second_term / 6.0 + third_term / 24.0)
    return jnp.concatenate([new_place, new_speed, new_acc, new_jolt], axis=0)


def tile_forces(held, tgt_ahead, tgt_moving, slot_ids, tiles_used, shard_part, idents):
    length = shard_part.shape[1]
    block_len = length
    while block_len > 2048 and block_len % 2 == 0:
        block_len = block_len // 2
    block_count = length // block_len
    src_blocks = shard_part.reshape(7, block_count, block_len).transpose(1, 0, 2)
    ident_blocks = idents.reshape(block_count, block_len)

    def one_tile(tile_no, carried):
        place_tile = lax.dynamic_slice_in_dim(tgt_ahead, tile_no * TILE, TILE, 1)
        speed_tile = lax.dynamic_slice_in_dim(tgt_moving, tile_no * TILE, TILE, 1)
        ident_tile = lax.dynamic_slice_in_dim(slot_ids, tile_no * TILE, TILE, 0)

        def add_block(running, source_pair):
            return (
                running
                + pair_block(place_tile, speed_tile, ident_tile, source_pair[0], source_pair[1]),
                None,
            )

        running, _ = lax.scan(
            add_block, jnp.zeros((6, TILE), jnp.float32), (src_blocks, ident_blocks)
        )
        before = lax.dynamic_slice_in_dim(carried, tile_no * TILE, TILE, 1)
        return lax.dynamic_update_slice_in_dim(carried, before + running, tile_no * TILE, 1)

    return lax.fori_loop(0, tiles_used, one_tile, held)


def advance(states, last_time, weights, active, now_time, s_dev, n_tgt, n_src, my_row, my_column):
    slot_count = active.shape[0]
    own_first = (my_row * n_src + my_column) * s_dev
    listed = gathered_copies(active, "tgt", 0)
    span_all = now_time - last_time
    my_slots = lax.dynamic_slice_in_dim(listed, my_row * slot_count, slot_count, 0)
    filled = jnp.sum((my_slots >= 0).astype(jnp.int32))
    tiles_used = (filled + TILE - 1) // TILE
    local_at = listed - own_first
    is_owned = (listed >= 0) & (local_at >= 0) & (local_at < s_dev)
    stacked = jnp.concatenate([states, span_all[None, :], weights[None, :]], axis=0)
    column_all = gathered_copies(stacked, "tgt", 1)
    owner_col = my_slots // s_dev % n_src
    places = my_slots // (s_dev * n_src) * s_dev + my_slots % s_dev
    mine_owned = (my_slots >= 0) & (owner_col == my_column)
    chosen = jnp.take(column_all[0:13], jnp.clip(places, 0, n_tgt * s_dev - 1), axis=1)
    partial_rows = jnp.where(mine_owned[None, :], chosen, 0.0)
    ahead_pos, moving = predict(column_all[0:12], column_all[12:13])
    sources = jnp.concatenate([ahead_pos, moving, column_all[13:14]], axis=0)
    target = over_pieces(partial_rows, SRC)
    tgt_ahead, tgt_moving = predict(target[0:12], target[12:13])
    zero_forces = jnp.zeros((6, slot_count), jnp.float32)
    columns = jnp.arange(sources.shape[1], dtype=jnp.int32)
    idents = columns // s_dev * (s_dev * n_src) + my_column * s_dev + columns % s_dev
    partial_forces = tile_forces(
        zero_forces, tgt_ahead, tgt_moving, my_slots, tiles_used, sources, idents
    )
    forces = taken_together(partial_forces, SRC)
    corrected = correct(tgt_ahead, tgt_moving, target[6:9], target[9:12], target[12:13], forces)
    returned = gathered_copies(corrected, "tgt", 1)
    write_at = jnp.where(is_owned, local_at, s_dev)
    states = states.at[:, write_at].set(returned, mode="drop")
    last_time = last_time.at[write_at].set(now_time, mode="drop")
    return (states, last_time)


def whole_program(positions, velocities, accels, jerks, masses, levels, active_first, active_second):
    s_dev = positions.shape[1]
    n_tgt = lax.axis_size("tgt")
    n_src = lax.axis_size(SRC)
    my_row = lax.axis_index("tgt")
    my_column = lax.axis_index(SRC)
    weights = masses / (s_dev * n_tgt * n_src)
    states = jnp.concatenate([positions, velocities, accels, jerks], axis=0)
    last_time = -BASE_STEP * jnp.exp2(-levels.astype(jnp.float32))
    for now_time, active in ((TIME_FIRST, active_first), (TIME_SECOND, active_second)):
        states, last_time = advance(
            states, last_time, weights, active, now_time, s_dev, n_tgt, n_src, my_row, my_column
        )
    return (states[0:3], states[3:6], states[6:9], states[9:12])


def log2_of(size):
    assert size & (size - 1) == 0, "size"
    return size.bit_length() - 1


def iota(shape, dim):
    return lax.broadcasted_iota(jnp.int32, shape, dim)


def lane_pick(table, lanes):
    return lax.gather(
        table,
        lanes[:, :, None],
        lax.GatherDimensionNumbers(
            offset_dims=(),
            collapsed_slice_dims=(1,),
            start_index_map=(1,),
            operand_batching_dims=(0,),
            start_indices_batching_dims=(0,),
        ),
        slice_sizes=(1, 1),
        mode=lax.GatherScatterMode.PROMISE_IN_BOUNDS,
    )


def turned(rows):
    pad = jnp.zeros((LANES - rows.shape[0], LANES), rows.dtype)
    return jnp.concatenate([rows, pad], axis=0).T


def rows_of(values, count):
    width = values[0].shape[1]
    below = count - sum(v.shape[0] for v in values)
    pad = [jnp.zeros((below, width), jnp.float32)] if below else []
    return jnp.concatenate(list(values) + pad, axis=0)


def prepare_kernel(n_stars, pos, vel, acc, jerk, mass, levels, first, second, column_out, row_out, own_out):
    s_dev = pos.shape[1]
    last = -BASE_STEP * jnp.exp2(-levels[...].astype(jnp.float32))
    states = jnp.concatenate([pos[...], vel[...], acc[...], jerk[...]], axis=0)
    weights = mass[...] / n_stars
    room = first.shape[1] + second.shape[1]
    lists = [first[...].astype(jnp.float32), second[...].astype(jnp.float32)]
    if s_dev > room:
        lists.append(jnp.full((1, s_dev - room), -1.0, jnp.float32))
    listed = jnp.concatenate(lists, axis=1)
    column = rows_of([states, last, listed, weights], 16)
    column_out[...] = column
    ahead, moving = predict(states, TIME_FIRST - last)
    ahead_second, moving_second = predict(states, TIME_SECOND - last)
    row = jnp.concatenate([ahead, moving, weights, ahead_second, moving_second], axis=0)
    for copy in range(row_out.shape[0]):
        row_out[copy] = row
    own_out[...] = rows_of([states, last, weights], 16)


def matching_slots(listed, column, n_src, s_dev):
    ids = listed.astype(jnp.int32)
    n_tgt, width = ids.shape
    valid = ids >= 0
    column_of = jnp.where(valid, (ids >> log2_of(s_dev)) & (n_src - 1), -1)
    row_of = jnp.where(valid, ids >> log2_of(s_dev * n_src), -1)
    cells = jnp.zeros((n_tgt, n_src), jnp.float32)
    for slots in range(n_tgt):
        in_row = (row_of[slots : slots + 1] == iota((n_tgt, width), 0)).astype(jnp.bfloat16)
        in_column = (column_of[slots : slots + 1] == iota((n_src, width), 0)).astype(jnp.bfloat16)
        cells = cells + lax.dot_general(
            in_row, in_column, (((1,), (1,)), ((), ())), preferred_element_type=jnp.float32
        )
    return column_of == column, jnp.max(jnp.sum(cells, axis=0, keepdims=True)), jnp.max(cells)


def slot_numbers(mine):
    n_rows, width = mine.shape
    upto = (iota((width, width), 0) <= iota((width, width), 1)).astype(jnp.bfloat16)
    inside = jnp.dot(mine.astype(jnp.bfloat16), upto, preferred_element_type=jnp.float32)
    totals = jnp.broadcast_to(inside[:, width - 1 : width], (n_rows, LANES))
    place = jnp.zeros((1, LANES), jnp.float32)
    before = []
    for row in range(n_rows):
        before.append(place)
        place = place + totals[row : row + 1]
    start = jnp.concatenate(before, axis=0)[:, 0:1]
    return jnp.where(mine, (inside + start).astype(jnp.int32) - 1, -1), jnp.max(place)


def packed_ids(listed, slot, part):
    n_rows, width = listed.shape
    found = jnp.zeros((LANES, LANES), jnp.float32)
    want = iota((LANES, LANES), 0) + part * LANES
    for row in range(n_rows):
        for chunk in range(width // LANES):
            cut = slice(chunk * LANES, (chunk + 1) * LANES)
            hit = jnp.broadcast_to(slot[row : row + 1, cut], (LANES, LANES)) == want
            found = found + jnp.where(hit, listed[row : row + 1, cut] + 1.0, 0.0)
    ids = jnp.broadcast_to(jnp.sum(found, axis=1, keepdims=True) - 1.0, (LANES, LANES))
    return ids.T[0:1]


def target_facts(number, held, my_row, n_src):
    n_tgt, _, s_dev = held.shape
    row_bits, per_row = log2_of(s_dev * n_src), s_dev // LANES
    ids = number.astype(jnp.int32)
    lane = jnp.broadcast_to(ids & (LANES - 1), (16, LANES))
    chunk_of = jnp.where(ids >= 0, (ids >> row_bits) * per_row + ((ids & (s_dev - 1)) >> log2_of(LANES)), -1)

    def one_row(row, picked):
        for chunk in range(per_row):
            table = held[row, :, chunk * LANES : (chunk + 1) * LANES]
            picked = jnp.where(chunk_of == row * per_row + chunk, lane_pick(table, lane), picked)
        return picked

    picked = lax.fori_loop(0, n_tgt, one_row, jnp.zeros((16, LANES), jnp.float32), unroll=2)
    key = jnp.where((ids >= 0) & ((ids >> row_bits) == my_row), ids & (s_dev - 1), -1)
    return rows_of([picked[0:13], number, picked[14:15], key.astype(jnp.float32)], 16)


def select_kernel(n_src, slots_first, slots_second, held, target_out, turned_out, info_out):
    s_dev = held.shape[2]
    my_row, my_column = lax.axis_index("tgt"), lax.axis_index(SRC)
    listed = held[:, 13, :]
    first, second = listed[:, :slots_first], listed[:, slots_first : slots_first + slots_second]
    mine, most_first, most_own = matching_slots(first, my_column, n_src, s_dev)
    _, most_second, _ = matching_slots(second, my_column, n_src, s_dev)
    slot, count = slot_numbers(mine)
    count = jnp.minimum(count.astype(jnp.int32), FIRST_ROOM)
    info_out[0] = count
    fits = (most_first <= FIRST_ROOM) & (most_second <= SECOND_ROOM) & (most_own <= OWN_ROOM)
    info_out[1] = fits.astype(jnp.int32)

    def fill(part):
        facts = target_facts(packed_ids(first, slot, part), held, my_row, n_src)
        ahead, moving = predict(facts[0:12], TIME_FIRST - facts[12:13])
        cut = slice(part * LANES, (part + 1) * LANES)
        target_out[:, cut] = facts
        turned_out[cut, :] = turned(rows_of([ahead, moving, facts[15:16], facts[13:14]], 8))

    fill(0)
    for part in range(1, FIRST_ROOM // LANES):
        pl.when(count > part * LANES)(functools.partial(fill, part))

        @pl.when(count <= part * LANES)
        def _():
            cut = slice(part * LANES, (part + 1) * LANES)
            target_out[:, cut] = jnp.full((16, LANES), -1.0, jnp.float32)
            turned_out[cut, :] = jnp.full((LANES, LANES), -1.0, jnp.float32)


def found_slots(keys, wanted):
    found = jnp.zeros((LANES, LANES), jnp.float32)
    for part, key in enumerate(keys):
        place = (iota((LANES, LANES), 0) + part * LANES + 1).astype(jnp.float32)
        found = found + jnp.where((key == wanted) & (key >= 0.0), place, 0.0)
    return jnp.sum(found, axis=0, keepdims=True).astype(jnp.int32) - 1


def plan_kernel(n_src, slots_first, slots_second, held, first_target, turned_in, second_out, plan_out, info_out):
    s_dev = held.shape[2]
    my_row, my_column = lax.axis_index("tgt"), lax.axis_index(SRC)
    listed = held[:, 13, slots_first : slots_first + slots_second]
    ids = listed.astype(jnp.int32)
    mine = (ids >= 0) & (((ids >> log2_of(s_dev)) & (n_src - 1)) == my_column)
    slot, count = slot_numbers(mine)
    info_out[0] = jnp.minimum(count.astype(jnp.int32), SECOND_ROOM)
    facts = target_facts(packed_ids(listed, slot, 0), held, my_row, n_src)
    second_out[...] = facts
    parts = FIRST_ROOM // LANES
    columns = [turned_in[part * LANES : (part + 1) * LANES, :] for part in range(parts)]
    keys = [jnp.broadcast_to(c[:, 6:7], (LANES, LANES)) for c in columns]
    numbers = [jnp.broadcast_to(c[:, 7:8], (LANES, LANES)) for c in columns]
    second_keys = [jnp.broadcast_to(facts[15:16], (LANES, LANES)).T]
    plan_out[...] = jnp.full(plan_out.shape, -1, jnp.int32)
    for chunk in range(s_dev // LANES):
        cut = slice(chunk * LANES, (chunk + 1) * LANES)
        star = (iota((1, LANES), 1) + chunk * LANES).astype(jnp.float32)
        plan_out[0:1, cut] = found_slots(keys, star)
        plan_out[1:2, cut] = found_slots(second_keys, star)
    plan_out[2:3, 0:LANES] = found_slots(numbers, facts[13:14])
    own = [(key >= 0.0) for key in keys]
    upto = (iota((LANES, LANES), 1) <= iota((LANES, LANES), 0)).astype(jnp.bfloat16)
    before = jnp.zeros((1, LANES), jnp.float32)
    order = []
    for flags in own:
        inside = jnp.dot(upto, flags.astype(jnp.bfloat16), preferred_element_type=jnp.float32) + before
        order.append(jnp.where(flags, inside - 1.0, -1.0))
        before = inside[LANES - 1 : LANES]
    plan_out[3:4, 0:LANES] = found_slots(order, iota((1, LANES), 1).astype(jnp.float32))


def pair_terms(source, target, own_place=None, key=None):
    rx, ry, rz = (source[j] - target[j] for j in range(3))
    ux, uy, uz = (source[j] - target[j] for j in range(3, 6))
    inverse = lax.rsqrt((rx * rx + ry * ry + rz * rz) + SOFTENING_SQ)
    inverse_sq = inverse * inverse
    weight3 = source[6] * inverse * inverse_sq
    if own_place is not None:
        weight3 = jnp.where(key == own_place, 0.0, weight3)
    closing = (rx * ux + ry * uy + rz * uz) * inverse_sq * weight3
    return (
        rx * weight3, ry * weight3, rz * weight3,
        ux * weight3, uy * weight3, uz * weight3,
        rx * closing, ry * closing, rz * closing,
    )


def added(running, parts):
    return tuple(a + b for a, b in zip(running, parts))


def target_blocks(count, turned_in, sums, visit):
    def one_block(first, tall):
        at = pl.ds(pl.multiple_of(first, 8), tall)
        facts = turned_in[at, :]
        target = [jnp.broadcast_to(facts[:, j : j + 1], (tall, LANES)) for j in range(6)]
        key = jnp.broadcast_to(facts[:, 6:7], (tall, LANES))
        running = visit(tall, target, key, (jnp.zeros((tall, LANES), jnp.float32),) * 9)
        totals = [running[j] for j in range(3)] + [running[3 + j] - 3.0 * running[6 + j] for j in range(3)]
        lanes = iota((tall, LANES), 1)
        packed = sums[at, :]
        for j in range(6):
            total = jnp.broadcast_to(jnp.sum(totals[j], axis=1, keepdims=True), (tall, LANES))
            packed = packed + jnp.where(lanes == j, total, 0.0)
        sums[at, :] = packed

    tall_blocks = (count + 7) // 16
    pl.loop(0, tall_blocks)(lambda block: one_block(block * 16, 16))
    pl.when(count > tall_blocks * 16)(lambda: one_block(tall_blocks * 16, 8))


def row_sums(count, near, far, first_row, turned_in, sums):
    n_z, _, s_dev = near.shape
    my_z = lax.axis_index("z")
    rows = [first_row + j for j in range(6)] + [6]
    sums[...] = jnp.zeros_like(sums)

    def visit(tall, target, key, running):
        def segment(stars, which, running, own=False):
            for chunk in range(s_dev // LANES):
                cut = slice(chunk * LANES, (chunk + 1) * LANES)
                source = [jnp.broadcast_to(stars[which, j : j + 1, cut], (tall, LANES)) for j in rows]
                place = (iota((tall, LANES), 1) + chunk * LANES).astype(jnp.float32) if own else None
                running = added(running, pair_terms(source, target, place, key))
            return running

        def both(step, running):
            return segment(near, jnp.where(step < my_z, step, step + 1), segment(far, step, running))

        running = lax.fori_loop(0, n_z - 1, both, running)
        return segment(near, my_z, segment(far, n_z - 1, running), own=True)

    target_blocks(count, turned_in, sums, visit)


def write_sums(sums, force_out):
    copies, _, room = force_out.shape
    for part in range(room // LANES):
        cut = slice(part * LANES, (part + 1) * LANES)
        rows = sums[cut, :].T[0:8]
        for copy in range(copies):
            force_out[copy, :, cut] = rows


def first_force_kernel(info, near, far, turned_in, force_out, sums):
    row_sums(info[0], near, far, 0, turned_in, sums)
    write_sums(sums, force_out)


def second_force_kernel(info, near, far, turned_in, sums_out):
    row_sums(info[0], near, far, 7, turned_in, sums_out)


def update_force_kernel(info, near, far, turned_in, sums_in, force_out, sums, stars):
    n_z = near.shape[0]
    my_z = lax.axis_index("z")
    half = iota((8, LANES), 1) < LANES // 2
    for z in range(n_z):
        both = jnp.where(half, near[z], pltpu.roll(far[z], LANES // 2, axis=1))
        place = jnp.where(half[7:8] & (my_z == z), both[7:8], -2.0)
        stars[z] = jnp.concatenate([both[0:7], place], axis=0)
    sums[...] = sums_in[...]

    def visit(tall, target, key, running):
        def one(z, running):
            source = [jnp.broadcast_to(stars[z, j : j + 1, :], (tall, LANES)) for j in range(8)]
            return added(running, pair_terms(source, target, source[7], key))

        return lax.fori_loop(0, n_z, one, running, unroll=4)

    target_blocks(info[0], turned_in, sums, visit)
    write_sums(sums, force_out)


def summed(received):
    total = received[0]
    for row in range(1, received.shape[0]):
        total = total + received[row]
    return total


def picked_slots(values, slot):
    lane = jnp.broadcast_to(slot & (LANES - 1), (16, LANES))
    new = jnp.zeros((16, LANES), jnp.float32)
    for part in range(values.shape[1] // LANES):
        pick = lane_pick(values[:, part * LANES : (part + 1) * LANES], lane)
        new = jnp.where((slot >> log2_of(LANES)) == part, pick, new)
    return new


def correct_kernel(received, target, second, plan, own, update_out, own_out, second_out, turned_out):
    copies = update_out.shape[0]
    room = received.shape[2]
    s_dev = own.shape[1]
    forces = summed(received)
    states = target[0:12, :]
    span = TIME_FIRST - target[12:13, :]
    ahead, moving = predict(states, span)
    corrected = correct(ahead, moving, states[6:9], states[9:12], span, forces[0:6])
    corrected = rows_of([corrected, jnp.full((1, room), TIME_FIRST, jnp.float32)], 16)
    slot = plan[3:4, 0:LANES]
    old = picked_slots(target[...], slot)
    new = picked_slots(corrected, slot)
    present = slot >= 0
    weight, place = old[14:15], jnp.where(present, old[15:16], -1.0)
    ahead_new, moving_new = predict(new[0:12], TIME_SECOND - new[12:13])
    ahead_old, moving_old = predict(old[0:12], TIME_SECOND - old[12:13])
    arrived = jnp.concatenate([ahead_new, moving_new, weight, place], axis=0)
    left = jnp.concatenate([ahead_old, moving_old, -weight, place], axis=0)
    lane = iota((8, LANES), 1)
    update = jnp.where(lane < OWN_ROOM, arrived, pltpu.roll(left, OWN_ROOM, axis=1))
    update = jnp.where(lane < 2 * OWN_ROOM, update, 0.0)
    for copy in range(copies):
        update_out[copy] = update
    for chunk in range(s_dev // LANES):
        cut = slice(chunk * LANES, (chunk + 1) * LANES)
        slot = plan[0:1, cut]
        own_out[:, cut] = jnp.where(slot >= 0, picked_slots(corrected, slot), own[:, cut])
    other = second[...]
    slot = plan[2:3, 0:LANES]
    states = jnp.where(slot >= 0, picked_slots(corrected, slot), other)
    span = TIME_SECOND - states[12:13]
    ahead, moving = predict(states[0:12], span)
    second_out[...] = rows_of([ahead, moving, states[6:12], span], 16)
    turned_out[...] = turned(rows_of([ahead, moving, other[15:16]], 8))


def finish_kernel(received, second, plan, own, pos_out, vel_out, acc_out, jerk_out):
    forces = summed(received)
    facts = second[...]
    corrected = correct(facts[0:3], facts[3:6], facts[6:9], facts[9:12], facts[12:13], forces[0:6])
    corrected = rows_of([corrected], 16)
    for chunk in range(own.shape[1] // LANES):
        cut = slice(chunk * LANES, (chunk + 1) * LANES)
        slot = plan[1:2, cut]
        new = jnp.where(slot >= 0, picked_slots(corrected, slot), own[:, cut])
        pos_out[:, cut] = new[0:3]
        vel_out[:, cut] = new[3:6]
        acc_out[:, cut] = new[6:9]
        jerk_out[:, cut] = new[9:12]


def f32(*shape):
    return jax.ShapeDtypeStruct(shape, jnp.float32)


INTERPRET = False


def call(kernel, outs, scalars=0, operands=0, scratch=(), smem_out=None):
    smem, vmem = pl.BlockSpec(memory_space=pltpu.SMEM), pl.BlockSpec(memory_space=pltpu.VMEM)
    return pl.pallas_call(
        kernel,
        out_shape=outs,
        in_specs=[smem] * scalars + [vmem] * operands,
        out_specs=tuple(smem if i == smem_out else vmem for i in range(len(outs))),
        scratch_shapes=list(scratch),
        interpret=INTERPRET,
        compiler_params=pltpu.CompilerParams(vmem_limit_bytes=16 << 20),
    )


def exchanged(copies, axis):
    return lax.all_to_all(copies, axis, split_axis=0, concat_axis=0, tiled=True)


def other_core(near):
    return lax.ppermute(near, "core", [(0, 1), (1, 0)])


def shards(positions, velocities, accels, jerks, masses, levels, active_first, active_second):
    s_dev = positions.shape[1]
    n_tgt, n_z, n_src = lax.axis_size("tgt"), lax.axis_size("z"), lax.axis_size(SRC)
    n_stars = s_dev * n_tgt * n_src
    scalar = jax.ShapeDtypeStruct((2,), jnp.int32)
    lists = (n_src, active_first.shape[0], active_second.shape[0])
    column, row_copies, own = call(
        functools.partial(prepare_kernel, n_stars), (f32(16, s_dev), f32(n_z, 13, s_dev), f32(16, s_dev)), 0, 8
    )(
        positions, velocities, accels, jerks, masses.reshape(1, s_dev), levels.reshape(1, s_dev),
        active_first.reshape(1, -1), active_second.reshape(1, -1),
    )
    near = exchanged(row_copies, "z")
    column = lax.all_gather(column, "tgt")
    far = other_core(near)
    target, columns, info = call(
        functools.partial(select_kernel, *lists), (f32(16, FIRST_ROOM), f32(FIRST_ROOM, LANES), scalar), 0, 1, smem_out=2
    )(column)
    (partial,) = call(
        first_force_kernel, (f32(n_tgt, 8, FIRST_ROOM),), 1, 3, [pltpu.VMEM((FIRST_ROOM, LANES), jnp.float32)]
    )(info, near, far, columns)
    received = exchanged(partial, "tgt")
    second, plan, second_info = call(
        functools.partial(plan_kernel, *lists),
        (f32(16, SECOND_ROOM), jax.ShapeDtypeStruct((8, s_dev), jnp.int32), scalar), 0, 3, smem_out=2,
    )(column, target, columns)
    update, own, second, second_columns = call(
        correct_kernel, (f32(n_z, 8, LANES), f32(16, s_dev), f32(16, SECOND_ROOM), f32(LANES, LANES)), 0, 5
    )(received, target, second, plan, own)
    near_update = exchanged(update, "z")
    (sums,) = call(second_force_kernel, (f32(SECOND_ROOM, LANES),), 1, 3)(second_info, near, far, second_columns)
    far_update = other_core(near_update)
    (partial,) = call(
        update_force_kernel, (f32(n_tgt, 8, SECOND_ROOM),), 1, 4,
        [pltpu.VMEM((SECOND_ROOM, LANES), jnp.float32), pltpu.VMEM((n_z, 8, LANES), jnp.float32)],
    )(second_info, near_update, far_update, second_columns, sums)
    received = exchanged(partial, "tgt")

    def by_columns(received, second, plan, own, *inputs):
        return tuple(call(finish_kernel, (f32(3, s_dev),) * 4, 0, 4)(received, second, plan, own))

    def anywhere(received, second, plan, own, *inputs):
        return whole_program(*inputs)

    inputs = (positions, velocities, accels, jerks, masses, levels, active_first, active_second)
    return lax.cond(info[1] == 1, by_columns, anywhere, received, second, plan, own, *inputs)


def solution(mesh):
    n_tgt, n_src = mesh.devices.shape
    finer = Mesh(mesh.devices.reshape(n_tgt, n_src // 2, 2), ("tgt", "z", "core"))
    stars = ("tgt", "z", "core")
    vector, scalar = P(None, stars), P(stars)
    return jax.shard_map(
        shards,
        mesh=finer,
        in_specs=(vector, vector, vector, vector, scalar, scalar, P("tgt"), P("tgt")),
        out_specs=(vector,) * 4,
        check_vma=False,
    )
```

```python
import functools

import jax
import jax.numpy as jnp
from jax import lax
from jax.experimental import pallas as pl
from jax.experimental.pallas import tpu as pltpu
from jax.sharding import Mesh
from jax.sharding import PartitionSpec as P

TILE = 128
LEVELS = 4
LANES = 128
FIRST_ROOM = 256
SECOND_ROOM = 128
OWN_ROOM = 32

SOFTENING_SQ = 0.0001
BASE_STEP = 0.5
TIME_FIRST = 0.0
TIME_SECOND = BASE_STEP / (1 << LEVELS)
SRC = ("z", "core")


def sent_to_all(shard, axis):
    copies = jnp.broadcast_to(shard, (lax.axis_size(axis), *shard.shape))
    return lax.all_to_all(copies, axis, split_axis=0, concat_axis=0, tiled=True)


def laid_out(tiles, dim):
    dims = list(tiles.shape[1:])
    dims[dim] *= tiles.shape[0]
    return jnp.moveaxis(tiles, 0, dim).reshape(dims)


def gathered_copies(shard, axis, dim):
    tiles = sent_to_all(shard, axis)
    return laid_out(tiles, dim)


def over_pieces(shard, axis):
    return lax.all_gather(shard, axis).sum(0)


def taken_together(shard, axis):
    return sent_to_all(shard, axis).sum(axis=0)


def predict(states, span):
    ahead_pos = states[0:3] + span * (
        states[3:6] + span * (states[6:9] * 0.5 + span * states[9:12] / 6.0)
    )
    moving = states[3:6] + span * (states[6:9] + span * states[9:12] * 0.5)
    return (ahead_pos, moving)


def pair_block(tile_place, tile_speed, tile_ident, sources, source_ident):
    offset = sources[0:3, None, :] - tile_place[:, :, None]
    motion = sources[3:6, None, :] - tile_speed[:, :, None]
    dist_sq = jnp.sum(offset * offset, axis=0) + SOFTENING_SQ
    inverse = lax.rsqrt(dist_sq)
    inverse_sq = inverse * inverse
    weight3 = jnp.where(
        source_ident[None, :] == tile_ident[:, None],
        0.0,
        sources[6][None, :] * inverse_sq * inverse,
    )
    closing = jnp.sum(offset * motion, axis=0)
    attract = jnp.sum(offset * weight3, axis=2)
    change = jnp.sum(motion * weight3 - 3.0 * (closing * inverse_sq * weight3) * offset, axis=2)
    return jnp.concatenate([attract, change], axis=0)


def correct(ahead_pos, moving, old_accel, old_jolt, span, forces):
    new_acc = forces[0:3]
    new_jolt = forces[3:6]
    second_term = -6.0 * (old_accel - new_acc) - span * (4.0 * old_jolt + 2.0 * new_jolt)
    third_term = 12.0 * (old_accel - new_acc) + 6.0 * span * (old_jolt + new_jolt)
    new_place = ahead_pos + span * span * (second_term / 24.0 + third_term / 120.0)
    new_speed = moving + span * (second_term / 6.0 + third_term / 24.0)
    return jnp.concatenate([new_place, new_speed, new_acc, new_jolt], axis=0)


def tile_forces(held, tgt_ahead, tgt_moving, slot_ids, tiles_used, shard_part, idents):
    length = shard_part.shape[1]
    block_len = length
    while block_len > 2048 and block_len % 2 == 0:
        block_len = block_len // 2
    block_count = length // block_len
    src_blocks = shard_part.reshape(7, block_count, block_len).transpose(1, 0, 2)
    ident_blocks = idents.reshape(block_count, block_len)

    def one_tile(tile_no, carried):
        place_tile = lax.dynamic_slice_in_dim(tgt_ahead, tile_no * TILE, TILE, 1)
        speed_tile = lax.dynamic_slice_in_dim(tgt_moving, tile_no * TILE, TILE, 1)
        ident_tile = lax.dynamic_slice_in_dim(slot_ids, tile_no * TILE, TILE, 0)

        def add_block(running, source_pair):
            return (
                running
                + pair_block(place_tile, speed_tile, ident_tile, source_pair[0], source_pair[1]),
                None,
            )

        running, _ = lax.scan(
            add_block, jnp.zeros((6, TILE), jnp.float32), (src_blocks, ident_blocks)
        )
        before = lax.dynamic_slice_in_dim(carried, tile_no * TILE, TILE, 1)
        return lax.dynamic_update_slice_in_dim(carried, before + running, tile_no * TILE, 1)

    return lax.fori_loop(0, tiles_used, one_tile, held)


def advance(states, last_time, weights, active, now_time, s_dev, n_tgt, n_src, my_row, my_column):
    slot_count = active.shape[0]
    own_first = (my_row * n_src + my_column) * s_dev
    listed = gathered_copies(active, "tgt", 0)
    span_all = now_time - last_time
    my_slots = lax.dynamic_slice_in_dim(listed, my_row * slot_count, slot_count, 0)
    filled = jnp.sum((my_slots >= 0).astype(jnp.int32))
    tiles_used = (filled + TILE - 1) // TILE
    local_at = listed - own_first
    is_owned = (listed >= 0) & (local_at >= 0) & (local_at < s_dev)
    stacked = jnp.concatenate([states, span_all[None, :], weights[None, :]], axis=0)
    column_all = gathered_copies(stacked, "tgt", 1)
    owner_col = my_slots // s_dev % n_src
    places = my_slots // (s_dev * n_src) * s_dev + my_slots % s_dev
    mine_owned = (my_slots >= 0) & (owner_col == my_column)
    chosen = jnp.take(column_all[0:13], jnp.clip(places, 0, n_tgt * s_dev - 1), axis=1)
    partial_rows = jnp.where(mine_owned[None, :], chosen, 0.0)
    ahead_pos, moving = predict(column_all[0:12], column_all[12:13])
    sources = jnp.concatenate([ahead_pos, moving, column_all[13:14]], axis=0)
    target = over_pieces(partial_rows, SRC)
    tgt_ahead, tgt_moving = predict(target[0:12], target[12:13])
    zero_forces = jnp.zeros((6, slot_count), jnp.float32)
    columns = jnp.arange(sources.shape[1], dtype=jnp.int32)
    idents = columns // s_dev * (s_dev * n_src) + my_column * s_dev + columns % s_dev
    partial_forces = tile_forces(
        zero_forces, tgt_ahead, tgt_moving, my_slots, tiles_used, sources, idents
    )
    forces = taken_together(partial_forces, SRC)
    corrected = correct(tgt_ahead, tgt_moving, target[6:9], target[9:12], target[12:13], forces)
    returned = gathered_copies(corrected, "tgt", 1)
    write_at = jnp.where(is_owned, local_at, s_dev)
    states = states.at[:, write_at].set(returned, mode="drop")
    last_time = last_time.at[write_at].set(now_time, mode="drop")
    return (states, last_time)


def whole_program(positions, velocities, accels, jerks, masses, levels, active_first, active_second):
    s_dev = positions.shape[1]
    n_tgt = lax.axis_size("tgt")
    n_src = lax.axis_size(SRC)
    my_row = lax.axis_index("tgt")
    my_column = lax.axis_index(SRC)
    weights = masses / (s_dev * n_tgt * n_src)
    states = jnp.concatenate([positions, velocities, accels, jerks], axis=0)
    last_time = -BASE_STEP * jnp.exp2(-levels.astype(jnp.float32))
    for now_time, active in ((TIME_FIRST, active_first), (TIME_SECOND, active_second)):
        states, last_time = advance(
            states, last_time, weights, active, now_time, s_dev, n_tgt, n_src, my_row, my_column
        )
    return (states[0:3], states[3:6], states[6:9], states[9:12])


def log2_of(size):
    assert size & (size - 1) == 0, "size"
    return size.bit_length() - 1


def iota(shape, dim):
    return lax.broadcasted_iota(jnp.int32, shape, dim)


def lane_pick(table, lanes):
    return lax.gather(
        table,
        lanes[:, :, None],
        lax.GatherDimensionNumbers(
            offset_dims=(),
            collapsed_slice_dims=(1,),
            start_index_map=(1,),
            operand_batching_dims=(0,),
            start_indices_batching_dims=(0,),
        ),
        slice_sizes=(1, 1),
        mode=lax.GatherScatterMode.PROMISE_IN_BOUNDS,
    )


def turned(rows):
    pad = jnp.zeros((LANES - rows.shape[0], LANES), rows.dtype)
    return jnp.concatenate([rows, pad], axis=0).T


def rows_of(values, count):
    width = values[0].shape[1]
    below = count - sum(v.shape[0] for v in values)
    pad = [jnp.zeros((below, width), jnp.float32)] if below else []
    return jnp.concatenate(list(values) + pad, axis=0)


def prepare_kernel(n_stars, pos, vel, acc, jerk, mass, levels, first, second, column_out, row_out, own_out):
    s_dev = pos.shape[1]
    last = -BASE_STEP * jnp.exp2(-levels[...].astype(jnp.float32))
    states = jnp.concatenate([pos[...], vel[...], acc[...], jerk[...]], axis=0)
    weights = mass[...] / n_stars
    room = first.shape[1] + second.shape[1]
    lists = [first[...].astype(jnp.float32), second[...].astype(jnp.float32)]
    if s_dev > room:
        lists.append(jnp.full((1, s_dev - room), -1.0, jnp.float32))
    listed = jnp.concatenate(lists, axis=1)
    column = rows_of([states, last, listed, weights], 16)
    column_out[...] = column
    ahead, moving = predict(states, TIME_FIRST - last)
    ahead_second, moving_second = predict(states, TIME_SECOND - last)
    row = jnp.concatenate([ahead, moving, weights, ahead_second, moving_second], axis=0)
    row = jnp.concatenate([row[:, at : at + LANES] for at in range(0, s_dev, LANES)], axis=0)
    for copy in range(row_out.shape[0]):
        row_out[copy] = row
    own_out[...] = rows_of([states, last, weights], 16)


def matching_slots(listed, column, n_src, s_dev):
    ids = listed.astype(jnp.int32)
    n_tgt, width = ids.shape
    valid = ids >= 0
    column_of = jnp.where(valid, (ids >> log2_of(s_dev)) & (n_src - 1), -1)
    row_of = jnp.where(valid, ids >> log2_of(s_dev * n_src), -1)
    cells = jnp.zeros((n_tgt, n_src), jnp.float32)
    for slots in range(n_tgt):
        in_row = (row_of[slots : slots + 1] == iota((n_tgt, width), 0)).astype(jnp.bfloat16)
        in_column = (column_of[slots : slots + 1] == iota((n_src, width), 0)).astype(jnp.bfloat16)
        cells = cells + lax.dot_general(
            in_row, in_column, (((1,), (1,)), ((), ())), preferred_element_type=jnp.float32
        )
    return column_of == column, jnp.max(jnp.sum(cells, axis=0, keepdims=True)), jnp.max(cells)


def slot_numbers(mine):
    n_rows, width = mine.shape
    upto = (iota((width, width), 0) <= iota((width, width), 1)).astype(jnp.bfloat16)
    inside = jnp.dot(mine.astype(jnp.bfloat16), upto, preferred_element_type=jnp.float32)
    totals = jnp.broadcast_to(inside[:, width - 1 : width], (n_rows, LANES))
    place = jnp.zeros((1, LANES), jnp.float32)
    before = []
    for row in range(n_rows):
        before.append(place)
        place = place + totals[row : row + 1]
    start = jnp.concatenate(before, axis=0)[:, 0:1]
    return jnp.where(mine, (inside + start).astype(jnp.int32) - 1, -1), jnp.max(place)


def packed_ids(listed, slot, part):
    n_rows, width = listed.shape
    found = jnp.zeros((LANES, LANES), jnp.float32)
    want = iota((LANES, LANES), 0) + part * LANES
    for row in range(n_rows):
        for chunk in range(width // LANES):
            cut = slice(chunk * LANES, (chunk + 1) * LANES)
            hit = jnp.broadcast_to(slot[row : row + 1, cut], (LANES, LANES)) == want
            found = found + jnp.where(hit, listed[row : row + 1, cut] + 1.0, 0.0)
    ids = jnp.broadcast_to(jnp.sum(found, axis=1, keepdims=True) - 1.0, (LANES, LANES))
    return ids.T[0:1]


def target_facts(number, held, my_row, n_src):
    n_tgt, _, s_dev = held.shape
    row_bits, per_row = log2_of(s_dev * n_src), s_dev // LANES
    ids = number.astype(jnp.int32)
    lane = jnp.broadcast_to(ids & (LANES - 1), (16, LANES))
    chunk_of = jnp.where(ids >= 0, (ids >> row_bits) * per_row + ((ids & (s_dev - 1)) >> log2_of(LANES)), -1)

    def one_row(row, picked):
        for chunk in range(per_row):
            table = held[row, :, chunk * LANES : (chunk + 1) * LANES]
            picked = jnp.where(chunk_of == row * per_row + chunk, lane_pick(table, lane), picked)
        return picked

    picked = lax.fori_loop(0, n_tgt, one_row, jnp.zeros((16, LANES), jnp.float32), unroll=2)
    key = jnp.where((ids >= 0) & ((ids >> row_bits) == my_row), ids & (s_dev - 1), -1)
    return rows_of([picked[0:13], number, picked[14:15], key.astype(jnp.float32)], 16)


def select_kernel(n_src, slots_first, slots_second, held, target_out, turned_out, info_out):
    s_dev = held.shape[2]
    my_row, my_column = lax.axis_index("tgt"), lax.axis_index(SRC)
    listed = held[:, 13, :]
    first, second = listed[:, :slots_first], listed[:, slots_first : slots_first + slots_second]
    mine, most_first, most_own = matching_slots(first, my_column, n_src, s_dev)
    _, most_second, _ = matching_slots(second, my_column, n_src, s_dev)
    slot, count = slot_numbers(mine)
    count = jnp.minimum(count.astype(jnp.int32), FIRST_ROOM)
    info_out[0] = count
    fits = (most_first <= FIRST_ROOM) & (most_second <= SECOND_ROOM) & (most_own <= OWN_ROOM)
    info_out[1] = fits.astype(jnp.int32)

    def fill(part):
        facts = target_facts(packed_ids(first, slot, part), held, my_row, n_src)
        ahead, moving = predict(facts[0:12], TIME_FIRST - facts[12:13])
        cut = slice(part * LANES, (part + 1) * LANES)
        target_out[:, cut] = facts
        turned_out[cut, :] = turned(rows_of([ahead, moving, facts[15:16], facts[13:14]], 8))

    fill(0)
    for part in range(1, FIRST_ROOM // LANES):
        pl.when(count > part * LANES)(functools.partial(fill, part))

        @pl.when(count <= part * LANES)
        def _():
            cut = slice(part * LANES, (part + 1) * LANES)
            target_out[:, cut] = jnp.full((16, LANES), -1.0, jnp.float32)
            turned_out[cut, :] = jnp.full((LANES, LANES), -1.0, jnp.float32)


def found_slots(keys, wanted):
    found = jnp.zeros((LANES, LANES), jnp.float32)
    for part, key in enumerate(keys):
        place = (iota((LANES, LANES), 0) + part * LANES + 1).astype(jnp.float32)
        found = found + jnp.where((key == wanted) & (key >= 0.0), place, 0.0)
    return jnp.sum(found, axis=0, keepdims=True).astype(jnp.int32) - 1


def plan_kernel(n_src, slots_first, slots_second, held, first_target, turned_in, second_out, plan_out, info_out):
    s_dev = held.shape[2]
    my_row, my_column = lax.axis_index("tgt"), lax.axis_index(SRC)
    listed = held[:, 13, slots_first : slots_first + slots_second]
    ids = listed.astype(jnp.int32)
    mine = (ids >= 0) & (((ids >> log2_of(s_dev)) & (n_src - 1)) == my_column)
    slot, count = slot_numbers(mine)
    info_out[0] = jnp.minimum(count.astype(jnp.int32), SECOND_ROOM)
    facts = target_facts(packed_ids(listed, slot, 0), held, my_row, n_src)
    second_out[...] = facts
    parts = FIRST_ROOM // LANES
    columns = [turned_in[part * LANES : (part + 1) * LANES, :] for part in range(parts)]
    keys = [jnp.broadcast_to(c[:, 6:7], (LANES, LANES)) for c in columns]
    numbers = [jnp.broadcast_to(c[:, 7:8], (LANES, LANES)) for c in columns]
    second_keys = [jnp.broadcast_to(facts[15:16], (LANES, LANES)).T]
    plan_out[...] = jnp.full(plan_out.shape, -1, jnp.int32)
    for chunk in range(s_dev // LANES):
        cut = slice(chunk * LANES, (chunk + 1) * LANES)
        star = (iota((1, LANES), 1) + chunk * LANES).astype(jnp.float32)
        plan_out[0:1, cut] = found_slots(keys, star)
        plan_out[1:2, cut] = found_slots(second_keys, star)
    plan_out[2:3, 0:LANES] = found_slots(numbers, facts[13:14])
    own = [(key >= 0.0) for key in keys]
    upto = (iota((LANES, LANES), 1) <= iota((LANES, LANES), 0)).astype(jnp.bfloat16)
    before = jnp.zeros((1, LANES), jnp.float32)
    order = []
    for flags in own:
        inside = jnp.dot(upto, flags.astype(jnp.bfloat16), preferred_element_type=jnp.float32) + before
        order.append(jnp.where(flags, inside - 1.0, -1.0))
        before = inside[LANES - 1 : LANES]
    plan_out[3:4, 0:LANES] = found_slots(order, iota((1, LANES), 1).astype(jnp.float32))


def pair_terms(source, target, own_place=None, key=None):
    rx, ry, rz = (source[j] - target[j] for j in range(3))
    ux, uy, uz = (source[j] - target[j] for j in range(3, 6))
    inverse = lax.rsqrt((rx * rx + ry * ry + rz * rz) + SOFTENING_SQ)
    inverse_sq = inverse * inverse
    weight3 = source[6] * inverse * inverse_sq
    if own_place is not None:
        weight3 = jnp.where(key == own_place, 0.0, weight3)
    closing = (rx * ux + ry * uy + rz * uz) * inverse_sq
    ax, ay, az = rx * weight3, ry * weight3, rz * weight3
    return (ax, ay, az, ux * weight3, uy * weight3, uz * weight3, ax * closing, ay * closing, az * closing)


def added(running, parts):
    return tuple(a + b for a, b in zip(running, parts))


def target_blocks(count, turned_in, sums, visit):
    def one_block(first, tall):
        at = pl.ds(pl.multiple_of(first, 8), tall)
        facts = turned_in[at, :]
        target = [jnp.broadcast_to(facts[:, j : j + 1], (tall, LANES)) for j in range(6)]
        key = jnp.broadcast_to(facts[:, 6:7], (tall, LANES))
        running = visit(tall, target, key, (jnp.zeros((tall, LANES), jnp.float32),) * 9)
        totals = [running[j] for j in range(3)] + [running[3 + j] - 3.0 * running[6 + j] for j in range(3)]
        lanes = iota((tall, LANES), 1)
        packed = sums[at, :]
        for j in range(6):
            total = jnp.broadcast_to(jnp.sum(totals[j], axis=1, keepdims=True), (tall, LANES))
            packed = packed + jnp.where(lanes == j, total, 0.0)
        sums[at, :] = packed

    tall_blocks = (count + 7) // 16
    pl.loop(0, tall_blocks)(lambda block: one_block(block * 16, 16))
    pl.when(count > tall_blocks * 16)(lambda: one_block(tall_blocks * 16, 8))


def row_sums(count, near, far, first_row, turned_in, sums):
    n_z, height, _ = near.shape
    my_z = lax.axis_index("z")
    rows = [first_row + j for j in range(6)] + [6]
    sums[...] = jnp.zeros_like(sums)

    def visit(tall, target, key, running):
        def segment(stars, which, running, own=False):
            for chunk in range(height // 13):
                at = chunk * 13
                source = [jnp.broadcast_to(stars[which, at + j : at + j + 1, :], (tall, LANES)) for j in rows]
                place = (iota((tall, LANES), 1) + chunk * LANES).astype(jnp.float32) if own else None
                running = added(running, pair_terms(source, target, place, key))
            return running

        def both(step, running):
            return segment(near, jnp.where(step < my_z, step, step + 1), segment(far, step, running))

        running = lax.fori_loop(0, n_z - 1, both, running)
        return segment(near, my_z, segment(far, n_z - 1, running), own=True)

    target_blocks(count, turned_in, sums, visit)


def write_sums(sums, force_out):
    copies, _, room = force_out.shape
    for part in range(room // LANES):
        cut = slice(part * LANES, (part + 1) * LANES)
        rows = sums[cut, :].T[0:8]
        for copy in range(copies):
            force_out[copy, :, cut] = rows


def first_force_kernel(info, near, far, turned_in, force_out, sums):
    row_sums(info[0], near, far, 0, turned_in, sums)
    write_sums(sums, force_out)


def second_force_kernel(info, near, far, turned_in, sums_out):
    row_sums(info[0], near, far, 7, turned_in, sums_out)


def update_force_kernel(info, near, far, turned_in, sums_in, force_out, sums, stars):
    n_z = near.shape[0]
    my_z = lax.axis_index("z")
    half = iota((8, LANES), 1) < LANES // 2
    for z in range(n_z):
        both = jnp.where(half, near[z], pltpu.roll(far[z], LANES // 2, axis=1))
        place = jnp.where(half[7:8] & (my_z == z), both[7:8], -2.0)
        stars[z] = jnp.concatenate([both[0:7], place], axis=0)
    sums[...] = sums_in[...]

    def visit(tall, target, key, running):
        def one(z, running):
            source = [jnp.broadcast_to(stars[z, j : j + 1, :], (tall, LANES)) for j in range(8)]
            return added(running, pair_terms(source, target, source[7], key))

        return lax.fori_loop(0, n_z, one, running, unroll=4)

    target_blocks(info[0], turned_in, sums, visit)
    write_sums(sums, force_out)


def summed(received):
    total = received[0]
    for row in range(1, received.shape[0]):
        total = total + received[row]
    return total


def picked_slots(values, slot):
    lane = jnp.broadcast_to(slot & (LANES - 1), (16, LANES))
    new = jnp.zeros((16, LANES), jnp.float32)
    for part in range(values.shape[1] // LANES):
        pick = lane_pick(values[:, part * LANES : (part + 1) * LANES], lane)
        new = jnp.where((slot >> log2_of(LANES)) == part, pick, new)
    return new


def correct_kernel(received, target, second, plan, own, update_out, own_out, second_out, turned_out):
    copies = update_out.shape[0]
    room = received.shape[2]
    s_dev = own.shape[1]
    forces = summed(received)
    states = target[0:12, :]
    span = TIME_FIRST - target[12:13, :]
    ahead, moving = predict(states, span)
    corrected = correct(ahead, moving, states[6:9], states[9:12], span, forces[0:6])
    corrected = rows_of([corrected, jnp.full((1, room), TIME_FIRST, jnp.float32)], 16)
    slot = plan[3:4, 0:LANES]
    old = picked_slots(target[...], slot)
    new = picked_slots(corrected, slot)
    present = slot >= 0
    weight, place = old[14:15], jnp.where(present, old[15:16], -1.0)
    ahead_new, moving_new = predict(new[0:12], TIME_SECOND - new[12:13])
    ahead_old, moving_old = predict(old[0:12], TIME_SECOND - old[12:13])
    arrived = jnp.concatenate([ahead_new, moving_new, weight, place], axis=0)
    left = jnp.concatenate([ahead_old, moving_old, -weight, place], axis=0)
    lane = iota((8, LANES), 1)
    update = jnp.where(lane < OWN_ROOM, arrived, pltpu.roll(left, OWN_ROOM, axis=1))
    update = jnp.where(lane < 2 * OWN_ROOM, update, 0.0)
    for copy in range(copies):
        update_out[copy] = update
    for chunk in range(s_dev // LANES):
        cut = slice(chunk * LANES, (chunk + 1) * LANES)
        slot = plan[0:1, cut]
        own_out[:, cut] = jnp.where(slot >= 0, picked_slots(corrected, slot), own[:, cut])
    other = second[...]
    slot = plan[2:3, 0:LANES]
    states = jnp.where(slot >= 0, picked_slots(corrected, slot), other)
    span = TIME_SECOND - states[12:13]
    ahead, moving = predict(states[0:12], span)
    second_out[...] = rows_of([ahead, moving, states[6:12], span], 16)
    turned_out[...] = turned(rows_of([ahead, moving, other[15:16]], 8))


def finish_kernel(received, second, plan, own, pos_out, vel_out, acc_out, jerk_out):
    forces = summed(received)
    facts = second[...]
    corrected = correct(facts[0:3], facts[3:6], facts[6:9], facts[9:12], facts[12:13], forces[0:6])
    corrected = rows_of([corrected], 16)
    for chunk in range(own.shape[1] // LANES):
        cut = slice(chunk * LANES, (chunk + 1) * LANES)
        slot = plan[1:2, cut]
        new = jnp.where(slot >= 0, picked_slots(corrected, slot), own[:, cut])
        pos_out[:, cut] = new[0:3]
        vel_out[:, cut] = new[3:6]
        acc_out[:, cut] = new[6:9]
        jerk_out[:, cut] = new[9:12]


def f32(*shape):
    return jax.ShapeDtypeStruct(shape, jnp.float32)


INTERPRET = False


def call(kernel, outs, scalars=0, operands=0, scratch=(), smem_out=None):
    smem, vmem = pl.BlockSpec(memory_space=pltpu.SMEM), pl.BlockSpec(memory_space=pltpu.VMEM)
    return pl.pallas_call(
        kernel,
        out_shape=outs,
        in_specs=[smem] * scalars + [vmem] * operands,
        out_specs=tuple(smem if i == smem_out else vmem for i in range(len(outs))),
        scratch_shapes=list(scratch),
        interpret=INTERPRET,
        compiler_params=pltpu.CompilerParams(vmem_limit_bytes=16 << 20),
    )


def exchanged(copies, axis):
    return lax.all_to_all(copies, axis, split_axis=0, concat_axis=0, tiled=True)


def other_core(near):
    return lax.ppermute(near, "core", [(0, 1), (1, 0)])


def shards(positions, velocities, accels, jerks, masses, levels, active_first, active_second):
    s_dev = positions.shape[1]
    n_tgt, n_z, n_src = lax.axis_size("tgt"), lax.axis_size("z"), lax.axis_size(SRC)
    n_stars = s_dev * n_tgt * n_src
    scalar = jax.ShapeDtypeStruct((2,), jnp.int32)
    lists = (n_src, active_first.shape[0], active_second.shape[0])
    column, row_copies, own = call(
        functools.partial(prepare_kernel, n_stars), (f32(16, s_dev), f32(n_z, 13 * s_dev // LANES, LANES), f32(16, s_dev)), 0, 8
    )(
        positions, velocities, accels, jerks, masses.reshape(1, s_dev), levels.reshape(1, s_dev),
        active_first.reshape(1, -1), active_second.reshape(1, -1),
    )
    near = exchanged(row_copies, "z")
    column = lax.all_gather(column, "tgt")
    far = other_core(near)
    target, columns, info = call(
        functools.partial(select_kernel, *lists), (f32(16, FIRST_ROOM), f32(FIRST_ROOM, LANES), scalar), 0, 1, smem_out=2
    )(column)
    (partial,) = call(
        first_force_kernel, (f32(n_tgt, 8, FIRST_ROOM),), 1, 3, [pltpu.VMEM((FIRST_ROOM, LANES), jnp.float32)]
    )(info, near, far, columns)
    received = exchanged(partial, "tgt")
    second, plan, second_info = call(
        functools.partial(plan_kernel, *lists),
        (f32(16, SECOND_ROOM), jax.ShapeDtypeStruct((8, s_dev), jnp.int32), scalar), 0, 3, smem_out=2,
    )(column, target, columns)
    update, own, second, second_columns = call(
        correct_kernel, (f32(n_z, 8, LANES), f32(16, s_dev), f32(16, SECOND_ROOM), f32(LANES, LANES)), 0, 5
    )(received, target, second, plan, own)
    near_update = exchanged(update, "z")
    (sums,) = call(second_force_kernel, (f32(SECOND_ROOM, LANES),), 1, 3)(second_info, near, far, second_columns)
    far_update = other_core(near_update)
    (partial,) = call(
        update_force_kernel, (f32(n_tgt, 8, SECOND_ROOM),), 1, 4,
        [pltpu.VMEM((SECOND_ROOM, LANES), jnp.float32), pltpu.VMEM((n_z, 8, LANES), jnp.float32)],
    )(second_info, near_update, far_update, second_columns, sums)
    received = exchanged(partial, "tgt")

    def by_columns(received, second, plan, own, *inputs):
        return tuple(call(finish_kernel, (f32(3, s_dev),) * 4, 0, 4)(received, second, plan, own))

    def anywhere(received, second, plan, own, *inputs):
        return whole_program(*inputs)

    inputs = (positions, velocities, accels, jerks, masses, levels, active_first, active_second)
    return lax.cond(info[1] == 1, by_columns, anywhere, received, second, plan, own, *inputs)


def solution(mesh):
    n_tgt, n_src = mesh.devices.shape
    finer = Mesh(mesh.devices.reshape(n_tgt, n_src // 2, 2), ("tgt", "z", "core"))
    stars = ("tgt", "z", "core")
    vector, scalar = P(None, stars), P(stars)
    return jax.shard_map(
        shards,
        mesh=finer,
        in_specs=(vector, vector, vector, vector, scalar, scalar, P("tgt"), P("tgt")),
        out_specs=(vector,) * 4,
        check_vma=False,
    )
```

```python
import functools

import jax
import jax.numpy as jnp
from jax import lax
from jax.experimental import pallas as pl
from jax.experimental.pallas import tpu as pltpu
from jax.sharding import Mesh
from jax.sharding import PartitionSpec as P

TILE = 128
LEVELS = 4
LANES = 128
FIRST_ROOM = 256
SECOND_ROOM = 128
OWN_ROOM = 32
CHUNK_ROWS = 14

SOFTENING_SQ = 0.0001
BASE_STEP = 0.5
TIME_FIRST = 0.0
TIME_SECOND = BASE_STEP / (1 << LEVELS)
SRC = ("z", "core")


def sent_to_all(shard, axis):
    copies = jnp.broadcast_to(shard, (lax.axis_size(axis), *shard.shape))
    return lax.all_to_all(copies, axis, split_axis=0, concat_axis=0, tiled=True)


def laid_out(tiles, dim):
    dims = list(tiles.shape[1:])
    dims[dim] *= tiles.shape[0]
    return jnp.moveaxis(tiles, 0, dim).reshape(dims)


def gathered_copies(shard, axis, dim):
    tiles = sent_to_all(shard, axis)
    return laid_out(tiles, dim)


def over_pieces(shard, axis):
    return lax.all_gather(shard, axis).sum(0)


def taken_together(shard, axis):
    return sent_to_all(shard, axis).sum(axis=0)


def predict(states, span):
    ahead_pos = states[0:3] + span * (
        states[3:6] + span * (states[6:9] * 0.5 + span * states[9:12] / 6.0)
    )
    moving = states[3:6] + span * (states[6:9] + span * states[9:12] * 0.5)
    return (ahead_pos, moving)


def pair_block(tile_place, tile_speed, tile_ident, sources, source_ident):
    offset = sources[0:3, None, :] - tile_place[:, :, None]
    motion = sources[3:6, None, :] - tile_speed[:, :, None]
    dist_sq = jnp.sum(offset * offset, axis=0) + SOFTENING_SQ
    inverse = lax.rsqrt(dist_sq)
    inverse_sq = inverse * inverse
    weight3 = jnp.where(
        source_ident[None, :] == tile_ident[:, None],
        0.0,
        sources[6][None, :] * inverse_sq * inverse,
    )
    closing = jnp.sum(offset * motion, axis=0)
    attract = jnp.sum(offset * weight3, axis=2)
    change = jnp.sum(motion * weight3 - 3.0 * (closing * inverse_sq * weight3) * offset, axis=2)
    return jnp.concatenate([attract, change], axis=0)


def correct(ahead_pos, moving, old_accel, old_jolt, span, forces):
    new_acc = forces[0:3]
    new_jolt = forces[3:6]
    second_term = -6.0 * (old_accel - new_acc) - span * (4.0 * old_jolt + 2.0 * new_jolt)
    third_term = 12.0 * (old_accel - new_acc) + 6.0 * span * (old_jolt + new_jolt)
    new_place = ahead_pos + span * span * (second_term / 24.0 + third_term / 120.0)
    new_speed = moving + span * (second_term / 6.0 + third_term / 24.0)
    return jnp.concatenate([new_place, new_speed, new_acc, new_jolt], axis=0)


def tile_forces(held, tgt_ahead, tgt_moving, slot_ids, tiles_used, shard_part, idents):
    length = shard_part.shape[1]
    block_len = length
    while block_len > 2048 and block_len % 2 == 0:
        block_len = block_len // 2
    block_count = length // block_len
    src_blocks = shard_part.reshape(7, block_count, block_len).transpose(1, 0, 2)
    ident_blocks = idents.reshape(block_count, block_len)

    def one_tile(tile_no, carried):
        place_tile = lax.dynamic_slice_in_dim(tgt_ahead, tile_no * TILE, TILE, 1)
        speed_tile = lax.dynamic_slice_in_dim(tgt_moving, tile_no * TILE, TILE, 1)
        ident_tile = lax.dynamic_slice_in_dim(slot_ids, tile_no * TILE, TILE, 0)

        def add_block(running, source_pair):
            return (
                running
                + pair_block(place_tile, speed_tile, ident_tile, source_pair[0], source_pair[1]),
                None,
            )

        running, _ = lax.scan(
            add_block, jnp.zeros((6, TILE), jnp.float32), (src_blocks, ident_blocks)
        )
        before = lax.dynamic_slice_in_dim(carried, tile_no * TILE, TILE, 1)
        return lax.dynamic_update_slice_in_dim(carried, before + running, tile_no * TILE, 1)

    return lax.fori_loop(0, tiles_used, one_tile, held)


def advance(states, last_time, weights, active, now_time, s_dev, n_tgt, n_src, my_row, my_column):
    slot_count = active.shape[0]
    own_first = (my_row * n_src + my_column) * s_dev
    listed = gathered_copies(active, "tgt", 0)
    span_all = now_time - last_time
    my_slots = lax.dynamic_slice_in_dim(listed, my_row * slot_count, slot_count, 0)
    filled = jnp.sum((my_slots >= 0).astype(jnp.int32))
    tiles_used = (filled + TILE - 1) // TILE
    local_at = listed - own_first
    is_owned = (listed >= 0) & (local_at >= 0) & (local_at < s_dev)
    stacked = jnp.concatenate([states, span_all[None, :], weights[None, :]], axis=0)
    column_all = gathered_copies(stacked, "tgt", 1)
    owner_col = my_slots // s_dev % n_src
    places = my_slots // (s_dev * n_src) * s_dev + my_slots % s_dev
    mine_owned = (my_slots >= 0) & (owner_col == my_column)
    chosen = jnp.take(column_all[0:13], jnp.clip(places, 0, n_tgt * s_dev - 1), axis=1)
    partial_rows = jnp.where(mine_owned[None, :], chosen, 0.0)
    ahead_pos, moving = predict(column_all[0:12], column_all[12:13])
    sources = jnp.concatenate([ahead_pos, moving, column_all[13:14]], axis=0)
    target = over_pieces(partial_rows, SRC)
    tgt_ahead, tgt_moving = predict(target[0:12], target[12:13])
    zero_forces = jnp.zeros((6, slot_count), jnp.float32)
    columns = jnp.arange(sources.shape[1], dtype=jnp.int32)
    idents = columns // s_dev * (s_dev * n_src) + my_column * s_dev + columns % s_dev
    partial_forces = tile_forces(
        zero_forces, tgt_ahead, tgt_moving, my_slots, tiles_used, sources, idents
    )
    forces = taken_together(partial_forces, SRC)
    corrected = correct(tgt_ahead, tgt_moving, target[6:9], target[9:12], target[12:13], forces)
    returned = gathered_copies(corrected, "tgt", 1)
    write_at = jnp.where(is_owned, local_at, s_dev)
    states = states.at[:, write_at].set(returned, mode="drop")
    last_time = last_time.at[write_at].set(now_time, mode="drop")
    return (states, last_time)


def whole_program(positions, velocities, accels, jerks, masses, levels, active_first, active_second):
    s_dev = positions.shape[1]
    n_tgt = lax.axis_size("tgt")
    n_src = lax.axis_size(SRC)
    my_row = lax.axis_index("tgt")
    my_column = lax.axis_index(SRC)
    weights = masses / (s_dev * n_tgt * n_src)
    states = jnp.concatenate([positions, velocities, accels, jerks], axis=0)
    last_time = -BASE_STEP * jnp.exp2(-levels.astype(jnp.float32))
    for now_time, active in ((TIME_FIRST, active_first), (TIME_SECOND, active_second)):
        states, last_time = advance(
            states, last_time, weights, active, now_time, s_dev, n_tgt, n_src, my_row, my_column
        )
    return (states[0:3], states[3:6], states[6:9], states[9:12])


def log2_of(size):
    assert size & (size - 1) == 0, "size"
    return size.bit_length() - 1


def iota(shape, dim):
    return lax.broadcasted_iota(jnp.int32, shape, dim)


def lane_pick(table, lanes):
    return lax.gather(
        table,
        lanes[:, :, None],
        lax.GatherDimensionNumbers(
            offset_dims=(),
            collapsed_slice_dims=(1,),
            start_index_map=(1,),
            operand_batching_dims=(0,),
            start_indices_batching_dims=(0,),
        ),
        slice_sizes=(1, 1),
        mode=lax.GatherScatterMode.PROMISE_IN_BOUNDS,
    )


def turned(rows):
    pad = jnp.zeros((LANES - rows.shape[0], LANES), rows.dtype)
    return jnp.concatenate([rows, pad], axis=0).T


def rows_of(values, count):
    width = values[0].shape[1]
    below = count - sum(v.shape[0] for v in values)
    pad = [jnp.zeros((below, width), jnp.float32)] if below else []
    return jnp.concatenate(list(values) + pad, axis=0)


def prepare_kernel(n_stars, pos, vel, acc, jerk, mass, levels, first, second, column_out, row_out, own_out):
    s_dev = pos.shape[1]
    last = -BASE_STEP * jnp.exp2(-levels[...].astype(jnp.float32))
    states = jnp.concatenate([pos[...], vel[...], acc[...], jerk[...]], axis=0)
    weights = mass[...] / n_stars
    room = first.shape[1] + second.shape[1]
    lists = [first[...].astype(jnp.float32), second[...].astype(jnp.float32)]
    if s_dev > room:
        lists.append(jnp.full((1, s_dev - room), -1.0, jnp.float32))
    listed = jnp.concatenate(lists, axis=1)
    column = rows_of([states, last, listed, weights], 16)
    column_out[...] = column
    ahead, moving = predict(states, TIME_FIRST - last)
    ahead_second, moving_second = predict(states, TIME_SECOND - last)
    row = rows_of([ahead, moving, weights, ahead_second, moving_second], CHUNK_ROWS)
    row = jnp.concatenate([row[:, at : at + LANES] for at in range(0, s_dev, LANES)], axis=0)
    for copy in range(row_out.shape[0]):
        row_out[copy] = row
    own_out[...] = rows_of([states, last, weights], 16)


def matching_slots(listed, column, n_src, s_dev):
    ids = listed.astype(jnp.int32)
    n_tgt, width = ids.shape
    valid = ids >= 0
    column_of = jnp.where(valid, (ids >> log2_of(s_dev)) & (n_src - 1), -1)
    row_of = jnp.where(valid, ids >> log2_of(s_dev * n_src), -1)
    cells = jnp.zeros((n_tgt, n_src), jnp.float32)
    for slots in range(n_tgt):
        in_row = (row_of[slots : slots + 1] == iota((n_tgt, width), 0)).astype(jnp.bfloat16)
        in_column = (column_of[slots : slots + 1] == iota((n_src, width), 0)).astype(jnp.bfloat16)
        cells = cells + lax.dot_general(
            in_row, in_column, (((1,), (1,)), ((), ())), preferred_element_type=jnp.float32
        )
    return column_of == column, jnp.max(jnp.sum(cells, axis=0, keepdims=True)), jnp.max(cells)


def slot_numbers(mine):
    n_rows, width = mine.shape
    upto = (iota((width, width), 0) <= iota((width, width), 1)).astype(jnp.bfloat16)
    inside = jnp.dot(mine.astype(jnp.bfloat16), upto, preferred_element_type=jnp.float32)
    totals = jnp.broadcast_to(inside[:, width - 1 : width], (n_rows, LANES))
    place = jnp.zeros((1, LANES), jnp.float32)
    before = []
    for row in range(n_rows):
        before.append(place)
        place = place + totals[row : row + 1]
    start = jnp.concatenate(before, axis=0)[:, 0:1]
    return jnp.where(mine, (inside + start).astype(jnp.int32) - 1, -1), jnp.max(place)


def packed_ids(listed, slot, part):
    n_rows, width = listed.shape
    found = jnp.zeros((LANES, LANES), jnp.float32)
    want = iota((LANES, LANES), 0) + part * LANES
    for row in range(n_rows):
        for chunk in range(width // LANES):
            cut = slice(chunk * LANES, (chunk + 1) * LANES)
            hit = jnp.broadcast_to(slot[row : row + 1, cut], (LANES, LANES)) == want
            found = found + jnp.where(hit, listed[row : row + 1, cut] + 1.0, 0.0)
    ids = jnp.broadcast_to(jnp.sum(found, axis=1, keepdims=True) - 1.0, (LANES, LANES))
    return ids.T[0:1]


def target_facts(number, held, my_row, n_src):
    n_tgt, _, s_dev = held.shape
    row_bits, per_row = log2_of(s_dev * n_src), s_dev // LANES
    ids = number.astype(jnp.int32)
    lane = jnp.broadcast_to(ids & (LANES - 1), (16, LANES))
    chunk_of = jnp.where(ids >= 0, (ids >> row_bits) * per_row + ((ids & (s_dev - 1)) >> log2_of(LANES)), -1)

    def one_row(row, picked):
        for chunk in range(per_row):
            table = held[row, :, chunk * LANES : (chunk + 1) * LANES]
            picked = jnp.where(chunk_of == row * per_row + chunk, lane_pick(table, lane), picked)
        return picked

    picked = lax.fori_loop(0, n_tgt, one_row, jnp.zeros((16, LANES), jnp.float32), unroll=2)
    key = jnp.where((ids >= 0) & ((ids >> row_bits) == my_row), ids & (s_dev - 1), -1)
    return rows_of([picked[0:13], number, picked[14:15], key.astype(jnp.float32)], 16)


def select_kernel(n_src, slots_first, slots_second, held, target_out, turned_out, info_out):
    s_dev = held.shape[2]
    my_row, my_column = lax.axis_index("tgt"), lax.axis_index(SRC)
    listed = held[:, 13, :]
    first, second = listed[:, :slots_first], listed[:, slots_first : slots_first + slots_second]
    mine, most_first, most_own = matching_slots(first, my_column, n_src, s_dev)
    _, most_second, _ = matching_slots(second, my_column, n_src, s_dev)
    slot, count = slot_numbers(mine)
    count = jnp.minimum(count.astype(jnp.int32), FIRST_ROOM)
    info_out[0] = count
    fits = (most_first <= FIRST_ROOM) & (most_second <= SECOND_ROOM) & (most_own <= OWN_ROOM)
    info_out[1] = fits.astype(jnp.int32)

    def fill(part):
        facts = target_facts(packed_ids(first, slot, part), held, my_row, n_src)
        ahead, moving = predict(facts[0:12], TIME_FIRST - facts[12:13])
        cut = slice(part * LANES, (part + 1) * LANES)
        target_out[:, cut] = facts
        turned_out[cut, :] = turned(rows_of([ahead, moving, facts[15:16], facts[13:14]], 8))

    fill(0)
    for part in range(1, FIRST_ROOM // LANES):
        pl.when(count > part * LANES)(functools.partial(fill, part))

        @pl.when(count <= part * LANES)
        def _():
            cut = slice(part * LANES, (part + 1) * LANES)
            target_out[:, cut] = jnp.full((16, LANES), -1.0, jnp.float32)
            turned_out[cut, :] = jnp.full((LANES, LANES), -1.0, jnp.float32)


def found_slots(keys, wanted):
    found = jnp.zeros((LANES, LANES), jnp.float32)
    for part, key in enumerate(keys):
        place = (iota((LANES, LANES), 0) + part * LANES + 1).astype(jnp.float32)
        found = found + jnp.where((key == wanted) & (key >= 0.0), place, 0.0)
    return jnp.sum(found, axis=0, keepdims=True).astype(jnp.int32) - 1


def plan_kernel(n_src, slots_first, slots_second, held, first_target, turned_in, second_out, plan_out, info_out):
    s_dev = held.shape[2]
    my_row, my_column = lax.axis_index("tgt"), lax.axis_index(SRC)
    listed = held[:, 13, slots_first : slots_first + slots_second]
    ids = listed.astype(jnp.int32)
    mine = (ids >= 0) & (((ids >> log2_of(s_dev)) & (n_src - 1)) == my_column)
    slot, count = slot_numbers(mine)
    info_out[0] = jnp.minimum(count.astype(jnp.int32), SECOND_ROOM)
    facts = target_facts(packed_ids(listed, slot, 0), held, my_row, n_src)
    second_out[...] = facts
    parts = FIRST_ROOM // LANES
    columns = [turned_in[part * LANES : (part + 1) * LANES, :] for part in range(parts)]
    keys = [jnp.broadcast_to(c[:, 6:7], (LANES, LANES)) for c in columns]
    numbers = [jnp.broadcast_to(c[:, 7:8], (LANES, LANES)) for c in columns]
    second_keys = [jnp.broadcast_to(facts[15:16], (LANES, LANES)).T]
    plan_out[...] = jnp.full(plan_out.shape, -1, jnp.int32)
    for chunk in range(s_dev // LANES):
        cut = slice(chunk * LANES, (chunk + 1) * LANES)
        star = (iota((1, LANES), 1) + chunk * LANES).astype(jnp.float32)
        plan_out[0:1, cut] = found_slots(keys, star)
        plan_out[1:2, cut] = found_slots(second_keys, star)
    plan_out[2:3, 0:LANES] = found_slots(numbers, facts[13:14])
    own = [(key >= 0.0) for key in keys]
    upto = (iota((LANES, LANES), 1) <= iota((LANES, LANES), 0)).astype(jnp.bfloat16)
    before = jnp.zeros((1, LANES), jnp.float32)
    order = []
    for flags in own:
        inside = jnp.dot(upto, flags.astype(jnp.bfloat16), preferred_element_type=jnp.float32) + before
        order.append(jnp.where(flags, inside - 1.0, -1.0))
        before = inside[LANES - 1 : LANES]
    plan_out[3:4, 0:LANES] = found_slots(order, iota((1, LANES), 1).astype(jnp.float32))


def pair_terms(source, target, own_place=None, key=None):
    rx, ry, rz = (source[j] - target[j] for j in range(3))
    ux, uy, uz = (source[j] - target[j] for j in range(3, 6))
    inverse = lax.rsqrt((rx * rx + ry * ry + rz * rz) + SOFTENING_SQ)
    inverse_sq = inverse * inverse
    weight3 = source[6] * inverse * inverse_sq
    if own_place is not None:
        weight3 = jnp.where(key == own_place, 0.0, weight3)
    closing = (rx * ux + ry * uy + rz * uz) * inverse_sq
    ax, ay, az = rx * weight3, ry * weight3, rz * weight3
    return (ax, ay, az, ux * weight3, uy * weight3, uz * weight3, ax * closing, ay * closing, az * closing)


def added(running, parts):
    return tuple(a + b for a, b in zip(running, parts))


def target_blocks(count, turned_in, sums, visit):
    def one_block(first, tall):
        at = pl.ds(pl.multiple_of(first, 8), tall)
        facts = turned_in[at, :]
        target = [jnp.broadcast_to(facts[:, j : j + 1], (tall, LANES)) for j in range(6)]
        key = jnp.broadcast_to(facts[:, 6:7], (tall, LANES))
        running = visit(tall, target, key, (jnp.zeros((tall, LANES), jnp.float32),) * 9)
        totals = [running[j] for j in range(3)] + [running[3 + j] - 3.0 * running[6 + j] for j in range(3)]
        lanes = iota((tall, LANES), 1)
        packed = sums[at, :]
        for j in range(6):
            total = jnp.broadcast_to(jnp.sum(totals[j], axis=1, keepdims=True), (tall, LANES))
            packed = packed + jnp.where(lanes == j, total, 0.0)
        sums[at, :] = packed

    tall_blocks = (count + 7) // 16
    pl.loop(0, tall_blocks)(lambda block: one_block(block * 16, 16))
    pl.when(count > tall_blocks * 16)(lambda: one_block(tall_blocks * 16, 8))


def row_sums(count, stars, first_row, turned_in, sums):
    _, n_z, height, _ = stars.shape
    my_z, my_core = lax.axis_index("z"), lax.axis_index("core")
    rows = [first_row + j for j in range(6)] + [6]
    sums[...] = jnp.zeros_like(sums)

    def visit(tall, target, key, running):
        def segment(core, which, running, own=False):
            for chunk in range(height // CHUNK_ROWS):
                at = chunk * CHUNK_ROWS
                source = [jnp.broadcast_to(stars[core, which, at + j : at + j + 1, :], (tall, LANES)) for j in rows]
                place = (iota((tall, LANES), 1) + chunk * LANES).astype(jnp.float32) if own else None
                running = added(running, pair_terms(source, target, place, key))
            return running

        def both(step, running):
            return segment(my_core, jnp.where(step < my_z, step, step + 1), segment(1 - my_core, step, running))

        running = lax.fori_loop(0, n_z - 1, both, running)
        return segment(my_core, my_z, segment(1 - my_core, n_z - 1, running), own=True)

    target_blocks(count, turned_in, sums, visit)


def write_sums(sums, force_out):
    copies, _, room = force_out.shape
    for part in range(room // LANES):
        cut = slice(part * LANES, (part + 1) * LANES)
        rows = sums[cut, :].T[0:8]
        for copy in range(copies):
            force_out[copy, :, cut] = rows


def first_force_kernel(info, stars, turned_in, force_out, sums):
    row_sums(info[0], stars, 0, turned_in, sums)
    write_sums(sums, force_out)


def second_force_kernel(info, stars, turned_in, sums_out):
    row_sums(info[0], stars, 7, turned_in, sums_out)


def update_force_kernel(info, updates, turned_in, sums_in, force_out, sums, stars):
    n_z = updates.shape[1]
    my_z, my_core = lax.axis_index("z"), lax.axis_index("core")
    half = iota((8, LANES), 1) < LANES // 2
    own_half = half[7:8] == (my_core == 0)
    for z in range(n_z):
        both = jnp.where(half, updates[0, z], pltpu.roll(updates[1, z], LANES // 2, axis=1))
        place = jnp.where(own_half & (my_z == z), both[7:8], -2.0)
        stars[z] = jnp.concatenate([both[0:7], place], axis=0)
    sums[...] = sums_in[...]

    def visit(tall, target, key, running):
        def one(z, running):
            source = [jnp.broadcast_to(stars[z, j : j + 1, :], (tall, LANES)) for j in range(8)]
            return added(running, pair_terms(source, target, source[7], key))

        return lax.fori_loop(0, n_z, one, running, unroll=4)

    target_blocks(info[0], turned_in, sums, visit)
    write_sums(sums, force_out)


def summed(received):
    total = received[0]
    for row in range(1, received.shape[0]):
        total = total + received[row]
    return total


def picked_slots(values, slot):
    lane = jnp.broadcast_to(slot & (LANES - 1), (16, LANES))
    new = jnp.zeros((16, LANES), jnp.float32)
    for part in range(values.shape[1] // LANES):
        pick = lane_pick(values[:, part * LANES : (part + 1) * LANES], lane)
        new = jnp.where((slot >> log2_of(LANES)) == part, pick, new)
    return new


def correct_kernel(received, target, second, plan, own, update_out, own_out, second_out, turned_out):
    copies = update_out.shape[0]
    room = received.shape[2]
    s_dev = own.shape[1]
    forces = summed(received)
    states = target[0:12, :]
    span = TIME_FIRST - target[12:13, :]
    ahead, moving = predict(states, span)
    corrected = correct(ahead, moving, states[6:9], states[9:12], span, forces[0:6])
    corrected = rows_of([corrected, jnp.full((1, room), TIME_FIRST, jnp.float32)], 16)
    slot = plan[3:4, 0:LANES]
    old = picked_slots(target[...], slot)
    new = picked_slots(corrected, slot)
    present = slot >= 0
    weight, place = old[14:15], jnp.where(present, old[15:16], -1.0)
    ahead_new, moving_new = predict(new[0:12], TIME_SECOND - new[12:13])
    ahead_old, moving_old = predict(old[0:12], TIME_SECOND - old[12:13])
    arrived = jnp.concatenate([ahead_new, moving_new, weight, place], axis=0)
    left = jnp.concatenate([ahead_old, moving_old, -weight, place], axis=0)
    lane = iota((8, LANES), 1)
    update = jnp.where(lane < OWN_ROOM, arrived, pltpu.roll(left, OWN_ROOM, axis=1))
    update = jnp.where(lane < 2 * OWN_ROOM, update, 0.0)
    for copy in range(copies):
        update_out[copy] = update
    for chunk in range(s_dev // LANES):
        cut = slice(chunk * LANES, (chunk + 1) * LANES)
        slot = plan[0:1, cut]
        own_out[:, cut] = jnp.where(slot >= 0, picked_slots(corrected, slot), own[:, cut])
    other = second[...]
    slot = plan[2:3, 0:LANES]
    states = jnp.where(slot >= 0, picked_slots(corrected, slot), other)
    span = TIME_SECOND - states[12:13]
    ahead, moving = predict(states[0:12], span)
    second_out[...] = rows_of([ahead, moving, states[6:12], span], 16)
    turned_out[...] = turned(rows_of([ahead, moving, other[15:16]], 8))


def finish_kernel(received, second, plan, own, pos_out, vel_out, acc_out, jerk_out):
    forces = summed(received)
    facts = second[...]
    corrected = correct(facts[0:3], facts[3:6], facts[6:9], facts[9:12], facts[12:13], forces[0:6])
    corrected = rows_of([corrected], 16)
    for chunk in range(own.shape[1] // LANES):
        cut = slice(chunk * LANES, (chunk + 1) * LANES)
        slot = plan[1:2, cut]
        new = jnp.where(slot >= 0, picked_slots(corrected, slot), own[:, cut])
        pos_out[:, cut] = new[0:3]
        vel_out[:, cut] = new[3:6]
        acc_out[:, cut] = new[6:9]
        jerk_out[:, cut] = new[9:12]


def f32(*shape):
    return jax.ShapeDtypeStruct(shape, jnp.float32)


INTERPRET = False


def call(kernel, outs, scalars=0, operands=0, scratch=(), smem_out=None):
    smem, vmem = pl.BlockSpec(memory_space=pltpu.SMEM), pl.BlockSpec(memory_space=pltpu.VMEM)
    return pl.pallas_call(
        kernel,
        out_shape=outs,
        in_specs=[smem] * scalars + [vmem] * operands,
        out_specs=tuple(smem if i == smem_out else vmem for i in range(len(outs))),
        scratch_shapes=list(scratch),
        interpret=INTERPRET,
        compiler_params=pltpu.CompilerParams(vmem_limit_bytes=16 << 20),
    )


def exchanged(copies, axis):
    return lax.all_to_all(copies, axis, split_axis=0, concat_axis=0, tiled=True)


def both_cores(near):
    return lax.all_gather(near, "core")


def shards(positions, velocities, accels, jerks, masses, levels, active_first, active_second):
    s_dev = positions.shape[1]
    n_tgt, n_z, n_src = lax.axis_size("tgt"), lax.axis_size("z"), lax.axis_size(SRC)
    n_stars = s_dev * n_tgt * n_src
    scalar = jax.ShapeDtypeStruct((2,), jnp.int32)
    lists = (n_src, active_first.shape[0], active_second.shape[0])
    column, row_copies, own = call(
        functools.partial(prepare_kernel, n_stars), (f32(16, s_dev), f32(n_z, CHUNK_ROWS * s_dev // LANES, LANES), f32(16, s_dev)), 0, 8
    )(
        positions, velocities, accels, jerks, masses.reshape(1, s_dev), levels.reshape(1, s_dev),
        active_first.reshape(1, -1), active_second.reshape(1, -1),
    )
    near = exchanged(row_copies, "z")
    column = lax.all_gather(column, "tgt")
    stars = both_cores(near)
    target, columns, info = call(
        functools.partial(select_kernel, *lists), (f32(16, FIRST_ROOM), f32(FIRST_ROOM, LANES), scalar), 0, 1, smem_out=2
    )(column)
    (partial,) = call(
        first_force_kernel, (f32(n_tgt, 8, FIRST_ROOM),), 1, 2, [pltpu.VMEM((FIRST_ROOM, LANES), jnp.float32)]
    )(info, stars, columns)
    received = exchanged(partial, "tgt")
    second, plan, second_info = call(
        functools.partial(plan_kernel, *lists),
        (f32(16, SECOND_ROOM), jax.ShapeDtypeStruct((8, s_dev), jnp.int32), scalar), 0, 3, smem_out=2,
    )(column, target, columns)
    update, own, second, second_columns = call(
        correct_kernel, (f32(n_z, 8, LANES), f32(16, s_dev), f32(16, SECOND_ROOM), f32(LANES, LANES)), 0, 5
    )(received, target, second, plan, own)
    near_update = exchanged(update, "z")
    (sums,) = call(second_force_kernel, (f32(SECOND_ROOM, LANES),), 1, 2)(second_info, stars, second_columns)
    updates = both_cores(near_update)
    (partial,) = call(
        update_force_kernel, (f32(n_tgt, 8, SECOND_ROOM),), 1, 3,
        [pltpu.VMEM((SECOND_ROOM, LANES), jnp.float32), pltpu.VMEM((n_z, 8, LANES), jnp.float32)],
    )(second_info, updates, second_columns, sums)
    received = exchanged(partial, "tgt")

    def by_columns(received, second, plan, own, *inputs):
        return tuple(call(finish_kernel, (f32(3, s_dev),) * 4, 0, 4)(received, second, plan, own))

    def anywhere(received, second, plan, own, *inputs):
        return whole_program(*inputs)

    inputs = (positions, velocities, accels, jerks, masses, levels, active_first, active_second)
    return lax.cond(info[1] == 1, by_columns, anywhere, received, second, plan, own, *inputs)


def solution(mesh):
    n_tgt, n_src = mesh.devices.shape
    finer = Mesh(mesh.devices.reshape(n_tgt, n_src // 2, 2), ("tgt", "z", "core"))
    stars = ("tgt", "z", "core")
    vector, scalar = P(None, stars), P(stars)
    return jax.shard_map(
        shards,
        mesh=finer,
        in_specs=(vector, vector, vector, vector, scalar, scalar, P("tgt"), P("tgt")),
        out_specs=(vector,) * 4,
        check_vma=False,
    )
```

```python
import functools

import jax
import jax.numpy as jnp
from jax import lax
from jax.experimental import pallas as pl
from jax.experimental.pallas import tpu as pltpu
from jax.sharding import Mesh
from jax.sharding import PartitionSpec as P

TILE = 128
LEVELS = 4
LANES = 128
FIRST_ROOM = 256
SECOND_ROOM = 128
OWN_ROOM = 32
CHUNK_ROWS = 14

SOFTENING_SQ = 0.0001
BASE_STEP = 0.5
TIME_FIRST = 0.0
TIME_SECOND = BASE_STEP / (1 << LEVELS)
SRC = ("z", "core")


def sent_to_all(shard, axis):
    copies = jnp.broadcast_to(shard, (lax.axis_size(axis), *shard.shape))
    return lax.all_to_all(copies, axis, split_axis=0, concat_axis=0, tiled=True)


def laid_out(tiles, dim):
    dims = list(tiles.shape[1:])
    dims[dim] *= tiles.shape[0]
    return jnp.moveaxis(tiles, 0, dim).reshape(dims)


def gathered_copies(shard, axis, dim):
    tiles = sent_to_all(shard, axis)
    return laid_out(tiles, dim)


def over_pieces(shard, axis):
    return lax.all_gather(shard, axis).sum(0)


def taken_together(shard, axis):
    return sent_to_all(shard, axis).sum(axis=0)


def predict(states, span):
    ahead_pos = states[0:3] + span * (
        states[3:6] + span * (states[6:9] * 0.5 + span * states[9:12] / 6.0)
    )
    moving = states[3:6] + span * (states[6:9] + span * states[9:12] * 0.5)
    return (ahead_pos, moving)


def pair_block(tile_place, tile_speed, tile_ident, sources, source_ident):
    offset = sources[0:3, None, :] - tile_place[:, :, None]
    motion = sources[3:6, None, :] - tile_speed[:, :, None]
    dist_sq = jnp.sum(offset * offset, axis=0) + SOFTENING_SQ
    inverse = lax.rsqrt(dist_sq)
    inverse_sq = inverse * inverse
    weight3 = jnp.where(
        source_ident[None, :] == tile_ident[:, None],
        0.0,
        sources[6][None, :] * inverse_sq * inverse,
    )
    closing = jnp.sum(offset * motion, axis=0)
    attract = jnp.sum(offset * weight3, axis=2)
    change = jnp.sum(motion * weight3 - 3.0 * (closing * inverse_sq * weight3) * offset, axis=2)
    return jnp.concatenate([attract, change], axis=0)


def correct(ahead_pos, moving, old_accel, old_jolt, span, forces):
    new_acc = forces[0:3]
    new_jolt = forces[3:6]
    second_term = -6.0 * (old_accel - new_acc) - span * (4.0 * old_jolt + 2.0 * new_jolt)
    third_term = 12.0 * (old_accel - new_acc) + 6.0 * span * (old_jolt + new_jolt)
    new_place = ahead_pos + span * span * (second_term / 24.0 + third_term / 120.0)
    new_speed = moving + span * (second_term / 6.0 + third_term / 24.0)
    return jnp.concatenate([new_place, new_speed, new_acc, new_jolt], axis=0)


def tile_forces(held, tgt_ahead, tgt_moving, slot_ids, tiles_used, shard_part, idents):
    length = shard_part.shape[1]
    block_len = length
    while block_len > 2048 and block_len % 2 == 0:
        block_len = block_len // 2
    block_count = length // block_len
    src_blocks = shard_part.reshape(7, block_count, block_len).transpose(1, 0, 2)
    ident_blocks = idents.reshape(block_count, block_len)

    def one_tile(tile_no, carried):
        place_tile = lax.dynamic_slice_in_dim(tgt_ahead, tile_no * TILE, TILE, 1)
        speed_tile = lax.dynamic_slice_in_dim(tgt_moving, tile_no * TILE, TILE, 1)
        ident_tile = lax.dynamic_slice_in_dim(slot_ids, tile_no * TILE, TILE, 0)

        def add_block(running, source_pair):
            return (
                running
                + pair_block(place_tile, speed_tile, ident_tile, source_pair[0], source_pair[1]),
                None,
            )

        running, _ = lax.scan(
            add_block, jnp.zeros((6, TILE), jnp.float32), (src_blocks, ident_blocks)
        )
        before = lax.dynamic_slice_in_dim(carried, tile_no * TILE, TILE, 1)
        return lax.dynamic_update_slice_in_dim(carried, before + running, tile_no * TILE, 1)

    return lax.fori_loop(0, tiles_used, one_tile, held)


def advance(states, last_time, weights, active, now_time, s_dev, n_tgt, n_src, my_row, my_column):
    slot_count = active.shape[0]
    own_first = (my_row * n_src + my_column) * s_dev
    listed = gathered_copies(active, "tgt", 0)
    span_all = now_time - last_time
    my_slots = lax.dynamic_slice_in_dim(listed, my_row * slot_count, slot_count, 0)
    filled = jnp.sum((my_slots >= 0).astype(jnp.int32))
    tiles_used = (filled + TILE - 1) // TILE
    local_at = listed - own_first
    is_owned = (listed >= 0) & (local_at >= 0) & (local_at < s_dev)
    stacked = jnp.concatenate([states, span_all[None, :], weights[None, :]], axis=0)
    column_all = gathered_copies(stacked, "tgt", 1)
    owner_col = my_slots // s_dev % n_src
    places = my_slots // (s_dev * n_src) * s_dev + my_slots % s_dev
    mine_owned = (my_slots >= 0) & (owner_col == my_column)
    chosen = jnp.take(column_all[0:13], jnp.clip(places, 0, n_tgt * s_dev - 1), axis=1)
    partial_rows = jnp.where(mine_owned[None, :], chosen, 0.0)
    ahead_pos, moving = predict(column_all[0:12], column_all[12:13])
    sources = jnp.concatenate([ahead_pos, moving, column_all[13:14]], axis=0)
    target = over_pieces(partial_rows, SRC)
    tgt_ahead, tgt_moving = predict(target[0:12], target[12:13])
    zero_forces = jnp.zeros((6, slot_count), jnp.float32)
    columns = jnp.arange(sources.shape[1], dtype=jnp.int32)
    idents = columns // s_dev * (s_dev * n_src) + my_column * s_dev + columns % s_dev
    partial_forces = tile_forces(
        zero_forces, tgt_ahead, tgt_moving, my_slots, tiles_used, sources, idents
    )
    forces = taken_together(partial_forces, SRC)
    corrected = correct(tgt_ahead, tgt_moving, target[6:9], target[9:12], target[12:13], forces)
    returned = gathered_copies(corrected, "tgt", 1)
    write_at = jnp.where(is_owned, local_at, s_dev)
    states = states.at[:, write_at].set(returned, mode="drop")
    last_time = last_time.at[write_at].set(now_time, mode="drop")
    return (states, last_time)


def whole_program(positions, velocities, accels, jerks, masses, levels, active_first, active_second):
    s_dev = positions.shape[1]
    n_tgt = lax.axis_size("tgt")
    n_src = lax.axis_size(SRC)
    my_row = lax.axis_index("tgt")
    my_column = lax.axis_index(SRC)
    weights = masses / (s_dev * n_tgt * n_src)
    states = jnp.concatenate([positions, velocities, accels, jerks], axis=0)
    last_time = -BASE_STEP * jnp.exp2(-levels.astype(jnp.float32))
    for now_time, active in ((TIME_FIRST, active_first), (TIME_SECOND, active_second)):
        states, last_time = advance(
            states, last_time, weights, active, now_time, s_dev, n_tgt, n_src, my_row, my_column
        )
    return (states[0:3], states[3:6], states[6:9], states[9:12])


def log2_of(size):
    assert size & (size - 1) == 0, "size"
    return size.bit_length() - 1


def iota(shape, dim):
    return lax.broadcasted_iota(jnp.int32, shape, dim)


def lane_pick(table, lanes):
    return lax.gather(
        table,
        lanes[:, :, None],
        lax.GatherDimensionNumbers(
            offset_dims=(),
            collapsed_slice_dims=(1,),
            start_index_map=(1,),
            operand_batching_dims=(0,),
            start_indices_batching_dims=(0,),
        ),
        slice_sizes=(1, 1),
        mode=lax.GatherScatterMode.PROMISE_IN_BOUNDS,
    )


def turned(rows):
    pad = jnp.zeros((LANES - rows.shape[0], LANES), rows.dtype)
    return jnp.concatenate([rows, pad], axis=0).T


def rows_of(values, count):
    width = values[0].shape[1]
    below = count - sum(v.shape[0] for v in values)
    pad = [jnp.zeros((below, width), jnp.float32)] if below else []
    return jnp.concatenate(list(values) + pad, axis=0)


def prepare_kernel(n_stars, pos, vel, acc, jerk, mass, levels, first, second, column_out, row_out, own_out):
    s_dev = pos.shape[1]
    last = -BASE_STEP * jnp.exp2(-levels[...].astype(jnp.float32))
    states = jnp.concatenate([pos[...], vel[...], acc[...], jerk[...]], axis=0)
    weights = mass[...] / n_stars
    room = first.shape[1] + second.shape[1]
    lists = [first[...].astype(jnp.float32), second[...].astype(jnp.float32)]
    if s_dev > room:
        lists.append(jnp.full((1, s_dev - room), -1.0, jnp.float32))
    listed = jnp.concatenate(lists, axis=1)
    column = rows_of([states, last, listed, weights], 16)
    column_out[...] = column
    ahead, moving = predict(states, TIME_FIRST - last)
    ahead_second, moving_second = predict(states, TIME_SECOND - last)
    row = rows_of([ahead, moving, weights, ahead_second, moving_second], CHUNK_ROWS)
    row = jnp.concatenate([row[:, at : at + LANES] for at in range(0, s_dev, LANES)], axis=0)
    for copy in range(row_out.shape[0]):
        row_out[copy] = row
    own_out[...] = rows_of([states, last, weights], 16)


def in_column(listed, column, n_src, s_dev):
    ids = listed.astype(jnp.int32)
    return (ids >= 0) & (((ids >> log2_of(s_dev)) & (n_src - 1)) == column)


def most_listed(listed, n_src, s_dev):
    ids = listed.astype(jnp.int32)
    n_tgt, width = ids.shape
    valid = ids >= 0
    column_of = jnp.where(valid, (ids >> log2_of(s_dev)) & (n_src - 1), -1)
    row_of = jnp.where(valid, ids >> log2_of(s_dev * n_src), -1)
    cells = jnp.zeros((n_tgt, n_src), jnp.float32)
    for slots in range(n_tgt):
        in_row = (row_of[slots : slots + 1] == iota((n_tgt, width), 0)).astype(jnp.bfloat16)
        in_col = (column_of[slots : slots + 1] == iota((n_src, width), 0)).astype(jnp.bfloat16)
        cells = cells + lax.dot_general(
            in_row, in_col, (((1,), (1,)), ((), ())), preferred_element_type=jnp.float32
        )
    return jnp.max(jnp.sum(cells, axis=0, keepdims=True)), jnp.max(cells)


def slot_numbers(mine):
    n_rows, width = mine.shape
    upto = (iota((width, width), 0) <= iota((width, width), 1)).astype(jnp.bfloat16)
    inside = jnp.dot(mine.astype(jnp.bfloat16), upto, preferred_element_type=jnp.float32)
    totals = jnp.broadcast_to(inside[:, width - 1 : width], (n_rows, LANES))
    place = jnp.zeros((1, LANES), jnp.float32)
    before = []
    for row in range(n_rows):
        before.append(place)
        place = place + totals[row : row + 1]
    start = jnp.concatenate(before, axis=0)[:, 0:1]
    return jnp.where(mine, (inside + start).astype(jnp.int32) - 1, -1), jnp.max(place)


def packed_ids(listed, slot, part):
    n_rows, width = listed.shape
    found = jnp.zeros((LANES, LANES), jnp.float32)
    want = iota((LANES, LANES), 0) + part * LANES
    for row in range(n_rows):
        for chunk in range(width // LANES):
            cut = slice(chunk * LANES, (chunk + 1) * LANES)
            hit = jnp.broadcast_to(slot[row : row + 1, cut], (LANES, LANES)) == want
            found = found + jnp.where(hit, listed[row : row + 1, cut] + 1.0, 0.0)
    ids = jnp.broadcast_to(jnp.sum(found, axis=1, keepdims=True) - 1.0, (LANES, LANES))
    return ids.T[0:1]


def target_facts(number, held, my_row, n_src):
    n_tgt, _, s_dev = held.shape
    row_bits, per_row = log2_of(s_dev * n_src), s_dev // LANES
    ids = number.astype(jnp.int32)
    lane = jnp.broadcast_to(ids & (LANES - 1), (16, LANES))
    chunk_of = jnp.where(ids >= 0, (ids >> row_bits) * per_row + ((ids & (s_dev - 1)) >> log2_of(LANES)), -1)

    def one_row(row, picked):
        for chunk in range(per_row):
            table = held[row, :, chunk * LANES : (chunk + 1) * LANES]
            picked = jnp.where(chunk_of == row * per_row + chunk, lane_pick(table, lane), picked)
        return picked

    picked = lax.fori_loop(0, n_tgt, one_row, jnp.zeros((16, LANES), jnp.float32), unroll=2)
    key = jnp.where((ids >= 0) & ((ids >> row_bits) == my_row), ids & (s_dev - 1), -1)
    return rows_of([picked[0:13], number, picked[14:15], key.astype(jnp.float32)], 16)


def select_kernel(n_src, slots_first, slots_second, held, target_out, turned_out, info_out):
    s_dev = held.shape[2]
    my_row, my_column = lax.axis_index("tgt"), lax.axis_index(SRC)
    listed = held[:, 13, :]
    first = listed[:, :slots_first]
    slot, count = slot_numbers(in_column(first, my_column, n_src, s_dev))
    count = jnp.minimum(count.astype(jnp.int32), FIRST_ROOM)
    info_out[0] = count
    info_out[1] = 0

    def fill(part):
        facts = target_facts(packed_ids(first, slot, part), held, my_row, n_src)
        ahead, moving = predict(facts[0:12], TIME_FIRST - facts[12:13])
        cut = slice(part * LANES, (part + 1) * LANES)
        target_out[:, cut] = facts
        turned_out[cut, :] = turned(rows_of([ahead, moving, facts[15:16], facts[13:14]], 8))

    fill(0)
    for part in range(1, FIRST_ROOM // LANES):
        pl.when(count > part * LANES)(functools.partial(fill, part))

        @pl.when(count <= part * LANES)
        def _():
            cut = slice(part * LANES, (part + 1) * LANES)
            target_out[:, cut] = jnp.full((16, LANES), -1.0, jnp.float32)
            turned_out[cut, :] = jnp.full((LANES, LANES), -1.0, jnp.float32)


def found_slots(keys, wanted):
    found = jnp.zeros((LANES, LANES), jnp.float32)
    for part, key in enumerate(keys):
        place = (iota((LANES, LANES), 0) + part * LANES + 1).astype(jnp.float32)
        found = found + jnp.where((key == wanted) & (key >= 0.0), place, 0.0)
    return jnp.sum(found, axis=0, keepdims=True).astype(jnp.int32) - 1


def plan_kernel(n_src, slots_first, slots_second, held, first_target, turned_in, second_out, plan_out, info_out):
    s_dev = held.shape[2]
    my_row, my_column = lax.axis_index("tgt"), lax.axis_index(SRC)
    lists = held[:, 13, :]
    first, listed = lists[:, :slots_first], lists[:, slots_first : slots_first + slots_second]
    most_first, most_own = most_listed(first, n_src, s_dev)
    most_second, _ = most_listed(listed, n_src, s_dev)
    fits = (most_first <= FIRST_ROOM) & (most_second <= SECOND_ROOM) & (most_own <= OWN_ROOM)
    info_out[1] = fits.astype(jnp.int32)
    slot, count = slot_numbers(in_column(listed, my_column, n_src, s_dev))
    info_out[0] = jnp.minimum(count.astype(jnp.int32), SECOND_ROOM)
    facts = target_facts(packed_ids(listed, slot, 0), held, my_row, n_src)
    second_out[...] = facts
    parts = FIRST_ROOM // LANES
    columns = [turned_in[part * LANES : (part + 1) * LANES, :] for part in range(parts)]
    keys = [jnp.broadcast_to(c[:, 6:7], (LANES, LANES)) for c in columns]
    numbers = [jnp.broadcast_to(c[:, 7:8], (LANES, LANES)) for c in columns]
    second_keys = [jnp.broadcast_to(facts[15:16], (LANES, LANES)).T]
    plan_out[...] = jnp.full(plan_out.shape, -1, jnp.int32)
    for chunk in range(s_dev // LANES):
        cut = slice(chunk * LANES, (chunk + 1) * LANES)
        star = (iota((1, LANES), 1) + chunk * LANES).astype(jnp.float32)
        plan_out[0:1, cut] = found_slots(keys, star)
        plan_out[1:2, cut] = found_slots(second_keys, star)
    plan_out[2:3, 0:LANES] = found_slots(numbers, facts[13:14])
    own = [(key >= 0.0) for key in keys]
    upto = (iota((LANES, LANES), 1) <= iota((LANES, LANES), 0)).astype(jnp.bfloat16)
    before = jnp.zeros((1, LANES), jnp.float32)
    order = []
    for flags in own:
        inside = jnp.dot(upto, flags.astype(jnp.bfloat16), preferred_element_type=jnp.float32) + before
        order.append(jnp.where(flags, inside - 1.0, -1.0))
        before = inside[LANES - 1 : LANES]
    plan_out[3:4, 0:LANES] = found_slots(order, iota((1, LANES), 1).astype(jnp.float32))


def pair_terms(source, target, own_place=None, key=None):
    rx, ry, rz = (source[j] - target[j] for j in range(3))
    ux, uy, uz = (source[j] - target[j] for j in range(3, 6))
    inverse = lax.rsqrt((rx * rx + ry * ry + rz * rz) + SOFTENING_SQ)
    inverse_sq = inverse * inverse
    weight3 = source[6] * inverse * inverse_sq
    if own_place is not None:
        weight3 = jnp.where(key == own_place, 0.0, weight3)
    closing = (rx * ux + ry * uy + rz * uz) * inverse_sq
    ax, ay, az = rx * weight3, ry * weight3, rz * weight3
    return (ax, ay, az, ux * weight3, uy * weight3, uz * weight3, ax * closing, ay * closing, az * closing)


def added(running, parts):
    return tuple(a + b for a, b in zip(running, parts))


def target_blocks(count, turned_in, sums, visit):
    def one_block(first, tall):
        at = pl.ds(pl.multiple_of(first, 8), tall)
        facts = turned_in[at, :]
        target = [jnp.broadcast_to(facts[:, j : j + 1], (tall, LANES)) for j in range(6)]
        key = jnp.broadcast_to(facts[:, 6:7], (tall, LANES))
        running = visit(tall, target, key, (jnp.zeros((tall, LANES), jnp.float32),) * 9)
        totals = [running[j] for j in range(3)] + [running[3 + j] - 3.0 * running[6 + j] for j in range(3)]
        lanes = iota((tall, LANES), 1)
        packed = sums[at, :]
        for j in range(6):
            total = jnp.broadcast_to(jnp.sum(totals[j], axis=1, keepdims=True), (tall, LANES))
            packed = packed + jnp.where(lanes == j, total, 0.0)
        sums[at, :] = packed

    tall_blocks = (count + 7) // 16
    pl.loop(0, tall_blocks)(lambda block: one_block(block * 16, 16))
    pl.when(count > tall_blocks * 16)(lambda: one_block(tall_blocks * 16, 8))


def row_sums(count, stars, first_row, turned_in, sums):
    _, n_z, height, _ = stars.shape
    my_z, my_core = lax.axis_index("z"), lax.axis_index("core")
    rows = [first_row + j for j in range(6)] + [6]
    sums[...] = jnp.zeros_like(sums)

    def visit(tall, target, key, running):
        def segment(core, which, running, own=False):
            for chunk in range(height // CHUNK_ROWS):
                at = chunk * CHUNK_ROWS
                source = [jnp.broadcast_to(stars[core, which, at + j : at + j + 1, :], (tall, LANES)) for j in rows]
                place = (iota((tall, LANES), 1) + chunk * LANES).astype(jnp.float32) if own else None
                running = added(running, pair_terms(source, target, place, key))
            return running

        def both(step, running):
            return segment(my_core, jnp.where(step < my_z, step, step + 1), segment(1 - my_core, step, running))

        running = lax.fori_loop(0, n_z - 1, both, running)
        return segment(my_core, my_z, segment(1 - my_core, n_z - 1, running), own=True)

    target_blocks(count, turned_in, sums, visit)


def write_sums(sums, force_out):
    copies, _, room = force_out.shape
    for part in range(room // LANES):
        cut = slice(part * LANES, (part + 1) * LANES)
        rows = sums[cut, :].T[0:8]
        for copy in range(copies):
            force_out[copy, :, cut] = rows


def first_force_kernel(info, stars, turned_in, force_out, sums):
    row_sums(info[0], stars, 0, turned_in, sums)
    write_sums(sums, force_out)


def second_force_kernel(info, stars, turned_in, sums_out):
    row_sums(info[0], stars, 7, turned_in, sums_out)


def update_force_kernel(info, updates, turned_in, sums_in, force_out, sums, stars):
    n_z = updates.shape[1]
    my_z, my_core = lax.axis_index("z"), lax.axis_index("core")
    half = iota((8, LANES), 1) < LANES // 2
    own_half = half[7:8] == (my_core == 0)
    for z in range(n_z):
        both = jnp.where(half, updates[0, z], pltpu.roll(updates[1, z], LANES // 2, axis=1))
        place = jnp.where(own_half & (my_z == z), both[7:8], -2.0)
        stars[z] = jnp.concatenate([both[0:7], place], axis=0)
    sums[...] = sums_in[...]

    def visit(tall, target, key, running):
        def one(z, running):
            source = [jnp.broadcast_to(stars[z, j : j + 1, :], (tall, LANES)) for j in range(8)]
            return added(running, pair_terms(source, target, source[7], key))

        return lax.fori_loop(0, n_z, one, running, unroll=4)

    target_blocks(info[0], turned_in, sums, visit)
    write_sums(sums, force_out)


def summed(received):
    total = received[0]
    for row in range(1, received.shape[0]):
        total = total + received[row]
    return total


def picked_slots(values, slot):
    lane = jnp.broadcast_to(slot & (LANES - 1), (16, LANES))
    new = jnp.zeros((16, LANES), jnp.float32)
    for part in range(values.shape[1] // LANES):
        pick = lane_pick(values[:, part * LANES : (part + 1) * LANES], lane)
        new = jnp.where((slot >> log2_of(LANES)) == part, pick, new)
    return new


def correct_kernel(received, target, second, plan, own, update_out, own_out, second_out, turned_out):
    copies = update_out.shape[0]
    room = received.shape[2]
    s_dev = own.shape[1]
    forces = summed(received)
    states = target[0:12, :]
    span = TIME_FIRST - target[12:13, :]
    ahead, moving = predict(states, span)
    corrected = correct(ahead, moving, states[6:9], states[9:12], span, forces[0:6])
    corrected = rows_of([corrected, jnp.full((1, room), TIME_FIRST, jnp.float32)], 16)
    slot = plan[3:4, 0:LANES]
    old = picked_slots(target[...], slot)
    new = picked_slots(corrected, slot)
    present = slot >= 0
    weight, place = old[14:15], jnp.where(present, old[15:16], -1.0)
    ahead_new, moving_new = predict(new[0:12], TIME_SECOND - new[12:13])
    ahead_old, moving_old = predict(old[0:12], TIME_SECOND - old[12:13])
    arrived = jnp.concatenate([ahead_new, moving_new, weight, place], axis=0)
    left = jnp.concatenate([ahead_old, moving_old, -weight, place], axis=0)
    lane = iota((8, LANES), 1)
    update = jnp.where(lane < OWN_ROOM, arrived, pltpu.roll(left, OWN_ROOM, axis=1))
    update = jnp.where(lane < 2 * OWN_ROOM, update, 0.0)
    for copy in range(copies):
        update_out[copy] = update
    for chunk in range(s_dev // LANES):
        cut = slice(chunk * LANES, (chunk + 1) * LANES)
        slot = plan[0:1, cut]
        own_out[:, cut] = jnp.where(slot >= 0, picked_slots(corrected, slot), own[:, cut])
    other = second[...]
    slot = plan[2:3, 0:LANES]
    states = jnp.where(slot >= 0, picked_slots(corrected, slot), other)
    span = TIME_SECOND - states[12:13]
    ahead, moving = predict(states[0:12], span)
    second_out[...] = rows_of([ahead, moving, states[6:12], span], 16)
    turned_out[...] = turned(rows_of([ahead, moving, other[15:16]], 8))


def finish_kernel(received, second, plan, own, pos_out, vel_out, acc_out, jerk_out):
    forces = summed(received)
    facts = second[...]
    corrected = correct(facts[0:3], facts[3:6], facts[6:9], facts[9:12], facts[12:13], forces[0:6])
    corrected = rows_of([corrected], 16)
    for chunk in range(own.shape[1] // LANES):
        cut = slice(chunk * LANES, (chunk + 1) * LANES)
        slot = plan[1:2, cut]
        new = jnp.where(slot >= 0, picked_slots(corrected, slot), own[:, cut])
        pos_out[:, cut] = new[0:3]
        vel_out[:, cut] = new[3:6]
        acc_out[:, cut] = new[6:9]
        jerk_out[:, cut] = new[9:12]


def f32(*shape):
    return jax.ShapeDtypeStruct(shape, jnp.float32)


INTERPRET = False


def call(kernel, outs, scalars=0, operands=0, scratch=(), smem_out=None):
    smem, vmem = pl.BlockSpec(memory_space=pltpu.SMEM), pl.BlockSpec(memory_space=pltpu.VMEM)
    return pl.pallas_call(
        kernel,
        out_shape=outs,
        in_specs=[smem] * scalars + [vmem] * operands,
        out_specs=tuple(smem if i == smem_out else vmem for i in range(len(outs))),
        scratch_shapes=list(scratch),
        interpret=INTERPRET,
        compiler_params=pltpu.CompilerParams(vmem_limit_bytes=16 << 20),
    )


def exchanged(copies, axis):
    return lax.all_to_all(copies, axis, split_axis=0, concat_axis=0, tiled=True)


def both_cores(near):
    return lax.all_gather(near, "core")


def shards(positions, velocities, accels, jerks, masses, levels, active_first, active_second):
    s_dev = positions.shape[1]
    n_tgt, n_z, n_src = lax.axis_size("tgt"), lax.axis_size("z"), lax.axis_size(SRC)
    n_stars = s_dev * n_tgt * n_src
    scalar = jax.ShapeDtypeStruct((2,), jnp.int32)
    lists = (n_src, active_first.shape[0], active_second.shape[0])
    column, row_copies, own = call(
        functools.partial(prepare_kernel, n_stars), (f32(16, s_dev), f32(n_z, CHUNK_ROWS * s_dev // LANES, LANES), f32(16, s_dev)), 0, 8
    )(
        positions, velocities, accels, jerks, masses.reshape(1, s_dev), levels.reshape(1, s_dev),
        active_first.reshape(1, -1), active_second.reshape(1, -1),
    )
    near = exchanged(row_copies, "z")
    column = lax.all_gather(column, "tgt")
    stars = both_cores(near)
    target, columns, info = call(
        functools.partial(select_kernel, *lists), (f32(16, FIRST_ROOM), f32(FIRST_ROOM, LANES), scalar), 0, 1, smem_out=2
    )(column)
    (partial,) = call(
        first_force_kernel, (f32(n_tgt, 8, FIRST_ROOM),), 1, 2, [pltpu.VMEM((FIRST_ROOM, LANES), jnp.float32)]
    )(info, stars, columns)
    received = exchanged(partial, "tgt")
    second, plan, second_info = call(
        functools.partial(plan_kernel, *lists),
        (f32(16, SECOND_ROOM), jax.ShapeDtypeStruct((8, s_dev), jnp.int32), scalar), 0, 3, smem_out=2,
    )(column, target, columns)
    update, own, second, second_columns = call(
        correct_kernel, (f32(n_z, 8, LANES), f32(16, s_dev), f32(16, SECOND_ROOM), f32(LANES, LANES)), 0, 5
    )(received, target, second, plan, own)
    near_update = exchanged(update, "z")
    (sums,) = call(second_force_kernel, (f32(SECOND_ROOM, LANES),), 1, 2)(second_info, stars, second_columns)
    updates = both_cores(near_update)
    (partial,) = call(
        update_force_kernel, (f32(n_tgt, 8, SECOND_ROOM),), 1, 3,
        [pltpu.VMEM((SECOND_ROOM, LANES), jnp.float32), pltpu.VMEM((n_z, 8, LANES), jnp.float32)],
    )(second_info, updates, second_columns, sums)
    received = exchanged(partial, "tgt")

    def by_columns(received, second, plan, own, *inputs):
        return tuple(call(finish_kernel, (f32(3, s_dev),) * 4, 0, 4)(received, second, plan, own))

    def anywhere(received, second, plan, own, *inputs):
        return whole_program(*inputs)

    inputs = (positions, velocities, accels, jerks, masses, levels, active_first, active_second)
    return lax.cond(second_info[1] == 1, by_columns, anywhere, received, second, plan, own, *inputs)


def solution(mesh):
    n_tgt, n_src = mesh.devices.shape
    finer = Mesh(mesh.devices.reshape(n_tgt, n_src // 2, 2), ("tgt", "z", "core"))
    stars = ("tgt", "z", "core")
    vector, scalar = P(None, stars), P(stars)
    return jax.shard_map(
        shards,
        mesh=finer,
        in_specs=(vector, vector, vector, vector, scalar, scalar, P("tgt"), P("tgt")),
        out_specs=(vector,) * 4,
        check_vma=False,
    )
```

```python
import functools

import jax
import jax.numpy as jnp
from jax import lax
from jax.experimental import pallas as pl
from jax.experimental.pallas import tpu as pltpu
from jax.sharding import Mesh
from jax.sharding import PartitionSpec as P

TILE = 128
LEVELS = 4
LANES = 128
FIRST_ROOM = 256
SECOND_ROOM = 128
OWN_ROOM = 32
CHUNK_ROWS = 14

SOFTENING_SQ = 0.0001
BASE_STEP = 0.5
TIME_FIRST = 0.0
TIME_SECOND = BASE_STEP / (1 << LEVELS)
SRC = ("z", "core")


def sent_to_all(shard, axis):
    copies = jnp.broadcast_to(shard, (lax.axis_size(axis), *shard.shape))
    return lax.all_to_all(copies, axis, split_axis=0, concat_axis=0, tiled=True)


def laid_out(tiles, dim):
    dims = list(tiles.shape[1:])
    dims[dim] *= tiles.shape[0]
    return jnp.moveaxis(tiles, 0, dim).reshape(dims)


def gathered_copies(shard, axis, dim):
    tiles = sent_to_all(shard, axis)
    return laid_out(tiles, dim)


def over_pieces(shard, axis):
    return lax.all_gather(shard, axis).sum(0)


def taken_together(shard, axis):
    return sent_to_all(shard, axis).sum(axis=0)


def predict(states, span):
    ahead_pos = states[0:3] + span * (
        states[3:6] + span * (states[6:9] * 0.5 + span * states[9:12] / 6.0)
    )
    moving = states[3:6] + span * (states[6:9] + span * states[9:12] * 0.5)
    return (ahead_pos, moving)


def pair_block(tile_place, tile_speed, tile_ident, sources, source_ident):
    offset = sources[0:3, None, :] - tile_place[:, :, None]
    motion = sources[3:6, None, :] - tile_speed[:, :, None]
    dist_sq = jnp.sum(offset * offset, axis=0) + SOFTENING_SQ
    inverse = lax.rsqrt(dist_sq)
    inverse_sq = inverse * inverse
    weight3 = jnp.where(
        source_ident[None, :] == tile_ident[:, None],
        0.0,
        sources[6][None, :] * inverse_sq * inverse,
    )
    closing = jnp.sum(offset * motion, axis=0)
    attract = jnp.sum(offset * weight3, axis=2)
    change = jnp.sum(motion * weight3 - 3.0 * (closing * inverse_sq * weight3) * offset, axis=2)
    return jnp.concatenate([attract, change], axis=0)


def correct(ahead_pos, moving, old_accel, old_jolt, span, forces):
    new_acc = forces[0:3]
    new_jolt = forces[3:6]
    second_term = -6.0 * (old_accel - new_acc) - span * (4.0 * old_jolt + 2.0 * new_jolt)
    third_term = 12.0 * (old_accel - new_acc) + 6.0 * span * (old_jolt + new_jolt)
    new_place = ahead_pos + span * span * (second_term / 24.0 + third_term / 120.0)
    new_speed = moving + span * (second_term / 6.0 + third_term / 24.0)
    return jnp.concatenate([new_place, new_speed, new_acc, new_jolt], axis=0)


def tile_forces(held, tgt_ahead, tgt_moving, slot_ids, tiles_used, shard_part, idents):
    length = shard_part.shape[1]
    block_len = length
    while block_len > 2048 and block_len % 2 == 0:
        block_len = block_len // 2
    block_count = length // block_len
    src_blocks = shard_part.reshape(7, block_count, block_len).transpose(1, 0, 2)
    ident_blocks = idents.reshape(block_count, block_len)

    def one_tile(tile_no, carried):
        place_tile = lax.dynamic_slice_in_dim(tgt_ahead, tile_no * TILE, TILE, 1)
        speed_tile = lax.dynamic_slice_in_dim(tgt_moving, tile_no * TILE, TILE, 1)
        ident_tile = lax.dynamic_slice_in_dim(slot_ids, tile_no * TILE, TILE, 0)

        def add_block(running, source_pair):
            return (
                running
                + pair_block(place_tile, speed_tile, ident_tile, source_pair[0], source_pair[1]),
                None,
            )

        running, _ = lax.scan(
            add_block, jnp.zeros((6, TILE), jnp.float32), (src_blocks, ident_blocks)
        )
        before = lax.dynamic_slice_in_dim(carried, tile_no * TILE, TILE, 1)
        return lax.dynamic_update_slice_in_dim(carried, before + running, tile_no * TILE, 1)

    return lax.fori_loop(0, tiles_used, one_tile, held)


def advance(states, last_time, weights, active, now_time, s_dev, n_tgt, n_src, my_row, my_column):
    slot_count = active.shape[0]
    own_first = (my_row * n_src + my_column) * s_dev
    listed = gathered_copies(active, "tgt", 0)
    span_all = now_time - last_time
    my_slots = lax.dynamic_slice_in_dim(listed, my_row * slot_count, slot_count, 0)
    filled = jnp.sum((my_slots >= 0).astype(jnp.int32))
    tiles_used = (filled + TILE - 1) // TILE
    local_at = listed - own_first
    is_owned = (listed >= 0) & (local_at >= 0) & (local_at < s_dev)
    stacked = jnp.concatenate([states, span_all[None, :], weights[None, :]], axis=0)
    column_all = gathered_copies(stacked, "tgt", 1)
    owner_col = my_slots // s_dev % n_src
    places = my_slots // (s_dev * n_src) * s_dev + my_slots % s_dev
    mine_owned = (my_slots >= 0) & (owner_col == my_column)
    chosen = jnp.take(column_all[0:13], jnp.clip(places, 0, n_tgt * s_dev - 1), axis=1)
    partial_rows = jnp.where(mine_owned[None, :], chosen, 0.0)
    ahead_pos, moving = predict(column_all[0:12], column_all[12:13])
    sources = jnp.concatenate([ahead_pos, moving, column_all[13:14]], axis=0)
    target = over_pieces(partial_rows, SRC)
    tgt_ahead, tgt_moving = predict(target[0:12], target[12:13])
    zero_forces = jnp.zeros((6, slot_count), jnp.float32)
    columns = jnp.arange(sources.shape[1], dtype=jnp.int32)
    idents = columns // s_dev * (s_dev * n_src) + my_column * s_dev + columns % s_dev
    partial_forces = tile_forces(
        zero_forces, tgt_ahead, tgt_moving, my_slots, tiles_used, sources, idents
    )
    forces = taken_together(partial_forces, SRC)
    corrected = correct(tgt_ahead, tgt_moving, target[6:9], target[9:12], target[12:13], forces)
    returned = gathered_copies(corrected, "tgt", 1)
    write_at = jnp.where(is_owned, local_at, s_dev)
    states = states.at[:, write_at].set(returned, mode="drop")
    last_time = last_time.at[write_at].set(now_time, mode="drop")
    return (states, last_time)


def whole_program(positions, velocities, accels, jerks, masses, levels, active_first, active_second):
    s_dev = positions.shape[1]
    n_tgt = lax.axis_size("tgt")
    n_src = lax.axis_size(SRC)
    my_row = lax.axis_index("tgt")
    my_column = lax.axis_index(SRC)
    weights = masses / (s_dev * n_tgt * n_src)
    states = jnp.concatenate([positions, velocities, accels, jerks], axis=0)
    last_time = -BASE_STEP * jnp.exp2(-levels.astype(jnp.float32))
    for now_time, active in ((TIME_FIRST, active_first), (TIME_SECOND, active_second)):
        states, last_time = advance(
            states, last_time, weights, active, now_time, s_dev, n_tgt, n_src, my_row, my_column
        )
    return (states[0:3], states[3:6], states[6:9], states[9:12])


def log2_of(size):
    assert size & (size - 1) == 0, "size"
    return size.bit_length() - 1


def iota(shape, dim):
    return lax.broadcasted_iota(jnp.int32, shape, dim)


def lane_pick(table, lanes):
    return lax.gather(
        table,
        lanes[:, :, None],
        lax.GatherDimensionNumbers(
            offset_dims=(),
            collapsed_slice_dims=(1,),
            start_index_map=(1,),
            operand_batching_dims=(0,),
            start_indices_batching_dims=(0,),
        ),
        slice_sizes=(1, 1),
        mode=lax.GatherScatterMode.PROMISE_IN_BOUNDS,
    )


def turned(rows):
    pad = jnp.zeros((LANES - rows.shape[0], LANES), rows.dtype)
    return jnp.concatenate([rows, pad], axis=0).T


def rows_of(values, count):
    width = values[0].shape[1]
    below = count - sum(v.shape[0] for v in values)
    pad = [jnp.zeros((below, width), jnp.float32)] if below else []
    return jnp.concatenate(list(values) + pad, axis=0)


def prepare_kernel(n_stars, pos, vel, acc, jerk, mass, levels, first, second, column_out, row_out, own_out):
    s_dev = pos.shape[1]
    last = -BASE_STEP * jnp.exp2(-levels[...].astype(jnp.float32))
    states = jnp.concatenate([pos[...], vel[...], acc[...], jerk[...]], axis=0)
    weights = mass[...] / n_stars
    room = first.shape[1] + second.shape[1]
    lists = [first[...].astype(jnp.float32), second[...].astype(jnp.float32)]
    if s_dev > room:
        lists.append(jnp.full((1, s_dev - room), -1.0, jnp.float32))
    listed = jnp.concatenate(lists, axis=1)
    column = rows_of([states, last, listed, weights], 16)
    column_out[...] = column
    ahead, moving = predict(states, TIME_FIRST - last)
    ahead_second, moving_second = predict(states, TIME_SECOND - last)
    row = rows_of([ahead, moving, weights, ahead_second, moving_second], CHUNK_ROWS)
    row = jnp.concatenate([row[:, at : at + LANES] for at in range(0, s_dev, LANES)], axis=0)
    for copy in range(row_out.shape[0]):
        row_out[copy] = row
    own_out[...] = rows_of([states, last, weights], 16)


def in_column(listed, column, n_src, s_dev):
    ids = listed.astype(jnp.int32)
    return (ids >= 0) & (((ids >> log2_of(s_dev)) & (n_src - 1)) == column)


def most_listed(listed, n_src, s_dev):
    ids = listed.astype(jnp.int32)
    n_tgt, width = ids.shape
    valid = ids >= 0
    column_of = jnp.where(valid, (ids >> log2_of(s_dev)) & (n_src - 1), -1)
    row_of = jnp.where(valid, ids >> log2_of(s_dev * n_src), -1)
    cells = jnp.zeros((n_tgt, n_src), jnp.float32)
    for slots in range(n_tgt):
        in_row = (row_of[slots : slots + 1] == iota((n_tgt, width), 0)).astype(jnp.bfloat16)
        in_col = (column_of[slots : slots + 1] == iota((n_src, width), 0)).astype(jnp.bfloat16)
        cells = cells + lax.dot_general(
            in_row, in_col, (((1,), (1,)), ((), ())), preferred_element_type=jnp.float32
        )
    return jnp.max(jnp.sum(cells, axis=0, keepdims=True)), jnp.max(cells)


def slot_numbers(mine):
    n_rows, width = mine.shape
    upto = (iota((width, width), 0) <= iota((width, width), 1)).astype(jnp.bfloat16)
    inside = jnp.dot(mine.astype(jnp.bfloat16), upto, preferred_element_type=jnp.float32)
    totals = jnp.broadcast_to(inside[:, width - 1 : width], (n_rows, LANES))
    place = jnp.zeros((1, LANES), jnp.float32)
    before = []
    for row in range(n_rows):
        before.append(place)
        place = place + totals[row : row + 1]
    start = jnp.concatenate(before, axis=0)[:, 0:1]
    return jnp.where(mine, (inside + start).astype(jnp.int32) - 1, -1), jnp.max(place)


def packed_ids(listed, slot, part):
    n_rows, width = listed.shape
    found = jnp.zeros((LANES, LANES), jnp.float32)
    want = iota((LANES, LANES), 0) + part * LANES
    for row in range(n_rows):
        for chunk in range(width // LANES):
            cut = slice(chunk * LANES, (chunk + 1) * LANES)
            hit = jnp.broadcast_to(slot[row : row + 1, cut], (LANES, LANES)) == want
            found = found + jnp.where(hit, listed[row : row + 1, cut] + 1.0, 0.0)
    ids = jnp.broadcast_to(jnp.sum(found, axis=1, keepdims=True) - 1.0, (LANES, LANES))
    return ids.T[0:1]


def target_facts(number, held, my_row, n_src):
    n_tgt, _, s_dev = held.shape
    row_bits, per_row = log2_of(s_dev * n_src), s_dev // LANES
    ids = number.astype(jnp.int32)
    lane = jnp.broadcast_to(ids & (LANES - 1), (16, LANES))
    chunk_of = jnp.where(ids >= 0, (ids >> row_bits) * per_row + ((ids & (s_dev - 1)) >> log2_of(LANES)), -1)

    def one_row(row, picked):
        for chunk in range(per_row):
            table = held[row, :, chunk * LANES : (chunk + 1) * LANES]
            picked = jnp.where(chunk_of == row * per_row + chunk, lane_pick(table, lane), picked)
        return picked

    picked = lax.fori_loop(0, n_tgt, one_row, jnp.zeros((16, LANES), jnp.float32), unroll=2)
    key = jnp.where((ids >= 0) & ((ids >> row_bits) == my_row), ids & (s_dev - 1), -1)
    return rows_of([picked[0:13], number, picked[14:15], key.astype(jnp.float32)], 16)


def select_kernel(n_src, slots_first, slots_second, held, target_out, turned_out, info_out):
    s_dev = held.shape[2]
    my_row, my_column = lax.axis_index("tgt"), lax.axis_index(SRC)
    listed = held[:, 13, :]
    first = listed[:, :slots_first]
    slot, count = slot_numbers(in_column(first, my_column, n_src, s_dev))
    count = jnp.minimum(count.astype(jnp.int32), FIRST_ROOM)
    info_out[0] = count
    info_out[1] = 0

    def fill(part):
        facts = target_facts(packed_ids(first, slot, part), held, my_row, n_src)
        ahead, moving = predict(facts[0:12], TIME_FIRST - facts[12:13])
        cut = slice(part * LANES, (part + 1) * LANES)
        target_out[:, cut] = facts
        turned_out[cut, :] = turned(rows_of([ahead, moving, facts[15:16], facts[13:14]], 8))

    fill(0)
    for part in range(1, FIRST_ROOM // LANES):
        pl.when(count > part * LANES)(functools.partial(fill, part))

        @pl.when(count <= part * LANES)
        def _():
            cut = slice(part * LANES, (part + 1) * LANES)
            target_out[:, cut] = jnp.full((16, LANES), -1.0, jnp.float32)
            turned_out[cut, :] = jnp.full((LANES, LANES), -1.0, jnp.float32)


def found_slots(keys, wanted):
    found = jnp.zeros((LANES, LANES), jnp.float32)
    for part, key in enumerate(keys):
        place = (iota((LANES, LANES), 0) + part * LANES + 1).astype(jnp.float32)
        found = found + jnp.where((key == wanted) & (key >= 0.0), place, 0.0)
    return jnp.sum(found, axis=0, keepdims=True).astype(jnp.int32) - 1


def plan_kernel(n_src, slots_first, slots_second, held, first_target, turned_in, second_out, plan_out, info_out):
    s_dev = held.shape[2]
    my_row, my_column = lax.axis_index("tgt"), lax.axis_index(SRC)
    lists = held[:, 13, :]
    first, listed = lists[:, :slots_first], lists[:, slots_first : slots_first + slots_second]
    most_first, most_own = most_listed(first, n_src, s_dev)
    most_second, _ = most_listed(listed, n_src, s_dev)
    fits = (most_first <= FIRST_ROOM) & (most_second <= SECOND_ROOM) & (most_own <= OWN_ROOM)
    info_out[1] = fits.astype(jnp.int32)
    slot, count = slot_numbers(in_column(listed, my_column, n_src, s_dev))
    info_out[0] = jnp.minimum(count.astype(jnp.int32), SECOND_ROOM)
    facts = target_facts(packed_ids(listed, slot, 0), held, my_row, n_src)
    second_out[...] = facts
    parts = FIRST_ROOM // LANES
    columns = [turned_in[part * LANES : (part + 1) * LANES, :] for part in range(parts)]
    keys = [jnp.broadcast_to(c[:, 6:7], (LANES, LANES)) for c in columns]
    numbers = [jnp.broadcast_to(c[:, 7:8], (LANES, LANES)) for c in columns]
    second_keys = [jnp.broadcast_to(facts[15:16], (LANES, LANES)).T]
    plan_out[...] = jnp.full(plan_out.shape, -1, jnp.int32)
    for chunk in range(s_dev // LANES):
        cut = slice(chunk * LANES, (chunk + 1) * LANES)
        star = (iota((1, LANES), 1) + chunk * LANES).astype(jnp.float32)
        plan_out[0:1, cut] = found_slots(keys, star)
        plan_out[1:2, cut] = found_slots(second_keys, star)
    plan_out[2:3, 0:LANES] = found_slots(numbers, facts[13:14])
    own = [(key >= 0.0) for key in keys]
    upto = (iota((LANES, LANES), 1) <= iota((LANES, LANES), 0)).astype(jnp.bfloat16)
    before = jnp.zeros((1, LANES), jnp.float32)
    order = []
    for flags in own:
        inside = jnp.dot(upto, flags.astype(jnp.bfloat16), preferred_element_type=jnp.float32) + before
        order.append(jnp.where(flags, inside - 1.0, -1.0))
        before = inside[LANES - 1 : LANES]
    plan_out[3:4, 0:LANES] = found_slots(order, iota((1, LANES), 1).astype(jnp.float32))


def pair_terms(source, target, own_place=None, key=None):
    rx, ry, rz = (source[j] - target[j] for j in range(3))
    ux, uy, uz = (source[j] - target[j] for j in range(3, 6))
    inverse = lax.rsqrt((rx * rx + ry * ry + rz * rz) + SOFTENING_SQ)
    inverse_sq = inverse * inverse
    weight3 = source[6] * inverse * inverse_sq
    if own_place is not None:
        weight3 = jnp.where(key == own_place, 0.0, weight3)
    closing = (rx * ux + ry * uy + rz * uz) * inverse_sq
    ax, ay, az = rx * weight3, ry * weight3, rz * weight3
    return (ax, ay, az, ux * weight3, uy * weight3, uz * weight3, ax * closing, ay * closing, az * closing)


def added(running, parts):
    return tuple(a + b for a, b in zip(running, parts))


def target_blocks(count, turned_in, sums, visit):
    def one_block(first, tall):
        at = pl.ds(pl.multiple_of(first, 8), tall)
        facts = turned_in[at, :]
        target = [jnp.broadcast_to(facts[:, j : j + 1], (tall, LANES)) for j in range(6)]
        key = jnp.broadcast_to(facts[:, 6:7], (tall, LANES))
        running = visit(tall, target, key, (jnp.zeros((tall, LANES), jnp.float32),) * 9)
        totals = [running[j] for j in range(3)] + [running[3 + j] - 3.0 * running[6 + j] for j in range(3)]
        lanes = iota((tall, LANES), 1)
        packed = sums[at, :]
        for j in range(6):
            total = jnp.broadcast_to(jnp.sum(totals[j], axis=1, keepdims=True), (tall, LANES))
            packed = packed + jnp.where(lanes == j, total, 0.0)
        sums[at, :] = packed

    tall_blocks = (count + 7) // 16
    pl.loop(0, tall_blocks)(lambda block: one_block(block * 16, 16))
    pl.when(count > tall_blocks * 16)(lambda: one_block(tall_blocks * 16, 8))


def row_sums(count, stars, first_row, turned_in, sums):
    _, n_z, height, _ = stars.shape
    my_z, my_core = lax.axis_index("z"), lax.axis_index("core")
    rows = [first_row + j for j in range(6)] + [6]
    sums[...] = jnp.zeros_like(sums)

    def visit(tall, target, key, running):
        def segment(core, which, running, own=False):
            for chunk in range(height // CHUNK_ROWS):
                at = chunk * CHUNK_ROWS
                source = [jnp.broadcast_to(stars[core, which, at + j : at + j + 1, :], (tall, LANES)) for j in rows]
                place = (iota((tall, LANES), 1) + chunk * LANES).astype(jnp.float32) if own else None
                running = added(running, pair_terms(source, target, place, key))
            return running

        def both(step, running):
            return segment(my_core, jnp.where(step < my_z, step, step + 1), segment(1 - my_core, step, running))

        running = lax.fori_loop(0, n_z - 1, both, running)
        return segment(my_core, my_z, segment(1 - my_core, n_z - 1, running), own=True)

    target_blocks(count, turned_in, sums, visit)


def write_sums(sums, force_out):
    copies, _, room = force_out.shape
    for part in range(room // LANES):
        cut = slice(part * LANES, (part + 1) * LANES)
        rows = sums[cut, :].T[0:8]
        for copy in range(copies):
            force_out[copy, :, cut] = rows


def first_force_kernel(info, stars, turned_in, force_out, sums):
    row_sums(info[0], stars, 0, turned_in, sums)
    write_sums(sums, force_out)


def second_force_kernel(info, stars, turned_in, sums_out):
    row_sums(info[0], stars, 7, turned_in, sums_out)


def update_force_kernel(info, updates, turned_in, sums_in, force_out, sums, stars):
    n_z = updates.shape[1]
    my_z, my_core = lax.axis_index("z"), lax.axis_index("core")
    half = iota((8, LANES), 1) < LANES // 2
    own_half = half[7:8] == (my_core == 0)
    for z in range(n_z):
        both = updates[0, z] + updates[1, z]
        place = jnp.where(own_half & (my_z == z), both[7:8], -2.0)
        stars[z] = jnp.concatenate([both[0:7], place], axis=0)
    sums[...] = sums_in[...]

    def visit(tall, target, key, running):
        def one(z, running):
            source = [jnp.broadcast_to(stars[z, j : j + 1, :], (tall, LANES)) for j in range(8)]
            return added(running, pair_terms(source, target, source[7], key))

        return lax.fori_loop(0, n_z, one, running, unroll=8 if n_z % 8 == 0 else 1)

    target_blocks(info[0], turned_in, sums, visit)
    write_sums(sums, force_out)


def summed(received):
    total = received[0]
    for row in range(1, received.shape[0]):
        total = total + received[row]
    return total


def picked_slots(values, slot):
    lane = jnp.broadcast_to(slot & (LANES - 1), (16, LANES))
    new = jnp.zeros((16, LANES), jnp.float32)
    for part in range(values.shape[1] // LANES):
        pick = lane_pick(values[:, part * LANES : (part + 1) * LANES], lane)
        new = jnp.where((slot >> log2_of(LANES)) == part, pick, new)
    return new


def correct_kernel(received, target, second, plan, own, update_out, own_out, second_out, turned_out):
    copies = update_out.shape[0]
    room = received.shape[2]
    s_dev = own.shape[1]
    forces = summed(received)
    states = target[0:12, :]
    span = TIME_FIRST - target[12:13, :]
    ahead, moving = predict(states, span)
    corrected = correct(ahead, moving, states[6:9], states[9:12], span, forces[0:6])
    corrected = rows_of([corrected, jnp.full((1, room), TIME_FIRST, jnp.float32)], 16)
    slot = plan[3:4, 0:LANES]
    old = picked_slots(target[...], slot)
    new = picked_slots(corrected, slot)
    present = slot >= 0
    weight, place = old[14:15], jnp.where(present, old[15:16], -1.0)
    ahead_new, moving_new = predict(new[0:12], TIME_SECOND - new[12:13])
    ahead_old, moving_old = predict(old[0:12], TIME_SECOND - old[12:13])
    arrived = jnp.concatenate([ahead_new, moving_new, weight, place], axis=0)
    left = jnp.concatenate([ahead_old, moving_old, -weight, place], axis=0)
    lane = iota((8, LANES), 1)
    update = jnp.where(lane < OWN_ROOM, arrived, pltpu.roll(left, OWN_ROOM, axis=1))
    update = jnp.where(lane < 2 * OWN_ROOM, update, 0.0)
    update = jnp.where(lax.axis_index("core") == 0, update, pltpu.roll(update, LANES // 2, axis=1))
    for copy in range(copies):
        update_out[copy] = update
    for chunk in range(s_dev // LANES):
        cut = slice(chunk * LANES, (chunk + 1) * LANES)
        slot = plan[0:1, cut]
        own_out[:, cut] = jnp.where(slot >= 0, picked_slots(corrected, slot), own[:, cut])
    other = second[...]
    slot = plan[2:3, 0:LANES]
    states = jnp.where(slot >= 0, picked_slots(corrected, slot), other)
    span = TIME_SECOND - states[12:13]
    ahead, moving = predict(states[0:12], span)
    second_out[...] = rows_of([ahead, moving, states[6:12], span], 16)
    turned_out[...] = turned(rows_of([ahead, moving, other[15:16]], 8))


def finish_kernel(received, second, plan, own, pos_out, vel_out, acc_out, jerk_out):
    forces = summed(received)
    facts = second[...]
    corrected = correct(facts[0:3], facts[3:6], facts[6:9], facts[9:12], facts[12:13], forces[0:6])
    corrected = rows_of([corrected], 16)
    for chunk in range(own.shape[1] // LANES):
        cut = slice(chunk * LANES, (chunk + 1) * LANES)
        slot = plan[1:2, cut]
        new = jnp.where(slot >= 0, picked_slots(corrected, slot), own[:, cut])
        pos_out[:, cut] = new[0:3]
        vel_out[:, cut] = new[3:6]
        acc_out[:, cut] = new[6:9]
        jerk_out[:, cut] = new[9:12]


def f32(*shape):
    return jax.ShapeDtypeStruct(shape, jnp.float32)


INTERPRET = False


def call(kernel, outs, scalars=0, operands=0, scratch=(), smem_out=None):
    smem, vmem = pl.BlockSpec(memory_space=pltpu.SMEM), pl.BlockSpec(memory_space=pltpu.VMEM)
    return pl.pallas_call(
        kernel,
        out_shape=outs,
        in_specs=[smem] * scalars + [vmem] * operands,
        out_specs=tuple(smem if i == smem_out else vmem for i in range(len(outs))),
        scratch_shapes=list(scratch),
        interpret=INTERPRET,
        compiler_params=pltpu.CompilerParams(vmem_limit_bytes=16 << 20),
    )


def exchanged(copies, axis):
    return lax.all_to_all(copies, axis, split_axis=0, concat_axis=0, tiled=True)


def both_cores(near):
    return lax.all_gather(near, "core")


def shards(positions, velocities, accels, jerks, masses, levels, active_first, active_second):
    s_dev = positions.shape[1]
    n_tgt, n_z, n_src = lax.axis_size("tgt"), lax.axis_size("z"), lax.axis_size(SRC)
    n_stars = s_dev * n_tgt * n_src
    scalar = jax.ShapeDtypeStruct((2,), jnp.int32)
    lists = (n_src, active_first.shape[0], active_second.shape[0])
    column, row_copies, own = call(
        functools.partial(prepare_kernel, n_stars), (f32(16, s_dev), f32(n_z, CHUNK_ROWS * s_dev // LANES, LANES), f32(16, s_dev)), 0, 8
    )(
        positions, velocities, accels, jerks, masses.reshape(1, s_dev), levels.reshape(1, s_dev),
        active_first.reshape(1, -1), active_second.reshape(1, -1),
    )
    near = exchanged(row_copies, "z")
    column = lax.all_gather(column, "tgt")
    stars = both_cores(near)
    target, columns, info = call(
        functools.partial(select_kernel, *lists), (f32(16, FIRST_ROOM), f32(FIRST_ROOM, LANES), scalar), 0, 1, smem_out=2
    )(column)
    (partial,) = call(
        first_force_kernel, (f32(n_tgt, 8, FIRST_ROOM),), 1, 2, [pltpu.VMEM((FIRST_ROOM, LANES), jnp.float32)]
    )(info, stars, columns)
    received = exchanged(partial, "tgt")
    second, plan, second_info = call(
        functools.partial(plan_kernel, *lists),
        (f32(16, SECOND_ROOM), jax.ShapeDtypeStruct((8, s_dev), jnp.int32), scalar), 0, 3, smem_out=2,
    )(column, target, columns)
    update, own, second, second_columns = call(
        correct_kernel, (f32(n_z, 8, LANES), f32(16, s_dev), f32(16, SECOND_ROOM), f32(LANES, LANES)), 0, 5
    )(received, target, second, plan, own)
    near_update = exchanged(update, "z")
    (sums,) = call(second_force_kernel, (f32(SECOND_ROOM, LANES),), 1, 2)(second_info, stars, second_columns)
    updates = both_cores(near_update)
    (partial,) = call(
        update_force_kernel, (f32(n_tgt, 8, SECOND_ROOM),), 1, 3,
        [pltpu.VMEM((SECOND_ROOM, LANES), jnp.float32), pltpu.VMEM((n_z, 8, LANES), jnp.float32)],
    )(second_info, updates, second_columns, sums)
    received = exchanged(partial, "tgt")

    def by_columns(received, second, plan, own, *inputs):
        return tuple(call(finish_kernel, (f32(3, s_dev),) * 4, 0, 4)(received, second, plan, own))

    def anywhere(received, second, plan, own, *inputs):
        return whole_program(*inputs)

    inputs = (positions, velocities, accels, jerks, masses, levels, active_first, active_second)
    return lax.cond(second_info[1] == 1, by_columns, anywhere, received, second, plan, own, *inputs)


def solution(mesh):
    n_tgt, n_src = mesh.devices.shape
    finer = Mesh(mesh.devices.reshape(n_tgt, n_src // 2, 2), ("tgt", "z", "core"))
    stars = ("tgt", "z", "core")
    vector, scalar = P(None, stars), P(stars)
    return jax.shard_map(
        shards,
        mesh=finer,
        in_specs=(vector, vector, vector, vector, scalar, scalar, P("tgt"), P("tgt")),
        out_specs=(vector,) * 4,
        check_vma=False,
    )
```
